32 devices in a mesh: leaf: 16 (over z, y, core), top: 2 (over x).
Axes of the slice: x: 2, y: 2, z: 4, core: 2. Of those that a mesh axis runs over, the one named last changes fastest.
Arguments:
- vectors: bfloat16 [2, 16, 768, 512], P('top', 'leaf'), may hold values from -6 to 6
- near_tiles: bfloat16 [2, 16, 8, 768, 768], P('top', 'leaf'), may hold values from -0.078125 to 0.078125
- leaf_basis: bfloat16 [2, 16, 768, 128], P('top', 'leaf'), may hold values from -0.21875 to 0.21875
- transfer: bfloat16 [2, 16, 128, 128], P('top', 'leaf'), may hold values from -0.25 to 0.25
- coupling: bfloat16 [2, 16, 7, 128, 128], P('top', 'leaf'), may hold values from -0.1875 to 0.1875
- top_coupling: bfloat16 [2, 2, 128, 128], P('top'), may hold values from -0.375 to 0.375
- near_list: int32 [2, 16, 8], P('top', 'leaf'), may hold values from -4 to 4, as said below
- far_list: int32 [2, 16, 7], P('top', 'leaf'), may hold values from 0 to 15, as said below
- row_counts: int32 [2, 16], P('top', 'leaf'), may hold values from 384 to 768
Outputs:
- product: float32 [2, 16, 768, 512], P('top', 'leaf')
The draws below stay inside these ranges and needn't reach their ends.
Inputs may be any that keep to these rules, and one draw needn't show every extreme that they name: `near_list`: each leaf's 8 offsets are distinct; an offset that leads outside the cluster's 16 leaves stands for an absent block. `far_list`: each leaf's entries are distinct positions in its cluster, each more than 4 away from the leaf's own position. `row_counts`: rows at and beyond the count are padding.
All inputs are finite; a program needn't handle non-finite values.
Results may differ from the reference program's by a relative error of at most 0.0045.
Values may be sent and summed in bfloat16 or wider, within the bound.
A program may use at most 128 MiB of HBM per device.

```python
import jax
import jax.numpy as jnp
from jax import lax

LEAF_ROWS = 768
RANK = 128
VECS = 512
REACH = 4
NEAR = 8
FAR = 7
CLUSTERS = 2
GROUP = 16
TOPFAR = 2


def draw_near_list(key, part):
    subkeys = jax.random.split(key, CLUSTERS * GROUP)
    orders = jax.vmap(lambda single: jax.random.permutation(single, 2 * REACH + 1))(subkeys)
    return (orders[:, :NEAR] - REACH).astype(jnp.int32).reshape(CLUSTERS, GROUP, NEAR)


def draw_far_list(key, part):
    scores = jax.random.randint(jax.random.fold_in(key, 7), (CLUSTERS, GROUP, GROUP), 0, 1 << 20)
    column = jnp.arange(GROUP, dtype=jnp.int32)
    scores = scores * GROUP + column[None, None, :]
    distance = jnp.abs(column[:, None] - column[None, :])
    scores = jnp.where(distance[None] > REACH, scores, -1)
    values, picked = lax.top_k(scores, FAR)
    return picked.astype(jnp.int32)


def touch_ends(result, stream_key, smallest, high):
    index_at = [jax.random.randint(jax.random.fold_in(stream_key, axis), (), 0, length) for axis, length in enumerate(result.shape)]
    widest = result.shape.index(max(result.shape))
    beside = index_at[:widest] + [(index_at[widest] + 1) % result.shape[widest]] + index_at[widest + 1:]
    return result.at[tuple(index_at)].set(smallest).at[tuple(beside)].set(high)


def shard_levels(own_key, extent, shards, smallest, high):
    gain, own = 1.0, jax.random.fold_in(own_key, 6)
    for dim, blocks in shards:
        heights = jnp.exp(jax.random.uniform(jax.random.fold_in(own, dim), (blocks,), jnp.float32, smallest / len(shards), high / len(shards)))
        gain = gain * jnp.repeat(heights, extent[dim] // blocks).reshape([-1 if axis == dim else 1 for axis in range(len(extent))])
    return gain


def normal_values(stream_key, extent, width, most, cuts=(), kind=jnp.bfloat16):
    factor_of = shard_levels(stream_key, extent, cuts, -0.22, 0.18) if cuts else 1.0
    result = jax.random.normal(stream_key, extent, jnp.float32) * width * factor_of
    return jnp.minimum(jnp.maximum(result, -most), most).astype(kind)


def setup_inputs(seed: int = 0) -> dict:
    streams_of = jax.random.split(jax.random.key(seed), 10)
    vectors = normal_values(streams_of[0], (CLUSTERS, GROUP, LEAF_ROWS, VECS), 1.0, 6.0, ((0, 2), (1, 16)))
    near_tiles = normal_values(streams_of[1], (CLUSTERS, GROUP, NEAR, LEAF_ROWS, LEAF_ROWS), (NEAR * LEAF_ROWS) ** -0.5, 0.078125, ((0, 2), (1, 16)))
    leaf_basis = normal_values(streams_of[2], (CLUSTERS, GROUP, LEAF_ROWS, RANK), LEAF_ROWS ** -0.5, 0.21875, ((0, 2), (1, 16)))
    transfer = normal_values(streams_of[3], (CLUSTERS, GROUP, RANK, RANK), (RANK * 4) ** -0.5, 0.25, ((0, 2), (1, 16)))
    coupling = normal_values(streams_of[4], (CLUSTERS, GROUP, FAR, RANK, RANK), (RANK * FAR) ** -0.5, 0.1875, ((0, 2), (1, 16)))
    top_coupling = normal_values(streams_of[5], (CLUSTERS, TOPFAR, RANK, RANK), (RANK * TOPFAR) ** -0.5, 0.375, ((0, 2),))
    near_list = draw_near_list(jax.random.fold_in(streams_of[9], 71), 0)
    far_list = draw_far_list(jax.random.fold_in(streams_of[9], 71), 0)
    row_counts = touch_ends(jax.random.randint(streams_of[8], (CLUSTERS, GROUP), LEAF_ROWS // 2, LEAF_ROWS + 1), jax.random.fold_in(streams_of[8], 1), LEAF_ROWS // 2, LEAF_ROWS).astype(jnp.int32)
    return {"vectors": vectors, "near_tiles": near_tiles, "leaf_basis": leaf_basis, "transfer": transfer, "coupling": coupling, "top_coupling": top_coupling, "near_list": near_list, "far_list": far_list, "row_counts": row_counts}


def reference(vectors, near_tiles, leaf_basis, transfer, coupling, top_coupling, near_list, far_list, row_counts):
    row_index = jnp.arange(LEAF_ROWS, dtype=jnp.int32)
    keep = (row_index[None, None, :] < row_counts[:, :, None]).astype(jnp.bfloat16)
    masked = vectors * keep[..., None]

    def near_leaf(index):
        cluster = index // GROUP
        member = index % GROUP
        targets = member + near_list[cluster, member]
        valid = ((targets >= 0) & (targets < GROUP)).astype(jnp.bfloat16)
        safe = jnp.clip(targets, 0, GROUP - 1).astype(jnp.int32)
        sources = masked[cluster][safe] * valid[:, None, None]
        return jnp.einsum("kij,kjv->iv", near_tiles[cluster, member].astype(jnp.float32), sources.astype(jnp.float32))

    near = lax.map(near_leaf, jnp.arange(CLUSTERS * GROUP, dtype=jnp.int32))
    near = near.reshape(CLUSTERS, GROUP, LEAF_ROWS, VECS)

    basis = leaf_basis.astype(jnp.float32)
    nested = transfer.astype(jnp.float32)
    coeff = jnp.einsum("cgir,cgiv->cgrv", basis, masked.astype(jnp.float32)).astype(jnp.bfloat16)
    upward = jnp.einsum("cgab,cgav->cgbv", nested, coeff.astype(jnp.float32))
    parent = jnp.sum(upward, axis=1).astype(jnp.bfloat16)
    cluster_ids = jnp.arange(CLUSTERS, dtype=jnp.int32)
    sibling_ids = (cluster_ids[:, None] + 1 + jnp.arange(TOPFAR, dtype=jnp.int32)[None, :]) % CLUSTERS
    chosen = parent[sibling_ids]
    parent_field = jnp.einsum("cmab,cmbv->cav", top_coupling.astype(jnp.float32), chosen.astype(jnp.float32)).astype(jnp.bfloat16)
    cluster_index = cluster_ids[:, None, None]
    siblings = coeff[cluster_index, far_list]
    local_field = jnp.einsum("cgmab,cgmbv->cgav", coupling.astype(jnp.float32), siblings.astype(jnp.float32))
    local_field = local_field + jnp.einsum("cgab,cbv->cgav", nested, parent_field.astype(jnp.float32))
    local_field = local_field.astype(jnp.bfloat16)
    far = jnp.einsum("cgir,cgrv->cgiv", basis, local_field.astype(jnp.float32))
    return (near + far) * keep[..., None].astype(jnp.float32)
```

```python
import functools

import jax
import jax.numpy as jnp
from jax import lax
from jax.experimental import pallas as pl
from jax.experimental.pallas import tpu as pltpu
from jax.sharding import PartitionSpec as P

REACH = 4
SLOTS = 2 * REACH + 2
PIECES = 3


def contract(left, right):
    return lax.dot_general(left, right, (((0,), (0,)), ((), ())), preferred_element_type=jnp.float32)


def dot(left, right):
    return jnp.dot(left, right, preferred_element_type=jnp.float32)


def send_count(levels, clusters):
    return 40 + 12 * levels + clusters


def exchange_kernel(
    levels,
    clusters,
    near_ref,
    far_ref,
    count_ref,
    vectors_ref,
    tiles_ref,
    basis_ref,
    nested_ref,
    coupling_ref,
    top_ref,
    acc,
    field_ref,
    raw,
    tiles,
    basis,
    nested,
    coupling,
    top,
    window,
    coeffs,
    halves,
    half_in,
    quarters,
    partial,
    quarter_in,
    sums,
    parents,
    fields,
    tile_sem,
    load_sem,
    send_sem,
    block_sem,
    piece_sem,
    coeff_sem,
    half_sem,
    quarter_sem,
    sum_sem,
    parent_sem,
    field_sem,
):
    me = lax.axis_index("leaf")
    cluster = lax.axis_index("top")
    core = lax.rem(me, 2)
    column = lax.rem(lax.div(me, 2), 2)
    level = lax.div(me, 4)
    other = 1 - core
    partner = me + 1 - 2 * core
    beside = me + 2 - 4 * column
    above = level < levels - 1
    below = level > 0
    first_column = column == 0
    rows, vecs = raw.shape
    half = vecs // 2
    quarter = vecs // 4
    piece = rows // PIECES
    tile_count = tiles.shape[0]

    def load(source, target, sem):
        return pltpu.make_async_copy(source, target, sem)

    raw_load = load(vectors_ref.at[0, 0], raw, load_sem.at[0])
    basis_load = load(basis_ref.at[0, 0], basis, load_sem.at[1])
    nested_load = load(nested_ref.at[0, 0], nested, load_sem.at[2])
    coupling_load = load(coupling_ref.at[0, 0], coupling, load_sem.at[3])
    top_load = load(top_ref.at[0], top, load_sem.at[4])
    tile_loads = [load(tiles_ref.at[0, 0, k], tiles.at[k], tile_sem.at[k]) for k in range(tile_count)]
    for copy in [raw_load, basis_load, nested_load] + tile_loads + [coupling_load, top_load]:
        copy.start()

    barrier = pltpu.get_barrier_semaphore()
    peers = [{"leaf": partner}, {"leaf": beside}]
    for step in range(1, levels):
        peers.append({"leaf": lax.rem(me + 4 * step, 4 * levels)})
    for step in range(1, clusters):
        peers.append({"top": lax.rem(cluster + step, clusters)})
    for peer in peers:
        pl.semaphore_signal(barrier, inc=1, device_id=peer, device_id_type=pl.DeviceIdType.MESH)

    sent = []

    def send(source, target, sem, peer, condition=None):
        copy = pltpu.make_async_remote_copy(
            src_ref=source,
            dst_ref=target,
            send_sem=send_sem.at[len(sent)],
            recv_sem=sem,
            device_id=peer,
            device_id_type=pl.DeviceIdType.MESH,
        )
        sent.append((condition, copy))
        if condition is None:
            copy.start()
        else:
            pl.when(condition)(copy.start)

    def receive(block, sem, condition=None):
        copy = pltpu.make_async_remote_copy(
            src_ref=block,
            dst_ref=block,
            send_sem=send_sem.at[0],
            recv_sem=sem,
            device_id={"leaf": partner},
            device_id_type=pl.DeviceIdType.MESH,
        )
        if condition is None:
            copy.wait_recv()
        else:
            pl.when(condition)(copy.wait_recv)

    to_partner, to_beside = {"leaf": partner}, {"leaf": beside}
    to_above, to_below = {"leaf": me + 4}, {"leaf": me - 4}

    own_slot = REACH + core
    partner_slot = REACH + other
    beside_slot = core + 6 - 4 * column
    diagonal_slot = core + 2 + 4 * column
    below_slot = core
    above_slot = core + 8
    diagonal = jnp.logical_or(
        jnp.logical_and(first_column, below), jnp.logical_and(column == 1, above)
    )
    relay_over = jnp.logical_or(
        jnp.logical_and(column == 1, below), jnp.logical_and(first_column, above)
    )
    relay_up = jnp.logical_and(first_column, above)
    relay_down = jnp.logical_and(column == 1, below)

    def send_block(slot, part, target, peer, condition=None):
        send(window.at[slot, part], window.at[target, part], block_sem.at[target, part], peer, condition)

    def wait_block(slot, part, condition=None):
        receive(window.at[slot, part], block_sem.at[slot, part], condition)

    def span_of(index):
        return pl.ds(index * piece, piece)

    def send_piece(slot, part, index, target, peer, condition=None):
        send(
            window.at[slot, part, span_of(index)],
            window.at[target, part, span_of(index)],
            piece_sem.at[target, part, index],
            peer,
            condition,
        )

    def wait_piece(slot, part, index, condition=None):
        receive(window.at[slot, part, span_of(index)], piece_sem.at[slot, part, index], condition)

    def send_coeff(leaf, peer, condition=None):
        send(coeffs.at[leaf], coeffs.at[leaf], coeff_sem.at[leaf], peer, condition)

    def wait_coeff(leaf, condition=None):
        receive(coeffs.at[leaf], coeff_sem.at[leaf], condition)

    def exists(step):
        return jnp.logical_and(level + step >= 0, level + step < levels)

    def crosses(step, from_first):
        return step <= -1 or step >= 2 if from_first else step >= 1 or step <= -2

    def crossing(step):
        if crosses(step, True) and crosses(step, False):
            return exists(step)
        return jnp.logical_and(exists(step), first_column if crosses(step, True) else column == 1)

    def crossed(step):
        if crosses(step, True) and crosses(step, False):
            return exists(step)
        return jnp.logical_and(exists(step), column == 1 if crosses(step, True) else first_column)

    def handed(step, which):
        if abs(step) >= 2:
            return exists(step)
        return jnp.logical_and(exists(step), which == (1 if step == 1 else 0))

    def relay_coeffs(hop):
        for step in (-hop, hop):
            wait_coeff(me + 4 * step, exists(step))
        if hop + 1 < levels:
            send_coeff(me - 4 * hop, to_above, jnp.logical_and(exists(-hop), above))
            send_coeff(me + 4 * hop, to_below, jnp.logical_and(exists(hop), below))

    def cross_coeffs(hop):
        for step in (-hop, hop):
            send_coeff(me + 4 * step, to_beside, crossing(step))
            send_coeff(me + 4 * step, to_partner, handed(step, core))

    def hand_crossed(hop):
        for step in (-hop, hop):
            wait_coeff(beside + 4 * step, crossed(step))
            send_coeff(beside + 4 * step, to_partner, crossed(step))

    def near(slot, part, condition=None, first=False, index=None):
        offset = slot - REACH - core
        place, hit = 0, 0
        for k in range(tile_count):
            here = near_ref[0, 0, k] == offset
            place = jnp.where(here, k, place)
            hit = jnp.where(here, 1, hit)
        scale = hit.astype(jnp.float32)

        def run():
            def step(block, carry):
                span = pl.ds(pl.multiple_of(block * piece, piece), piece)
                if index is None:
                    product = dot(tiles[place, span, :], window[slot, part])
                else:
                    product = dot(
                        tiles[place, span, index * piece : (index + 1) * piece],
                        window[slot, part, index * piece : (index + 1) * piece, :],
                    )
                if first:
                    acc[part, span, :] = product * scale
                else:
                    acc[part, span, :] += product * scale
                return carry

            lax.fori_loop(0, PIECES, step, 0)

        if condition is None:
            run()
        else:
            pl.when(condition)(run)

    raw_load.wait()
    live = lax.broadcasted_iota(jnp.int32, (rows, half), 0) < count_ref[0, 0]
    basis_load.wait()
    for part in range(2):
        columns = slice(part * half, (part + 1) * half)
        masked = jnp.where(live, raw[:, columns], jnp.zeros((), jnp.bfloat16))
        window[own_slot, part] = masked
        coeffs[me, :, columns] = contract(basis[...], masked).astype(jnp.bfloat16)
    nested_load.wait()
    for part in range(2):
        halves[part] = contract(nested[...], coeffs[me, :, part * half : (part + 1) * half])
    pl.semaphore_wait(barrier, len(peers))

    send_coeff(me, to_above, above)
    send_coeff(me, to_below, below)
    send(halves.at[other], half_in, half_sem.at[0], to_partner)
    for index in range(PIECES - 1):
        send_piece(own_slot, 0, index, own_slot + 4 * column - 2, to_beside)
    send_block(own_slot, 0, core, to_above, above)
    send_block(own_slot, 0, core + 8, to_below, below)
    for part in range(2):
        send_block(own_slot, part, own_slot, to_partner)

    receive(half_in, half_sem.at[0])
    total = halves[core] + half_in[...]
    for part in range(2):
        value = total[:, part * quarter : (part + 1) * quarter]
        partial[part] = value
        quarters[part] = value.astype(jnp.bfloat16)
    for copy in tile_loads:
        copy.wait()
    near(own_slot, 0, first=True)
    send(quarters.at[1 - column], quarter_in, quarter_sem.at[0], to_beside)
    send_piece(own_slot, 0, PIECES - 1, own_slot + 4 * column - 2, to_beside)
    near(own_slot, 1, first=True)
    for part in range(2):
        wait_block(partner_slot, part)
        near(partner_slot, part)

    relay_coeffs(1)
    cross_coeffs(1)
    send_block(own_slot, 1, own_slot + 4 * column - 2, to_beside)
    receive(quarter_in, quarter_sem.at[0])
    sums[level] = (partial[column] + quarter_in[...].astype(jnp.float32)).astype(jnp.bfloat16)
    send_sums = []
    for step in range(1, levels):
        send_sums.append(lax.rem(me + 4 * step, 4 * levels))
    for leaf in send_sums:
        send(sums.at[level], sums.at[level], sum_sem.at[level], {"leaf": leaf})
    send_block(own_slot, 1, core, to_above, above)
    send_block(own_slot, 1, core + 8, to_below, below)

    bridged_slot = jnp.where(core == 0, 1, 8)
    bridged = jnp.logical_or(
        jnp.logical_and(core == 0, below), jnp.logical_and(core == 1, above)
    )
    hand_below = jnp.logical_and(core == 1, below)
    hand_above = jnp.logical_and(core == 0, above)
    far_beside_slot = other + 6 - 4 * column
    far_diagonal_slot = other + 2 + 4 * column

    def hand_neighbours(part):
        send_block(below_slot, part, below_slot, to_partner, hand_below)
        send_block(above_slot, part, above_slot, to_partner, hand_above)

    for index in range(PIECES):
        wait_piece(beside_slot, 0, index)
    send_block(beside_slot, 0, beside_slot, to_partner)
    near(beside_slot, 0)
    wait_block(below_slot, 0, below)
    wait_block(above_slot, 0, above)
    hand_neighbours(0)
    near(below_slot, 0, below)
    near(above_slot, 0, above)

    hand_crossed(1)
    if levels > 2:
        relay_coeffs(2)
        cross_coeffs(2)
    for step in range(1, levels):
        source = lax.rem(level + step, levels)
        receive(sums.at[source], sum_sem.at[source])
    whole = sums[0].astype(jnp.float32)
    for index in range(1, levels):
        whole = whole + sums[index].astype(jnp.float32)
    parents[cluster] = whole.astype(jnp.bfloat16)
    for step in range(1, clusters):
        send(
            parents.at[cluster],
            parents.at[cluster],
            parent_sem.at[cluster],
            {"top": lax.rem(cluster + step, clusters)},
        )
    wait_block(far_beside_slot, 0)
    near(far_beside_slot, 0)
    wait_block(bridged_slot, 0, bridged)
    near(bridged_slot, 0, bridged)

    coupling_load.wait()
    top_load.wait()
    for step in range(1, clusters):
        source = lax.rem(cluster + step, clusters)
        receive(parents.at[source], parent_sem.at[source])
    over = jnp.zeros(parents.shape[1:], jnp.float32)
    for m in range(top.shape[0]):
        over = over + dot(top[m], parents[lax.rem(cluster + 1 + m, clusters)])
    place = 2 * core + column
    fields[place] = over.astype(jnp.bfloat16)
    send(fields.at[place], fields.at[place], field_sem.at[place], to_beside)
    send_block(below_slot, 0, core + 2, to_beside, relay_down)
    send_block(above_slot, 0, core + 6, to_beside, relay_up)

    wait_block(beside_slot, 1)
    for index in range(PIECES):
        send_piece(beside_slot, 1, index, core + 2, to_above, relay_up)
        send_piece(beside_slot, 1, index, core + 6, to_below, relay_down)
    send_block(beside_slot, 1, beside_slot, to_partner)
    near(beside_slot, 1)
    wait_block(below_slot, 1, below)
    wait_block(above_slot, 1, above)
    hand_neighbours(1)
    near(below_slot, 1, below)
    near(above_slot, 1, above)
    if levels > 2:
        hand_crossed(2)
    for hop in range(3, levels):
        relay_coeffs(hop)
        cross_coeffs(hop)
    next_place = 2 * core + 1 - column
    receive(fields.at[next_place], field_sem.at[next_place])
    pair = fields.at[pl.ds(2 * core, 2)]
    send(pair, pair, field_sem.at[4 + core], to_partner)
    wait_block(far_beside_slot, 1)
    near(far_beside_slot, 1)
    wait_block(bridged_slot, 1, bridged)
    near(bridged_slot, 1, bridged)

    wait_block(diagonal_slot, 0, diagonal)
    send_block(diagonal_slot, 0, diagonal_slot, to_partner, diagonal)
    near(diagonal_slot, 0, diagonal)
    wait_block(far_diagonal_slot, 0, diagonal)
    near(far_diagonal_slot, 0, diagonal)
    for hop in range(3, levels):
        hand_crossed(hop)
    for index in range(PIECES):
        wait_piece(diagonal_slot, 1, index, diagonal)
        send_piece(diagonal_slot, 1, index, diagonal_slot, to_partner, diagonal)
        near(diagonal_slot, 1, diagonal, index=index)
        if index > 0:
            wait_piece(far_diagonal_slot, 1, index - 1, diagonal)
            near(far_diagonal_slot, 1, diagonal, index=index - 1)

    for hop in range(1, levels):
        for step in (-hop, hop):
            wait_coeff(partner + 4 * step, handed(step, other))
            wait_coeff(beside + 1 - 2 * core + 4 * step, crossed(step))
    theirs = fields.at[pl.ds(2 * other, 2)]
    receive(theirs, field_sem.at[4 + other])
    field = dot(nested[...], jnp.concatenate([fields[k] for k in range(4)], axis=1))
    for m in range(coupling.shape[0]):
        field = field + dot(coupling[m], coeffs[far_ref[0, 0, m]])
    field_ref[...] = field.astype(jnp.bfloat16)
    wait_piece(far_diagonal_slot, 1, PIECES - 1, diagonal)
    near(far_diagonal_slot, 1, diagonal, index=PIECES - 1)

    for condition, copy in sent:
        if condition is None:
            copy.wait_send()
        else:
            pl.when(condition)(copy.wait_send)


def finish_kernel(count_ref, acc_ref, field_ref, basis_ref, out_ref):
    rows, vecs = out_ref.shape
    half = vecs // 2
    row = lax.broadcasted_iota(jnp.int32, (rows, half), 0) + pl.program_id(0) * rows
    live = row < count_ref[0, 0]
    for part in range(2):
        columns = slice(part * half, (part + 1) * half)
        value = acc_ref[part] + dot(basis_ref[0, 0], field_ref[:, columns])
        out_ref[:, columns] = jnp.where(live, value, 0.0)


def body(
    vectors,
    near_tiles,
    leaf_basis,
    transfer,
    coupling,
    top_coupling,
    near_list,
    far_list,
    row_counts,
):
    leaves = lax.axis_size("leaf")
    clusters = lax.axis_size("top")
    levels = leaves // 4
    rows, vecs = vectors.shape[2:]
    rank = transfer.shape[2]
    half, quarter = vecs // 2, vecs // 4
    smem = pl.BlockSpec(memory_space=pltpu.SMEM)
    vmem = pl.BlockSpec(memory_space=pltpu.VMEM)
    hbm = pl.BlockSpec(memory_space=pltpu.HBM)
    dma = pltpu.SemaphoreType.DMA
    acc, field = pl.pallas_call(
        functools.partial(exchange_kernel, levels, clusters),
        out_shape=(
            jax.ShapeDtypeStruct((2, rows, half), jnp.float32),
            jax.ShapeDtypeStruct((rank, vecs), jnp.bfloat16),
        ),
        in_specs=[smem] * 3 + [hbm] * 6,
        out_specs=(vmem, vmem),
        scratch_shapes=[
            pltpu.VMEM((rows, vecs), jnp.bfloat16),
            pltpu.VMEM(near_tiles.shape[2:], jnp.bfloat16),
            pltpu.VMEM(leaf_basis.shape[2:], jnp.bfloat16),
            pltpu.VMEM(transfer.shape[2:], jnp.bfloat16),
            pltpu.VMEM(coupling.shape[2:], jnp.bfloat16),
            pltpu.VMEM(top_coupling.shape[1:], jnp.bfloat16),
            pltpu.VMEM((SLOTS, 2, rows, half), jnp.bfloat16),
            pltpu.VMEM((leaves, rank, vecs), jnp.bfloat16),
            pltpu.VMEM((2, rank, half), jnp.float32),
            pltpu.VMEM((rank, half), jnp.float32),
            pltpu.VMEM((2, rank, quarter), jnp.bfloat16),
            pltpu.VMEM((2, rank, quarter), jnp.float32),
            pltpu.VMEM((rank, quarter), jnp.bfloat16),
            pltpu.VMEM((levels, rank, quarter), jnp.bfloat16),
            pltpu.VMEM((clusters, rank, quarter), jnp.bfloat16),
            pltpu.VMEM((4, rank, quarter), jnp.bfloat16),
            dma((near_tiles.shape[2],)),
            dma((5,)),
            dma((send_count(levels, clusters),)),
            dma((SLOTS, 2)),
            dma((SLOTS, 2, PIECES)),
            dma((leaves,)),
            dma((1,)),
            dma((1,)),
            dma((levels,)),
            dma((clusters,)),
            dma((6,)),
        ],
        compiler_params=pltpu.CompilerParams(
            collective_id=0, has_side_effects=True, vmem_limit_bytes=62 * 1024 * 1024
        ),
    )(
        near_list,
        far_list,
        row_counts,
        vectors,
        near_tiles,
        leaf_basis,
        transfer,
        coupling,
        top_coupling,
    )
    steps = PIECES
    result = pl.pallas_call(
        finish_kernel,
        out_shape=jax.ShapeDtypeStruct((rows, vecs), jnp.float32),
        grid=(steps,),
        in_specs=[
            smem,
            pl.BlockSpec((2, rows // steps, half), lambda i: (0, i, 0)),
            pl.BlockSpec((rank, vecs), lambda i: (0, 0)),
            pl.BlockSpec((1, 1, rows // steps, rank), lambda i: (0, 0, i, 0)),
        ],
        out_specs=pl.BlockSpec((rows // steps, vecs), lambda i: (i, 0)),
        compiler_params=pltpu.CompilerParams(
            dimension_semantics=("arbitrary",), vmem_limit_bytes=12 * 1024 * 1024
        ),
    )(row_counts, acc, field, leaf_basis)
    return result[None, None]


def solution(mesh):
    in_specs = (
        P("top", "leaf", None, None),
        P("top", "leaf", None, None, None),
        P("top", "leaf", None, None),
        P("top", "leaf", None, None),
        P("top", "leaf", None, None, None),
        P("top", None, None, None),
        P("top", "leaf", None),
        P("top", "leaf", None),
        P("top", "leaf"),
    )
    out_specs = P("top", "leaf", None, None)
    return jax.shard_map(body, mesh=mesh, in_specs=in_specs, out_specs=out_specs, check_vma=False)
```

```python
import functools

import jax
import jax.numpy as jnp
from jax import lax
from jax.experimental import pallas as pl
from jax.experimental.pallas import tpu as pltpu
from jax.sharding import PartitionSpec as P

REACH = 4
SLOTS = 2 * REACH + 2
PIECES = 3


def contract(left, right):
    return lax.dot_general(left, right, (((0,), (0,)), ((), ())), preferred_element_type=jnp.float32)


def dot(left, right):
    return jnp.dot(left, right, preferred_element_type=jnp.float32)


def send_count(levels, clusters):
    return 40 + 12 * levels + clusters


def exchange_kernel(
    levels,
    clusters,
    count_ref,
    near_source,
    far_source,
    vectors_ref,
    tiles_ref,
    basis_ref,
    nested_ref,
    coupling_ref,
    top_ref,
    acc,
    field_ref,
    near_ref,
    far_ref,
    raw,
    tiles,
    basis,
    nested,
    coupling,
    top,
    window,
    coeffs,
    halves,
    half_in,
    quarters,
    partial,
    quarter_in,
    line_out,
    line_in,
    parents,
    fields,
    tile_sem,
    load_sem,
    send_sem,
    block_sem,
    piece_sem,
    coeff_sem,
    half_sem,
    quarter_sem,
    line_sem,
    parent_sem,
    field_sem,
):
    me = lax.axis_index("leaf")
    cluster = lax.axis_index("top")
    core = lax.rem(me, 2)
    column = lax.rem(lax.div(me, 2), 2)
    level = lax.div(me, 4)
    other = 1 - core
    partner = me + 1 - 2 * core
    beside = me + 2 - 4 * column
    above = level < levels - 1
    below = level > 0
    first_column = column == 0
    rows, vecs = raw.shape
    half = vecs // 2
    quarter = vecs // 4
    piece = rows // PIECES
    tile_count = tiles.shape[0]

    def load(source, target, sem):
        return pltpu.make_async_copy(source, target, sem)

    raw_load = load(vectors_ref.at[0, 0], raw, load_sem.at[0])
    basis_load = load(basis_ref.at[0, 0], basis, load_sem.at[1])
    nested_load = load(nested_ref.at[0, 0], nested, load_sem.at[2])
    coupling_load = load(coupling_ref.at[0, 0], coupling, load_sem.at[3])
    top_load = load(top_ref.at[0], top, load_sem.at[4])
    tile_loads = [load(tiles_ref.at[0, 0, k], tiles.at[k], tile_sem.at[k]) for k in range(tile_count)]
    near_load = load(near_source, near_ref, load_sem.at[5])
    far_load = load(far_source, far_ref, load_sem.at[6])

    barrier = pltpu.get_barrier_semaphore()

    def greet(peer):
        pl.semaphore_signal(barrier, inc=1, device_id=peer, device_id_type=pl.DeviceIdType.MESH)

    greet({"leaf": partner})
    greet({"leaf": beside})
    for step in range(1, clusters):
        greet({"top": lax.rem(cluster + step, clusters)})
    pl.when(above)(lambda: greet({"leaf": me + 4}))
    pl.when(below)(lambda: greet({"leaf": me - 4}))
    expected = clusters + 1 + above.astype(jnp.int32) + below.astype(jnp.int32)
    loads = [raw_load, basis_load, nested_load, near_load]
    for copy in loads + tile_loads + [far_load, coupling_load, top_load]:
        copy.start()

    sent = []

    def send(source, target, sem, peer, condition=None):
        copy = pltpu.make_async_remote_copy(
            src_ref=source,
            dst_ref=target,
            send_sem=send_sem.at[len(sent)],
            recv_sem=sem,
            device_id=peer,
            device_id_type=pl.DeviceIdType.MESH,
        )
        sent.append((condition, copy))
        if condition is None:
            copy.start()
        else:
            pl.when(condition)(copy.start)

    def receive(block, sem, condition=None):
        copy = pltpu.make_async_remote_copy(
            src_ref=block,
            dst_ref=block,
            send_sem=send_sem.at[0],
            recv_sem=sem,
            device_id={"leaf": partner},
            device_id_type=pl.DeviceIdType.MESH,
        )
        if condition is None:
            copy.wait_recv()
        else:
            pl.when(condition)(copy.wait_recv)

    to_partner, to_beside = {"leaf": partner}, {"leaf": beside}
    to_above, to_below = {"leaf": me + 4}, {"leaf": me - 4}

    own_slot = REACH + core
    partner_slot = REACH + other
    beside_slot = core + 6 - 4 * column
    diagonal_slot = core + 2 + 4 * column
    below_slot = core
    above_slot = core + 8
    diagonal = jnp.logical_or(
        jnp.logical_and(first_column, below), jnp.logical_and(column == 1, above)
    )
    relay_over = jnp.logical_or(
        jnp.logical_and(column == 1, below), jnp.logical_and(first_column, above)
    )
    relay_up = jnp.logical_and(first_column, above)
    relay_down = jnp.logical_and(column == 1, below)

    def send_block(slot, part, target, peer, condition=None):
        send(window.at[slot, part], window.at[target, part], block_sem.at[target, part], peer, condition)

    def wait_block(slot, part, condition=None):
        receive(window.at[slot, part], block_sem.at[slot, part], condition)

    def span_of(index):
        return pl.ds(index * piece, piece)

    def send_piece(slot, part, index, target, peer, condition=None):
        send(
            window.at[slot, part, span_of(index)],
            window.at[target, part, span_of(index)],
            piece_sem.at[target, part, index],
            peer,
            condition,
        )

    def wait_piece(slot, part, index, condition=None):
        receive(window.at[slot, part, span_of(index)], piece_sem.at[slot, part, index], condition)

    def send_coeff(leaf, peer, condition=None):
        send(coeffs.at[leaf], coeffs.at[leaf], coeff_sem.at[leaf], peer, condition)

    def wait_coeff(leaf, condition=None):
        receive(coeffs.at[leaf], coeff_sem.at[leaf], condition)

    def exists(step):
        return jnp.logical_and(level + step >= 0, level + step < levels)

    def crosses(step, from_first):
        return step <= -1 or step >= 2 if from_first else step >= 1 or step <= -2

    def crossing(step):
        if crosses(step, True) and crosses(step, False):
            return exists(step)
        return jnp.logical_and(exists(step), first_column if crosses(step, True) else column == 1)

    def crossed(step):
        if crosses(step, True) and crosses(step, False):
            return exists(step)
        return jnp.logical_and(exists(step), column == 1 if crosses(step, True) else first_column)

    def handed(step, which):
        if abs(step) >= 2:
            return exists(step)
        return jnp.logical_and(exists(step), which == (1 if step == 1 else 0))

    def relay_coeffs(hop):
        for step in (-hop, hop):
            wait_coeff(me + 4 * step, exists(step))
        if hop + 1 < levels:
            send_coeff(me - 4 * hop, to_above, jnp.logical_and(exists(-hop), above))
            send_coeff(me + 4 * hop, to_below, jnp.logical_and(exists(hop), below))

    def cross_coeffs(hop):
        for step in (-hop, hop):
            send_coeff(me + 4 * step, to_beside, crossing(step))
            send_coeff(me + 4 * step, to_partner, handed(step, core))

    def hand_crossed(hop):
        for step in (-hop, hop):
            wait_coeff(beside + 4 * step, crossed(step))
            send_coeff(beside + 4 * step, to_partner, crossed(step))

    def near(slot, part, condition=None, first=False, index=None):
        offset = slot - REACH - core
        place, hit = 0, 0
        for k in range(tile_count):
            here = near_ref[0, 0, k] == offset
            place = jnp.where(here, k, place)
            hit = jnp.where(here, 1, hit)
        scale = hit.astype(jnp.float32)

        def run():
            if index is None:
                product = dot(tiles[place], window[slot, part]) * scale
            else:
                span = slice(index * piece, (index + 1) * piece)
                product = dot(tiles[place, :, span], window[slot, part, span, :]) * scale
            if first:
                acc[part] = product
            else:
                acc[part] += product

        if condition is None:
            run()
        else:
            pl.when(condition)(run)

    raw_load.wait()
    live = lax.broadcasted_iota(jnp.int32, (rows, half), 0) < count_ref[0, 0]
    basis_load.wait()
    for part in range(2):
        columns = slice(part * half, (part + 1) * half)
        masked = jnp.where(live, raw[:, columns], jnp.zeros((), jnp.bfloat16))
        window[own_slot, part] = masked
        coeffs[me, :, columns] = contract(basis[...], masked).astype(jnp.bfloat16)
    nested_load.wait()
    for part in range(2):
        halves[part] = contract(nested[...], coeffs[me, :, part * half : (part + 1) * half])
    pl.semaphore_wait(barrier, expected)

    own_beside = own_slot + 4 * column - 2
    send_coeff(me, to_above, above)
    send_coeff(me, to_below, below)
    send(halves.at[other], half_in, half_sem.at[0], to_partner)
    for index in range(PIECES - 1):
        send_piece(own_slot, 0, index, own_beside, to_beside)
    send_block(own_slot, 0, core, to_above, above)
    send_block(own_slot, 0, core + 8, to_below, below)
    for part in range(2):
        send_block(own_slot, part, own_slot, to_partner)

    def send_own(index):
        send_piece(own_slot, 1, index, core, to_above, above)
        send_piece(own_slot, 1, index, core + 8, to_below, below)

    receive(half_in, half_sem.at[0])
    total = halves[core] + half_in[...]
    for part in range(2):
        value = total[:, part * quarter : (part + 1) * quarter]
        partial[part] = value
        quarters[part] = value.astype(jnp.bfloat16)
    send(quarters.at[1 - column], quarter_in, quarter_sem.at[0], to_beside)
    send_piece(own_slot, 0, PIECES - 1, own_beside, to_beside)
    for copy in [near_load] + tile_loads:
        copy.wait()
    near(own_slot, 0, first=True)
    near(own_slot, 1, first=True)
    for part in range(2):
        wait_block(partner_slot, part)
        near(partner_slot, part)

    relay_coeffs(1)
    cross_coeffs(1)
    send_block(own_slot, 1, own_beside, to_beside)
    receive(quarter_in, quarter_sem.at[0])
    partial[column] += quarter_in[...].astype(jnp.float32)

    def line(turn):
        for way, at, step in ((0, turn - 1, 4), (1, levels - turn, -4)):
            here = level == at
            if turn > 1:
                receive(line_in.at[way], line_sem.at[way], here)
            if turn < levels:

                @pl.when(here)
                def _(way=way):
                    value = partial[column]
                    if turn > 1:
                        value = value + line_in[way].astype(jnp.float32)
                    line_out[way] = value.astype(jnp.bfloat16)

                send(line_out.at[way], line_in.at[way], line_sem.at[way], {"leaf": me + step}, here)

    line(1)
    send_own(0)

    bridged_slot = jnp.where(core == 0, 1, 8)
    bridged = jnp.logical_or(
        jnp.logical_and(core == 0, below), jnp.logical_and(core == 1, above)
    )
    hand_below = jnp.logical_and(core == 1, below)
    hand_above = jnp.logical_and(core == 0, above)
    far_beside_slot = other + 6 - 4 * column
    far_diagonal_slot = other + 2 + 4 * column

    def hand_neighbours(part):
        send_block(below_slot, part, below_slot, to_partner, hand_below)
        send_block(above_slot, part, above_slot, to_partner, hand_above)

    def send_over(index):
        send_piece(below_slot, 0, index, core + 2, to_beside, relay_down)
        send_piece(above_slot, 0, index, core + 6, to_beside, relay_up)

    for index in range(PIECES):
        wait_piece(beside_slot, 0, index)
    send_block(beside_slot, 0, beside_slot, to_partner)
    near(beside_slot, 0)
    wait_block(below_slot, 0, below)
    wait_block(above_slot, 0, above)
    hand_neighbours(0)
    near(below_slot, 0, below)
    near(above_slot, 0, above)
    line(2)
    send_own(1)

    hand_crossed(1)
    if levels > 2:
        relay_coeffs(2)
        cross_coeffs(2)
    send_over(0)
    send_over(1)
    wait_block(far_beside_slot, 0)
    near(far_beside_slot, 0)
    wait_block(bridged_slot, 0, bridged)
    near(bridged_slot, 0, bridged)
    for turn in range(3, levels):
        line(turn)
    send_own(2)

    wait_block(beside_slot, 1)
    for index in range(PIECES):
        send_piece(beside_slot, 1, index, core + 2, to_above, relay_up)
        send_piece(beside_slot, 1, index, core + 6, to_below, relay_down)
    send_block(beside_slot, 1, beside_slot, to_partner)
    near(beside_slot, 1)
    if levels > 2:
        line(levels)
    whole = partial[column]
    for way, condition in ((0, below), (1, above)):
        whole = whole + jnp.where(condition, line_in[way].astype(jnp.float32), 0.0)
    parents[cluster] = whole.astype(jnp.bfloat16)
    for step in range(1, clusters):
        send(
            parents.at[cluster],
            parents.at[cluster],
            parent_sem.at[cluster],
            {"top": lax.rem(cluster + step, clusters)},
        )
    wait_block(far_beside_slot, 1)
    near(far_beside_slot, 1)
    coupling_load.wait()
    top_load.wait()
    for step in range(1, clusters):
        source = lax.rem(cluster + step, clusters)
        receive(parents.at[source], parent_sem.at[source])
    over = jnp.zeros(parents.shape[1:], jnp.float32)
    for m in range(top.shape[0]):
        over = over + dot(top[m], parents[lax.rem(cluster + 1 + m, clusters)])
    place = 2 * core + column
    fields[place] = over.astype(jnp.bfloat16)
    send(fields.at[place], fields.at[place], field_sem.at[place], to_beside)
    send_over(2)
    if levels > 2:
        hand_crossed(2)
    for hop in range(3, levels):
        relay_coeffs(hop)
        cross_coeffs(hop)
    for index in range(PIECES):
        wait_piece(below_slot, 1, index, below)
        wait_piece(above_slot, 1, index, above)
    hand_neighbours(1)
    near(below_slot, 1, below)
    near(above_slot, 1, above)
    next_place = 2 * core + 1 - column
    receive(fields.at[next_place], field_sem.at[next_place])
    pair = fields.at[pl.ds(2 * core, 2)]
    send(pair, pair, field_sem.at[4 + core], to_partner)

    def hand_diagonal(part, index):
        wait_piece(diagonal_slot, part, index, diagonal)
        send_piece(diagonal_slot, part, index, diagonal_slot, to_partner, diagonal)

    def far_diagonal(index):
        wait_piece(far_diagonal_slot, 1, index, diagonal)
        near(far_diagonal_slot, 1, diagonal, index=index)

    for index in range(PIECES - 1):
        hand_diagonal(0, index)
    wait_block(bridged_slot, 1, bridged)
    near(bridged_slot, 1, bridged)
    hand_diagonal(1, 0)
    near(diagonal_slot, 1, diagonal, index=0)
    hand_diagonal(0, PIECES - 1)
    near(diagonal_slot, 0, diagonal)
    hand_diagonal(1, 1)
    near(diagonal_slot, 1, diagonal, index=1)
    for index in range(PIECES):
        wait_piece(far_diagonal_slot, 0, index, diagonal)
    near(far_diagonal_slot, 0, diagonal)
    for hop in range(3, levels):
        hand_crossed(hop)
    far_diagonal(0)
    far_diagonal(1)

    for hop in range(1, levels):
        for step in (-hop, hop):
            wait_coeff(partner + 4 * step, handed(step, other))
            wait_coeff(beside + 1 - 2 * core + 4 * step, crossed(step))
    theirs = fields.at[pl.ds(2 * other, 2)]
    receive(theirs, field_sem.at[4 + other])
    far_load.wait()
    field = dot(nested[...], jnp.concatenate([fields[k] for k in range(4)], axis=1))
    for m in range(coupling.shape[0]):
        field = field + dot(coupling[m], coeffs[far_ref[0, 0, m]])
    field_ref[...] = field.astype(jnp.bfloat16)
    hand_diagonal(1, 2)
    near(diagonal_slot, 1, diagonal, index=2)
    far_diagonal(2)

    for condition, copy in sent:
        if condition is None:
            copy.wait_send()
        else:
            pl.when(condition)(copy.wait_send)


def finish_kernel(count_ref, acc_ref, field_ref, basis_ref, out_ref, staged, sem):
    steps, rows = staged.shape[:2]
    half = acc_ref.shape[2]
    copies = []
    for step in range(steps):
        span = slice(step * rows, (step + 1) * rows)
        live = lax.broadcasted_iota(jnp.int32, (rows, half), 0) < count_ref[0, 0] - step * rows
        for part in range(2):
            columns = slice(part * half, (part + 1) * half)
            value = acc_ref[part, span] + dot(basis_ref[0, 0, span], field_ref[:, columns])
            staged[step, :, columns] = jnp.where(live, value, 0.0)
        copy = pltpu.make_async_copy(staged.at[step], out_ref.at[span], sem.at[step])
        copy.start()
        copies.append(copy)
    for copy in copies:
        copy.wait()


def body(
    vectors,
    near_tiles,
    leaf_basis,
    transfer,
    coupling,
    top_coupling,
    near_list,
    far_list,
    row_counts,
):
    leaves = lax.axis_size("leaf")
    clusters = lax.axis_size("top")
    levels = leaves // 4
    rows, vecs = vectors.shape[2:]
    rank = transfer.shape[2]
    half, quarter = vecs // 2, vecs // 4
    smem = pl.BlockSpec(memory_space=pltpu.SMEM)
    vmem = pl.BlockSpec(memory_space=pltpu.VMEM)
    hbm = pl.BlockSpec(memory_space=pltpu.HBM)
    dma = pltpu.SemaphoreType.DMA
    acc, field = pl.pallas_call(
        functools.partial(exchange_kernel, levels, clusters),
        out_shape=(
            jax.ShapeDtypeStruct((2, rows, half), jnp.float32),
            jax.ShapeDtypeStruct((rank, vecs), jnp.bfloat16),
        ),
        in_specs=[smem] + [hbm] * 8,
        out_specs=(vmem, vmem),
        scratch_shapes=[
            pltpu.SMEM(near_list.shape, jnp.int32),
            pltpu.SMEM(far_list.shape, jnp.int32),
            pltpu.VMEM((rows, vecs), jnp.bfloat16),
            pltpu.VMEM(near_tiles.shape[2:], jnp.bfloat16),
            pltpu.VMEM(leaf_basis.shape[2:], jnp.bfloat16),
            pltpu.VMEM(transfer.shape[2:], jnp.bfloat16),
            pltpu.VMEM(coupling.shape[2:], jnp.bfloat16),
            pltpu.VMEM(top_coupling.shape[1:], jnp.bfloat16),
            pltpu.VMEM((SLOTS, 2, rows, half), jnp.bfloat16),
            pltpu.VMEM((leaves, rank, vecs), jnp.bfloat16),
            pltpu.VMEM((2, rank, half), jnp.float32),
            pltpu.VMEM((rank, half), jnp.float32),
            pltpu.VMEM((2, rank, quarter), jnp.bfloat16),
            pltpu.VMEM((2, rank, quarter), jnp.float32),
            pltpu.VMEM((rank, quarter), jnp.bfloat16),
            pltpu.VMEM((2, rank, quarter), jnp.bfloat16),
            pltpu.VMEM((2, rank, quarter), jnp.bfloat16),
            pltpu.VMEM((clusters, rank, quarter), jnp.bfloat16),
            pltpu.VMEM((4, rank, quarter), jnp.bfloat16),
            dma((near_tiles.shape[2],)),
            dma((7,)),
            dma((send_count(levels, clusters),)),
            dma((SLOTS, 2)),
            dma((SLOTS, 2, PIECES)),
            dma((leaves,)),
            dma((1,)),
            dma((1,)),
            dma((2,)),
            dma((clusters,)),
            dma((6,)),
        ],
        compiler_params=pltpu.CompilerParams(
            collective_id=0, has_side_effects=True, vmem_limit_bytes=48 * 1024 * 1024
        ),
    )(
        row_counts,
        *[
            pltpu.with_memory_space_constraint(array, pltpu.HBM)
            for array in (
                near_list,
                far_list,
                vectors,
                near_tiles,
                leaf_basis,
                transfer,
                coupling,
                top_coupling,
            )
        ],
    )
    result = pl.pallas_call(
        finish_kernel,
        out_shape=jax.ShapeDtypeStruct((rows, vecs), jnp.float32),
        in_specs=[smem, vmem, vmem, vmem],
        out_specs=pl.BlockSpec(memory_space=pl.ANY),
        scratch_shapes=[
            pltpu.VMEM((PIECES, rows // PIECES, vecs), jnp.float32),
            dma((PIECES,)),
        ],
        compiler_params=pltpu.CompilerParams(vmem_limit_bytes=8 * 1024 * 1024),
    )(row_counts, acc, field, leaf_basis)
    return result[None, None]


def solution(mesh):
    in_specs = (
        P("top", "leaf", None, None),
        P("top", "leaf", None, None, None),
        P("top", "leaf", None, None),
        P("top", "leaf", None, None),
        P("top", "leaf", None, None, None),
        P("top", None, None, None),
        P("top", "leaf", None),
        P("top", "leaf", None),
        P("top", "leaf"),
    )
    out_specs = P("top", "leaf", None, None)
    return jax.shard_map(body, mesh=mesh, in_specs=in_specs, out_specs=out_specs, check_vma=False)
```

```python
import functools

import jax
import jax.numpy as jnp
from jax import lax
from jax.experimental import pallas as pl
from jax.experimental.pallas import tpu as pltpu
from jax.sharding import PartitionSpec as P

REACH = 4
SLOTS = 2 * REACH + 2
PIECES = 3


def contract(left, right):
    return lax.dot_general(left, right, (((0,), (0,)), ((), ())), preferred_element_type=jnp.float32)


def dot(left, right):
    return jnp.dot(left, right, preferred_element_type=jnp.float32)


def send_count(levels, clusters):
    return 40 + 12 * levels + clusters


def exchange_kernel(
    levels,
    clusters,
    count_ref,
    near_source,
    far_source,
    vectors_ref,
    tiles_ref,
    basis_ref,
    nested_ref,
    coupling_ref,
    top_ref,
    acc,
    near_ref,
    far_ref,
    raw,
    tiles,
    basis,
    nested,
    coupling,
    top,
    window,
    coeffs,
    halves,
    half_in,
    partial,
    quarter_in,
    line_out,
    line_in,
    parents,
    fields,
    tile_sem,
    load_sem,
    send_sem,
    block_sem,
    piece_sem,
    coeff_sem,
    half_sem,
    quarter_sem,
    line_sem,
    parent_sem,
    field_sem,
):
    me = lax.axis_index("leaf")
    cluster = lax.axis_index("top")
    core = lax.rem(me, 2)
    column = lax.rem(lax.div(me, 2), 2)
    level = lax.div(me, 4)
    other = 1 - core
    partner = me + 1 - 2 * core
    beside = me + 2 - 4 * column
    above = level < levels - 1
    below = level > 0
    first_column = column == 0
    rows, half = raw.shape[1:]
    vecs = 2 * half
    quarter = half // 2
    piece = rows // PIECES
    tile_count = tiles.shape[0]

    def load(source, target, sem):
        return pltpu.make_async_copy(source, target, sem)

    raw_loads = [
        load(vectors_ref.at[0, 0, :, pl.ds(part * half, half)], raw.at[part], load_sem.at[part])
        for part in range(2)
    ]
    basis_load = load(basis_ref.at[0, 0], basis, load_sem.at[2])
    nested_load = load(nested_ref.at[0, 0], nested, load_sem.at[7])
    coupling_load = load(coupling_ref.at[0, 0], coupling, load_sem.at[3])
    top_load = load(top_ref.at[0], top, load_sem.at[4])
    tile_loads = [load(tiles_ref.at[0, 0, k], tiles.at[k], tile_sem.at[k]) for k in range(tile_count)]
    near_load = load(near_source, near_ref, load_sem.at[5])
    far_load = load(far_source, far_ref, load_sem.at[6])

    barrier = pltpu.get_barrier_semaphore()

    def greet(peer):
        pl.semaphore_signal(barrier, inc=1, device_id=peer, device_id_type=pl.DeviceIdType.MESH)

    greet({"leaf": partner})
    greet({"leaf": beside})
    for step in range(1, clusters):
        greet({"top": lax.rem(cluster + step, clusters)})
    pl.when(above)(lambda: greet({"leaf": me + 4}))
    pl.when(below)(lambda: greet({"leaf": me - 4}))
    expected = clusters + 1 + above.astype(jnp.int32) + below.astype(jnp.int32)
    for copy in raw_loads + [basis_load, nested_load, near_load]:
        copy.start()

    sent = []

    def send(source, target, sem, peer, condition=None):
        copy = pltpu.make_async_remote_copy(
            src_ref=source,
            dst_ref=target,
            send_sem=send_sem.at[len(sent)],
            recv_sem=sem,
            device_id=peer,
            device_id_type=pl.DeviceIdType.MESH,
        )
        sent.append((condition, copy))
        if condition is None:
            copy.start()
        else:
            pl.when(condition)(copy.start)

    def receive(block, sem, condition=None):
        copy = pltpu.make_async_remote_copy(
            src_ref=block,
            dst_ref=block,
            send_sem=send_sem.at[0],
            recv_sem=sem,
            device_id={"leaf": partner},
            device_id_type=pl.DeviceIdType.MESH,
        )
        if condition is None:
            copy.wait_recv()
        else:
            pl.when(condition)(copy.wait_recv)

    to_partner, to_beside = {"leaf": partner}, {"leaf": beside}
    to_above, to_below = {"leaf": me + 4}, {"leaf": me - 4}

    own_slot = REACH + core
    partner_slot = REACH + other
    beside_slot = core + 6 - 4 * column
    diagonal_slot = core + 2 + 4 * column
    below_slot = core
    above_slot = core + 8
    diagonal = jnp.logical_or(
        jnp.logical_and(first_column, below), jnp.logical_and(column == 1, above)
    )
    relay_over = jnp.logical_or(
        jnp.logical_and(column == 1, below), jnp.logical_and(first_column, above)
    )
    relay_up = jnp.logical_and(first_column, above)
    relay_down = jnp.logical_and(column == 1, below)

    def send_block(slot, part, target, peer, condition=None):
        send(window.at[slot, part], window.at[target, part], block_sem.at[target, part], peer, condition)

    def wait_block(slot, part, condition=None):
        receive(window.at[slot, part], block_sem.at[slot, part], condition)

    def span_of(index):
        return pl.ds(index * piece, piece)

    def send_piece(slot, part, index, target, peer, condition=None):
        send(
            window.at[slot, part, span_of(index)],
            window.at[target, part, span_of(index)],
            piece_sem.at[target, part, index],
            peer,
            condition,
        )

    def wait_piece(slot, part, index, condition=None):
        receive(window.at[slot, part, span_of(index)], piece_sem.at[slot, part, index], condition)

    def send_coeff(leaf, peer, condition=None):
        send(coeffs.at[leaf], coeffs.at[leaf], coeff_sem.at[leaf], peer, condition)

    def wait_coeff(leaf, condition=None):
        receive(coeffs.at[leaf], coeff_sem.at[leaf], condition)

    def exists(step):
        return jnp.logical_and(level + step >= 0, level + step < levels)

    def crosses(step, from_first):
        return step <= -1 or step >= 2 if from_first else step >= 1 or step <= -2

    def crossing(step):
        if crosses(step, True) and crosses(step, False):
            return exists(step)
        return jnp.logical_and(exists(step), first_column if crosses(step, True) else column == 1)

    def crossed(step):
        if crosses(step, True) and crosses(step, False):
            return exists(step)
        return jnp.logical_and(exists(step), column == 1 if crosses(step, True) else first_column)

    def handed(step, which):
        if abs(step) >= 2:
            return exists(step)
        return jnp.logical_and(exists(step), which == (1 if step == 1 else 0))

    def relay_coeffs(hop):
        for step in (-hop, hop):
            wait_coeff(me + 4 * step, exists(step))
        if hop + 1 < levels:
            send_coeff(me - 4 * hop, to_above, jnp.logical_and(exists(-hop), above))
            send_coeff(me + 4 * hop, to_below, jnp.logical_and(exists(hop), below))

    def cross_coeffs(hop):
        for step in (-hop, hop):
            send_coeff(me + 4 * step, to_beside, crossing(step))
            send_coeff(me + 4 * step, to_partner, handed(step, core))

    def hand_crossed(hop):
        for step in (-hop, hop):
            wait_coeff(beside + 4 * step, crossed(step))
            send_coeff(beside + 4 * step, to_partner, crossed(step))

    def near(slot, part, condition=None, first=False, index=None):
        offset = slot - REACH - core
        place, hit = 0, 0
        for k in range(tile_count):
            here = near_ref[0, 0, k] == offset
            place = jnp.where(here, k, place)
            hit = jnp.where(here, 1, hit)
        scale = hit.astype(jnp.float32)

        def run():
            if index is None:
                product = dot(tiles[place], window[slot, part]) * scale
            else:
                span = slice(index * piece, (index + 1) * piece)
                product = dot(tiles[place, :, span], window[slot, part, span, :]) * scale
            if first:
                acc[part] = product
            else:
                acc[part] += product

        if condition is None:
            run()
        else:
            pl.when(condition)(run)

    own_beside = own_slot + 4 * column - 2

    def send_own(part, index):
        send_piece(own_slot, part, index, core, to_above, above)
        send_piece(own_slot, part, index, core + 8, to_below, below)

    live = lax.broadcasted_iota(jnp.int32, (rows, half), 0) < count_ref[0, 0]

    def mask(part):
        raw_loads[part].wait()
        window[own_slot, part] = jnp.where(live, raw[part], jnp.zeros((), jnp.bfloat16))

    mask(0)
    pl.semaphore_wait(barrier, expected)
    for index in range(PIECES - 1):
        send_piece(own_slot, 0, index, own_beside, to_beside)
    send_own(0, 0)
    mask(1)
    basis_load.wait()
    for part in range(2):
        product = contract(basis[...], window[own_slot, part])
        coeffs[me, :, part * half : (part + 1) * half] = product.astype(jnp.bfloat16)
    nested_load.wait()
    for part in range(2):
        halves[part] = contract(nested[...], coeffs[me, :, part * half : (part + 1) * half])
    send_coeff(me, to_above, above)
    send_coeff(me, to_below, below)
    for index in range(1, PIECES):
        send_own(0, index)
    send(halves.at[other], half_in, half_sem.at[0], to_partner)
    for part in range(2):
        send_block(own_slot, part, own_slot, to_partner)
    for copy in tile_loads + [far_load, coupling_load, top_load]:
        copy.start()

    receive(half_in, half_sem.at[0])
    total = halves[core] + half_in[...]
    for part in range(2):
        partial[part] = total[:, part * quarter : (part + 1) * quarter]
    send(partial.at[1 - column], quarter_in, quarter_sem.at[0], to_beside)
    send_piece(own_slot, 0, PIECES - 1, own_beside, to_beside)
    for copy in [near_load] + tile_loads:
        copy.wait()
    near(own_slot, 0, first=True)
    near(own_slot, 1, first=True)
    for part in range(2):
        wait_block(partner_slot, part)
        near(partner_slot, part)

    relay_coeffs(1)
    cross_coeffs(1)
    send_block(own_slot, 1, own_beside, to_beside)
    receive(quarter_in, quarter_sem.at[0])
    partial[column] += quarter_in[...]

    def line(turn):
        for way, at, step in ((0, turn - 1, 4), (1, levels - turn, -4)):
            here = level == at
            if turn > 1:
                receive(line_in.at[way], line_sem.at[way], here)
            if turn < levels:

                @pl.when(here)
                def _(way=way):
                    value = partial[column]
                    if turn > 1:
                        value = value + line_in[way]
                    line_out[way] = value

                send(line_out.at[way], line_in.at[way], line_sem.at[way], {"leaf": me + step}, here)

    line(1)
    send_own(1, 0)

    bridged_slot = jnp.where(core == 0, 1, 8)
    bridged = jnp.logical_or(
        jnp.logical_and(core == 0, below), jnp.logical_and(core == 1, above)
    )
    hand_below = jnp.logical_and(core == 1, below)
    hand_above = jnp.logical_and(core == 0, above)
    far_beside_slot = other + 6 - 4 * column
    far_diagonal_slot = other + 2 + 4 * column

    def hand_neighbours(part):
        send_block(below_slot, part, below_slot, to_partner, hand_below)
        send_block(above_slot, part, above_slot, to_partner, hand_above)

    def send_over(index):
        send_piece(below_slot, 0, index, core + 2, to_beside, relay_down)
        send_piece(above_slot, 0, index, core + 6, to_beside, relay_up)

    for index in range(PIECES):
        wait_piece(beside_slot, 0, index)
    send_block(beside_slot, 0, beside_slot, to_partner)
    near(beside_slot, 0)
    for index in range(PIECES):
        wait_piece(below_slot, 0, index, below)
        wait_piece(above_slot, 0, index, above)
    hand_neighbours(0)
    near(below_slot, 0, below)
    near(above_slot, 0, above)
    line(2)
    send_own(1, 1)

    hand_crossed(1)
    if levels > 2:
        relay_coeffs(2)
        cross_coeffs(2)
    send_over(0)
    send_over(1)
    wait_block(far_beside_slot, 0)
    near(far_beside_slot, 0)
    wait_block(bridged_slot, 0, bridged)
    near(bridged_slot, 0, bridged)
    for turn in range(3, levels):
        line(turn)
    send_own(1, 2)

    wait_block(beside_slot, 1)
    for index in range(PIECES):
        send_piece(beside_slot, 1, index, core + 2, to_above, relay_up)
        send_piece(beside_slot, 1, index, core + 6, to_below, relay_down)
    send_block(beside_slot, 1, beside_slot, to_partner)
    near(beside_slot, 1)
    if levels > 2:
        line(levels)
    whole = partial[column]
    for way, condition in ((0, below), (1, above)):
        whole = whole + jnp.where(condition, line_in[way], 0.0)
    parents[cluster] = whole.astype(jnp.bfloat16)
    for step in range(1, clusters):
        send(
            parents.at[cluster],
            parents.at[cluster],
            parent_sem.at[cluster],
            {"top": lax.rem(cluster + step, clusters)},
        )
    wait_block(far_beside_slot, 1)
    near(far_beside_slot, 1)
    coupling_load.wait()
    top_load.wait()
    for step in range(1, clusters):
        source = lax.rem(cluster + step, clusters)
        receive(parents.at[source], parent_sem.at[source])
    over = jnp.zeros(parents.shape[1:], jnp.float32)
    for m in range(top.shape[0]):
        over = over + dot(top[m], parents[lax.rem(cluster + 1 + m, clusters)])
    place = 2 * core + column
    fields[place] = over.astype(jnp.bfloat16)
    send(fields.at[place], fields.at[place], field_sem.at[place], to_beside)
    send_over(2)
    if levels > 2:
        hand_crossed(2)
    for hop in range(3, levels):
        relay_coeffs(hop)
        cross_coeffs(hop)
    for index in range(PIECES):
        wait_piece(below_slot, 1, index, below)
        wait_piece(above_slot, 1, index, above)
    hand_neighbours(1)
    near(below_slot, 1, below)
    near(above_slot, 1, above)
    next_place = 2 * core + 1 - column
    receive(fields.at[next_place], field_sem.at[next_place])
    pair = fields.at[pl.ds(2 * core, 2)]
    send(pair, pair, field_sem.at[4 + core], to_partner)

    def hand_diagonal(part, index):
        wait_piece(diagonal_slot, part, index, diagonal)
        send_piece(diagonal_slot, part, index, diagonal_slot, to_partner, diagonal)

    def far_diagonal(index):
        wait_piece(far_diagonal_slot, 1, index, diagonal)
        near(far_diagonal_slot, 1, diagonal, index=index)

    for index in range(PIECES - 1):
        hand_diagonal(0, index)
    wait_block(bridged_slot, 1, bridged)
    near(bridged_slot, 1, bridged)
    hand_diagonal(1, 0)
    near(diagonal_slot, 1, diagonal, index=0)
    hand_diagonal(0, PIECES - 1)
    near(diagonal_slot, 0, diagonal)
    hand_diagonal(1, 1)
    near(diagonal_slot, 1, diagonal, index=1)
    for index in range(PIECES):
        wait_piece(far_diagonal_slot, 0, index, diagonal)
    near(far_diagonal_slot, 0, diagonal)
    for hop in range(3, levels):
        hand_crossed(hop)
    far_diagonal(0)
    far_diagonal(1)

    for hop in range(1, levels):
        for step in (-hop, hop):
            wait_coeff(partner + 4 * step, handed(step, other))
            wait_coeff(beside + 1 - 2 * core + 4 * step, crossed(step))
    theirs = fields.at[pl.ds(2 * other, 2)]
    receive(theirs, field_sem.at[4 + other])
    far_load.wait()
    field = dot(nested[...], jnp.concatenate([fields[k] for k in range(4)], axis=1))
    for m in range(coupling.shape[0]):
        field = field + dot(coupling[m], coeffs[far_ref[0, 0, m]])
    field = field.astype(jnp.bfloat16)
    for part in range(2):
        acc[part] += dot(basis[...], field[:, part * half : (part + 1) * half])
    hand_diagonal(1, 2)
    near(diagonal_slot, 1, diagonal, index=2)
    far_diagonal(2)

    for condition, copy in sent:
        if condition is None:
            copy.wait_send()
        else:
            pl.when(condition)(copy.wait_send)


def finish_kernel(count_ref, acc_ref, out_ref, staged, sem):
    steps, rows = staged.shape[:2]
    half = acc_ref.shape[2]
    copies = []
    for step in range(steps):
        span = slice(step * rows, (step + 1) * rows)
        live = lax.broadcasted_iota(jnp.int32, (rows, half), 0) < count_ref[0, 0] - step * rows
        for part in range(2):
            columns = slice(part * half, (part + 1) * half)
            staged[step, :, columns] = jnp.where(live, acc_ref[part, span], 0.0)
        copy = pltpu.make_async_copy(staged.at[step], out_ref.at[span], sem.at[step])
        copy.start()
        copies.append(copy)
    for copy in copies:
        copy.wait()


def body(
    vectors,
    near_tiles,
    leaf_basis,
    transfer,
    coupling,
    top_coupling,
    near_list,
    far_list,
    row_counts,
):
    leaves = lax.axis_size("leaf")
    clusters = lax.axis_size("top")
    levels = leaves // 4
    rows, vecs = vectors.shape[2:]
    rank = transfer.shape[2]
    half, quarter = vecs // 2, vecs // 4
    smem = pl.BlockSpec(memory_space=pltpu.SMEM)
    vmem = pl.BlockSpec(memory_space=pltpu.VMEM)
    hbm = pl.BlockSpec(memory_space=pltpu.HBM)
    dma = pltpu.SemaphoreType.DMA
    acc = pl.pallas_call(
        functools.partial(exchange_kernel, levels, clusters),
        out_shape=jax.ShapeDtypeStruct((2, rows, half), jnp.float32),
        in_specs=[smem] + [hbm] * 8,
        out_specs=vmem,
        scratch_shapes=[
            pltpu.SMEM(near_list.shape, jnp.int32),
            pltpu.SMEM(far_list.shape, jnp.int32),
            pltpu.VMEM((2, rows, half), jnp.bfloat16),
            pltpu.VMEM(near_tiles.shape[2:], jnp.bfloat16),
            pltpu.VMEM(leaf_basis.shape[2:], jnp.bfloat16),
            pltpu.VMEM(transfer.shape[2:], jnp.bfloat16),
            pltpu.VMEM(coupling.shape[2:], jnp.bfloat16),
            pltpu.VMEM(top_coupling.shape[1:], jnp.bfloat16),
            pltpu.VMEM((SLOTS, 2, rows, half), jnp.bfloat16),
            pltpu.VMEM((leaves, rank, vecs), jnp.bfloat16),
            pltpu.VMEM((2, rank, half), jnp.float32),
            pltpu.VMEM((rank, half), jnp.float32),
            pltpu.VMEM((2, rank, quarter), jnp.float32),
            pltpu.VMEM((rank, quarter), jnp.float32),
            pltpu.VMEM((2, rank, quarter), jnp.float32),
            pltpu.VMEM((2, rank, quarter), jnp.float32),
            pltpu.VMEM((clusters, rank, quarter), jnp.bfloat16),
            pltpu.VMEM((4, rank, quarter), jnp.bfloat16),
            dma((near_tiles.shape[2],)),
            dma((8,)),
            dma((send_count(levels, clusters),)),
            dma((SLOTS, 2)),
            dma((SLOTS, 2, PIECES)),
            dma((leaves,)),
            dma((1,)),
            dma((1,)),
            dma((2,)),
            dma((clusters,)),
            dma((6,)),
        ],
        compiler_params=pltpu.CompilerParams(
            collective_id=0, has_side_effects=True, vmem_limit_bytes=48 * 1024 * 1024
        ),
    )(
        row_counts,
        *[
            pltpu.with_memory_space_constraint(array, pltpu.HBM)
            for array in (
                near_list,
                far_list,
                vectors,
                near_tiles,
                leaf_basis,
                transfer,
                coupling,
                top_coupling,
            )
        ],
    )
    result = pl.pallas_call(
        finish_kernel,
        out_shape=jax.ShapeDtypeStruct((rows, vecs), jnp.float32),
        in_specs=[smem, vmem],
        out_specs=pl.BlockSpec(memory_space=pl.ANY),
        scratch_shapes=[
            pltpu.VMEM((PIECES, rows // PIECES, vecs), jnp.float32),
            dma((PIECES,)),
        ],
        compiler_params=pltpu.CompilerParams(vmem_limit_bytes=8 * 1024 * 1024),
    )(row_counts, acc)
    return result[None, None]


def solution(mesh):
    in_specs = (
        P("top", "leaf", None, None),
        P("top", "leaf", None, None, None),
        P("top", "leaf", None, None),
        P("top", "leaf", None, None),
        P("top", "leaf", None, None, None),
        P("top", None, None, None),
        P("top", "leaf", None),
        P("top", "leaf", None),
        P("top", "leaf"),
    )
    out_specs = P("top", "leaf", None, None)
    return jax.shard_map(body, mesh=mesh, in_specs=in_specs, out_specs=out_specs, check_vma=False)
```

```python
import functools

import jax
import jax.numpy as jnp
from jax import lax
from jax.experimental import pallas as pl
from jax.experimental.pallas import tpu as pltpu
from jax.sharding import PartitionSpec as P

REACH = 4
SLOTS = 2 * REACH + 2
PIECES = 3
SPANS = ((0, 1), (1, 3), (3, 5), (5, 6))
BESIDE, BELOW, ABOVE, PARTNER, FAR_BESIDE, BRIDGED, DIAGONAL, FAR_DIAGONAL = 0, 2, 4, 6, 8, 10, 12, 15
SPAN, FAR_SPAN = 16, 16 + len(SPANS)
ARRIVALS = FAR_SPAN + len(SPANS)
(
    TO_BESIDE,
    TO_ABOVE,
    TO_BELOW,
    TO_PARTNER,
    OVER,
    OVER_SPAN,
    ALONG,
    HAND_BESIDE,
    HAND_COLUMN,
    HAND_DIAGONAL,
    COEFF_ABOVE,
    COEFF_BELOW,
    COEFF_BESIDE,
    COEFF_PARTNER,
    HALF,
    QUARTER,
    LINE,
    FIELD,
    FIELD_PAIR,
    PARENT,
) = range(20)


def contract(left, right):
    return lax.dot_general(left, right, (((0,), (0,)), ((), ())), preferred_element_type=jnp.float32)


def dot(left, right):
    return jnp.dot(left, right, preferred_element_type=jnp.float32)


def exchange_kernel(
    levels,
    clusters,
    count_ref,
    near_source,
    far_source,
    vectors_ref,
    tiles_ref,
    basis_ref,
    nested_ref,
    coupling_ref,
    top_ref,
    acc,
    near_ref,
    far_ref,
    raw,
    tiles,
    basis,
    nested,
    coupling,
    top,
    window,
    coeffs,
    halves,
    half_in,
    partial,
    quarter_in,
    line_out,
    line_in,
    parents,
    fields,
    load_sem,
    send_sem,
    block_sem,
    coeff_sem,
    half_sem,
    quarter_sem,
    line_sem,
    parent_sem,
    field_sem,
):
    me = lax.axis_index("leaf")
    cluster = lax.axis_index("top")
    core = lax.rem(me, 2)
    column = lax.rem(lax.div(me, 2), 2)
    level = lax.div(me, 4)
    other = 1 - core
    partner = me + 1 - 2 * core
    beside = me + 2 - 4 * column
    above = level < levels - 1
    below = level > 0
    first_column = column == 0
    rows, half = raw.shape[1:]
    vecs = 2 * half
    quarter = half // 2
    sixth = rows // 6
    piece = rows // PIECES
    tile_count = tiles.shape[0]

    def load(source, target, sem):
        return pltpu.make_async_copy(source, target, sem)

    raw_loads = [
        load(vectors_ref.at[0, 0, :, pl.ds(part * half, half)], raw.at[part], load_sem.at[part])
        for part in range(2)
    ]
    basis_load = load(basis_ref.at[0, 0], basis, load_sem.at[2])
    nested_load = load(nested_ref.at[0, 0], nested, load_sem.at[7])
    coupling_load = load(coupling_ref.at[0, 0], coupling, load_sem.at[3])
    top_load = load(top_ref.at[0], top, load_sem.at[4])
    tile_loads = [load(tiles_ref.at[0, 0, k], tiles.at[k], load_sem.at[8]) for k in range(tile_count)]
    all_tiles = load(tiles_ref.at[0, 0], tiles, load_sem.at[8])
    near_load = load(near_source, near_ref, load_sem.at[5])
    far_load = load(far_source, far_ref, load_sem.at[6])

    barrier = pltpu.get_barrier_semaphore()

    def greet(peer):
        pl.semaphore_signal(barrier, inc=1, device_id=peer, device_id_type=pl.DeviceIdType.MESH)

    greet({"leaf": partner})
    greet({"leaf": beside})
    for step in range(1, clusters):
        greet({"top": lax.rem(cluster + step, clusters)})
    pl.when(above)(lambda: greet({"leaf": me + 4}))
    pl.when(below)(lambda: greet({"leaf": me - 4}))
    expected = clusters + 1 + above.astype(jnp.int32) + below.astype(jnp.int32)
    for copy in raw_loads + [basis_load, nested_load, near_load]:
        copy.start()

    def remote(source, target, sem, peer, done):
        return pltpu.make_async_remote_copy(
            src_ref=source,
            dst_ref=target,
            send_sem=send_sem.at[done],
            recv_sem=sem,
            device_id=peer,
            device_id_type=pl.DeviceIdType.MESH,
        )

    def send(source, target, sem, peer, done, condition=None):
        copy = remote(source, target, sem, peer, done)
        if condition is None:
            copy.start()
        else:
            pl.when(condition)(copy.start)

    def receive(block, sem, condition=None):
        copy = remote(block, block, sem, {"leaf": partner}, 0)
        if condition is None:
            copy.wait_recv()
        else:
            pl.when(condition)(copy.wait_recv)

    def drain(block, done, condition=None):
        copy = remote(block, block, block_sem.at[0], {"leaf": partner}, done)
        if condition is None:
            copy.wait_send()
        else:
            pl.when(condition)(copy.wait_send)

    to_partner, to_beside = {"leaf": partner}, {"leaf": beside}
    to_above, to_below = {"leaf": me + 4}, {"leaf": me - 4}

    own_slot = REACH + core
    partner_slot = REACH + other
    beside_slot = core + 6 - 4 * column
    diagonal_slot = core + 2 + 4 * column
    below_slot = core
    above_slot = core + 8
    diagonal = jnp.logical_or(
        jnp.logical_and(first_column, below), jnp.logical_and(column == 1, above)
    )
    relay_over = jnp.logical_or(
        jnp.logical_and(column == 1, below), jnp.logical_and(first_column, above)
    )
    relay_up = jnp.logical_and(first_column, above)
    relay_down = jnp.logical_and(column == 1, below)

    def send_block(slot, part, target, arrival, peer, done, condition=None):
        send(
            window.at[slot, part],
            window.at[target, part],
            block_sem.at[arrival + part],
            peer,
            done,
            condition,
        )

    def wait_block(slot, part, arrival, condition=None):
        receive(window.at[slot, part], block_sem.at[arrival + part], condition)

    def rows_of(index):
        return pl.ds(index * piece, piece)

    def span_of(index):
        start, stop = SPANS[index]
        return pl.ds(start * sixth, (stop - start) * sixth)

    def send_rows(slot, part, span, target, arrival, peer, done, condition=None):
        send(
            window.at[slot, part, span],
            window.at[target, part, span],
            block_sem.at[arrival],
            peer,
            done,
            condition,
        )

    def wait_rows(slot, part, span, arrival, condition=None):
        receive(window.at[slot, part, span], block_sem.at[arrival], condition)

    def send_coeff(leaf, peer, done, condition=None):
        send(coeffs.at[leaf], coeffs.at[leaf], coeff_sem.at[lax.div(leaf, 2)], peer, done, condition)

    def hand_coeff(leaf, condition):
        send(
            coeffs.at[leaf],
            coeffs.at[leaf],
            coeff_sem.at[2 * levels],
            to_partner,
            COEFF_PARTNER,
            condition,
        )

    def wait_coeff(leaf, condition=None):
        receive(coeffs.at[leaf], coeff_sem.at[lax.div(leaf, 2)], condition)

    def for_count(conditions, run):
        count = 0
        for condition in conditions:
            count = count + jnp.where(condition, 1, 0)
        for n in range(1, len(conditions) + 1):
            pl.when(count == n)(lambda n=n: run(coeffs.at[pl.ds(0, n)]))

    def exists(step):
        return jnp.logical_and(level + step >= 0, level + step < levels)

    def crosses(step, from_first):
        return step <= -1 or step >= 2 if from_first else step >= 1 or step <= -2

    def crossing(step):
        if crosses(step, True) and crosses(step, False):
            return exists(step)
        return jnp.logical_and(exists(step), first_column if crosses(step, True) else column == 1)

    def crossed(step):
        if crosses(step, True) and crosses(step, False):
            return exists(step)
        return jnp.logical_and(exists(step), column == 1 if crosses(step, True) else first_column)

    def handed(step, which):
        if abs(step) >= 2:
            return exists(step)
        return jnp.logical_and(exists(step), which == (1 if step == 1 else 0))

    def relay_coeffs(hop):
        for step in (-hop, hop):
            wait_coeff(me + 4 * step, exists(step))
        if hop + 1 < levels:
            send_coeff(me - 4 * hop, to_above, COEFF_ABOVE, jnp.logical_and(exists(-hop), above))
            send_coeff(me + 4 * hop, to_below, COEFF_BELOW, jnp.logical_and(exists(hop), below))

    def cross_coeffs(hop):
        for step in (-hop, hop):
            send_coeff(me + 4 * step, to_beside, COEFF_BESIDE, crossing(step))
            hand_coeff(me + 4 * step, handed(step, core))

    def hand_crossed(hop):
        for step in (-hop, hop):
            wait_coeff(beside + 4 * step, crossed(step))
            hand_coeff(beside + 4 * step, crossed(step))

    def near(slot, part, condition=None, first=False, index=None):
        offset = slot - REACH - core
        place, hit = 0, 0
        for k in range(tile_count):
            here = near_ref[0, 0, k] == offset
            place = jnp.where(here, k, place)
            hit = jnp.where(here, 1, hit)
        scale = hit.astype(jnp.float32)

        def run():
            if index is None:
                product = dot(tiles[place], window[slot, part]) * scale
            else:
                start, stop = SPANS[index]
                span = slice(start * sixth, stop * sixth)
                product = dot(tiles[place, :, span], window[slot, part, span, :]) * scale
            if first:
                acc[part] = product
            else:
                acc[part] += product

        if condition is None:
            run()
        else:
            pl.when(condition)(run)

    own_beside = own_slot + 4 * column - 2

    def send_own(part, index):
        span = rows_of(index)
        send_rows(own_slot, part, span, core, BELOW + part, to_above, TO_ABOVE, above)
        send_rows(own_slot, part, span, core + 8, ABOVE + part, to_below, TO_BELOW, below)

    def send_first(index):
        send_rows(own_slot, 0, rows_of(index), own_beside, BESIDE, to_beside, TO_BESIDE)

    live = lax.broadcasted_iota(jnp.int32, (rows, half), 0) < count_ref[0, 0]

    def mask(part):
        raw_loads[part].wait()
        window[own_slot, part] = jnp.where(live, raw[part], jnp.zeros((), jnp.bfloat16))

    mask(0)
    pl.semaphore_wait(barrier, expected)
    for index in range(PIECES - 1):
        send_first(index)
    send_own(0, 0)
    mask(1)
    basis_load.wait()
    for part in range(2):
        product = contract(basis[...], window[own_slot, part])
        coeffs[me, :, part * half : (part + 1) * half] = product.astype(jnp.bfloat16)
    nested_load.wait()
    for part in range(2):
        halves[part] = contract(nested[...], coeffs[me, :, part * half : (part + 1) * half])
    send_coeff(me, to_above, COEFF_ABOVE, above)
    send_coeff(me, to_below, COEFF_BELOW, below)
    for index in range(1, PIECES):
        send_own(0, index)
    send(halves.at[other], half_in, half_sem.at[0], to_partner, HALF)
    for part in range(2):
        send_block(own_slot, part, own_slot, PARTNER, to_partner, TO_PARTNER)
    for copy in tile_loads + [far_load, coupling_load, top_load]:
        copy.start()

    receive(half_in, half_sem.at[0])
    total = halves[core] + half_in[...]
    for part in range(2):
        partial[part] = total[:, part * quarter : (part + 1) * quarter]
    send(partial.at[1 - column], quarter_in, quarter_sem.at[0], to_beside, QUARTER)
    send_first(PIECES - 1)
    near_load.wait()
    all_tiles.wait()
    near(own_slot, 0, first=True)
    near(own_slot, 1, first=True)
    for part in range(2):
        wait_block(partner_slot, part, PARTNER)
        near(partner_slot, part)

    relay_coeffs(1)
    cross_coeffs(1)
    send_block(own_slot, 1, own_beside, BESIDE, to_beside, TO_BESIDE)
    receive(quarter_in, quarter_sem.at[0])
    partial[column] += quarter_in[...]

    def line(turn):
        for way, at, step in ((0, turn - 1, 4), (1, levels - turn, -4)):
            here = level == at
            if turn > 1:
                receive(line_in.at[way], line_sem.at[way], here)
            if turn < levels:

                @pl.when(here)
                def _(way=way):
                    value = partial[column]
                    if turn > 1:
                        value = value + line_in[way]
                    line_out[way] = value

                send(line_out.at[way], line_in.at[way], line_sem.at[way], {"leaf": me + step}, LINE, here)

    line(1)
    send_own(1, 0)

    bridged_slot = jnp.where(core == 0, 1, 8)
    bridged = jnp.logical_or(
        jnp.logical_and(core == 0, below), jnp.logical_and(core == 1, above)
    )
    hand_below = jnp.logical_and(core == 1, below)
    hand_above = jnp.logical_and(core == 0, above)
    far_beside_slot = other + 6 - 4 * column
    far_diagonal_slot = other + 2 + 4 * column

    def hand_neighbours(part):
        send_block(below_slot, part, below_slot, BRIDGED, to_partner, HAND_COLUMN, hand_below)
        send_block(above_slot, part, above_slot, BRIDGED, to_partner, HAND_COLUMN, hand_above)

    def send_over(index):
        span = rows_of(index)
        arrival = DIAGONAL + index
        send_rows(below_slot, 0, span, core + 2, arrival, to_beside, OVER, relay_down)
        send_rows(above_slot, 0, span, core + 6, arrival, to_beside, OVER, relay_up)

    wait_block(beside_slot, 0, BESIDE)
    send_block(beside_slot, 0, beside_slot, FAR_BESIDE, to_partner, HAND_BESIDE)
    near(beside_slot, 0)
    wait_block(below_slot, 0, BELOW, below)
    wait_block(above_slot, 0, ABOVE, above)
    hand_neighbours(0)
    near(below_slot, 0, below)
    near(above_slot, 0, above)
    line(2)
    send_own(1, 1)

    hand_crossed(1)
    if levels > 2:
        relay_coeffs(2)
        cross_coeffs(2)
    for index in range(PIECES):
        send_over(index)
    wait_block(far_beside_slot, 0, FAR_BESIDE)
    near(far_beside_slot, 0)
    wait_block(bridged_slot, 0, BRIDGED, bridged)
    near(bridged_slot, 0, bridged)
    for turn in range(3, levels):
        line(turn)
    send_own(1, 2)

    wait_block(beside_slot, 1, BESIDE)
    for index in range(1, len(SPANS)):
        span = span_of(index)
        arrival = SPAN + index
        send_rows(beside_slot, 1, span, core + 2, arrival, to_above, ALONG, relay_up)
        send_rows(beside_slot, 1, span, core + 6, arrival, to_below, ALONG, relay_down)
    send_block(beside_slot, 1, beside_slot, FAR_BESIDE, to_partner, HAND_BESIDE)
    near(beside_slot, 1)
    if levels > 2:
        line(levels)
    whole = partial[column]
    for way, condition in ((0, below), (1, above)):
        whole = whole + jnp.where(condition, line_in[way], 0.0)
    parents[cluster] = whole.astype(jnp.bfloat16)
    for step in range(1, clusters):
        send(
            parents.at[cluster],
            parents.at[cluster],
            parent_sem.at[cluster],
            {"top": lax.rem(cluster + step, clusters)},
            PARENT + step - 1,
        )
    wait_block(far_beside_slot, 1, FAR_BESIDE)
    near(far_beside_slot, 1)
    coupling_load.wait()
    top_load.wait()
    for step in range(1, clusters):
        source = lax.rem(cluster + step, clusters)
        receive(parents.at[source], parent_sem.at[source])
    over = jnp.zeros(parents.shape[1:], jnp.float32)
    for m in range(top.shape[0]):
        over = over + dot(top[m], parents[lax.rem(cluster + 1 + m, clusters)])
    place = 2 * core + column
    fields[place] = over.astype(jnp.bfloat16)
    send(fields.at[place], fields.at[place], field_sem.at[0], to_beside, FIELD)
    if levels > 2:
        hand_crossed(2)
    for hop in range(3, levels):
        relay_coeffs(hop)
        cross_coeffs(hop)
    wait_block(below_slot, 1, BELOW, below)
    wait_block(above_slot, 1, ABOVE, above)
    span = span_of(0)
    send_rows(below_slot, 1, span, core + 2, SPAN, to_beside, OVER_SPAN, relay_down)
    send_rows(above_slot, 1, span, core + 6, SPAN, to_beside, OVER_SPAN, relay_up)
    hand_neighbours(1)
    near(below_slot, 1, below)
    near(above_slot, 1, above)

    def hand_first(index):
        span = rows_of(index)
        wait_rows(diagonal_slot, 0, span, DIAGONAL + index, diagonal)
        send_rows(
            diagonal_slot, 0, span, diagonal_slot, FAR_DIAGONAL, to_partner, HAND_DIAGONAL, diagonal
        )

    def hand_second(index):
        span = span_of(index)
        wait_rows(diagonal_slot, 1, span, SPAN + index, diagonal)
        arrival = FAR_SPAN + index
        send_rows(
            diagonal_slot, 1, span, diagonal_slot, arrival, to_partner, HAND_DIAGONAL, diagonal
        )

    def far_second(index):
        wait_rows(far_diagonal_slot, 1, span_of(index), FAR_SPAN + index, diagonal)
        near(far_diagonal_slot, 1, diagonal, index=index)

    def own_second(index):
        near(diagonal_slot, 1, diagonal, index=index)

    hand_first(0)
    wait_block(bridged_slot, 1, BRIDGED, bridged)
    near(bridged_slot, 1, bridged)
    hand_second(1)
    hand_first(1)
    own_second(1)
    hand_first(2)
    hand_second(2)
    near(diagonal_slot, 0, diagonal)
    own_second(2)
    next_place = 2 * core + 1 - column
    receive(fields.at[next_place], field_sem.at[0])
    pair = fields.at[pl.ds(2 * core, 2)]
    send(pair, pair, field_sem.at[1], to_partner, FIELD_PAIR)
    wait_block(far_diagonal_slot, 0, FAR_DIAGONAL, diagonal)
    near(far_diagonal_slot, 0, diagonal)
    far_second(1)
    for hop in range(3, levels):
        hand_crossed(hop)
    far_second(2)
    hand_second(3)

    steps = [step for hop in range(1, levels) for step in (-hop, hop)]
    theirs_count = [handed(step, other) for step in steps] + [crossed(step) for step in steps]
    for_count(theirs_count, lambda block: receive(block, coeff_sem.at[2 * levels]))
    theirs = fields.at[pl.ds(2 * other, 2)]
    receive(theirs, field_sem.at[1])
    far_load.wait()
    field = dot(nested[...], jnp.concatenate([fields[k] for k in range(4)], axis=1))
    for m in range(coupling.shape[0]):
        field = field + dot(coupling[m], coeffs[far_ref[0, 0, m]])
    field = field.astype(jnp.bfloat16)
    for part in range(2):
        acc[part] += dot(basis[...], field[:, part * half : (part + 1) * half])
    hand_second(0)
    own_second(3)
    own_second(0)
    far_second(3)
    far_second(0)

    whole_block = window.at[own_slot]
    for done, condition in (
        (TO_BESIDE, None),
        (TO_ABOVE, above),
        (TO_BELOW, below),
        (TO_PARTNER, None),
        (HAND_BESIDE, None),
        (HAND_COLUMN, jnp.logical_or(hand_below, hand_above)),
        (HAND_DIAGONAL, diagonal),
    ):
        drain(whole_block, done, condition)
    drain(window.at[own_slot, 0], OVER, relay_over)
    drain(window.at[own_slot, 1, span_of(0)], OVER_SPAN, relay_over)
    drain(window.at[own_slot, 1, pl.ds(sixth, 5 * sixth)], ALONG, relay_over)
    drain(halves.at[0], HALF)
    drain(partial.at[0], QUARTER)
    drain(fields.at[0], FIELD)
    drain(fields.at[pl.ds(0, 2)], FIELD_PAIR)
    for step in range(1, clusters):
        drain(parents.at[0], PARENT + step - 1)
    drain(line_out.at[0], LINE, jnp.logical_xor(above, below))
    drain(line_out, LINE, jnp.logical_and(above, below))
    ours = [handed(step, core) for step in steps] + [crossed(step) for step in steps]
    for_count(ours, lambda block: drain(block, COEFF_PARTNER))
    for_count([crossing(step) for step in steps], lambda block: drain(block, COEFF_BESIDE))
    up = [above] + [jnp.logical_and(exists(-hop), above) for hop in range(1, levels)]
    down = [below] + [jnp.logical_and(exists(hop), below) for hop in range(1, levels)]
    for_count(up, lambda block: drain(block, COEFF_ABOVE))
    for_count(down, lambda block: drain(block, COEFF_BELOW))


def finish_kernel(count_ref, acc_ref, out_ref, staged, sem):
    steps, rows = staged.shape[:2]
    half = acc_ref.shape[2]
    copies = []
    for step in range(steps):
        span = slice(step * rows, (step + 1) * rows)
        live = lax.broadcasted_iota(jnp.int32, (rows, half), 0) < count_ref[0, 0] - step * rows
        for part in range(2):
            columns = slice(part * half, (part + 1) * half)
            staged[step, :, columns] = jnp.where(live, acc_ref[part, span], 0.0)
        copy = pltpu.make_async_copy(staged.at[step], out_ref.at[span], sem.at[step])
        copy.start()
        copies.append(copy)
    for copy in copies:
        copy.wait()


def body(
    vectors,
    near_tiles,
    leaf_basis,
    transfer,
    coupling,
    top_coupling,
    near_list,
    far_list,
    row_counts,
):
    leaves = lax.axis_size("leaf")
    clusters = lax.axis_size("top")
    levels = leaves // 4
    rows, vecs = vectors.shape[2:]
    rank = transfer.shape[2]
    half, quarter = vecs // 2, vecs // 4
    smem = pl.BlockSpec(memory_space=pltpu.SMEM)
    vmem = pl.BlockSpec(memory_space=pltpu.VMEM)
    hbm = pl.BlockSpec(memory_space=pltpu.HBM)
    dma = pltpu.SemaphoreType.DMA
    acc = pl.pallas_call(
        functools.partial(exchange_kernel, levels, clusters),
        out_shape=jax.ShapeDtypeStruct((2, rows, half), jnp.float32),
        in_specs=[smem] + [hbm] * 8,
        out_specs=vmem,
        scratch_shapes=[
            pltpu.SMEM(near_list.shape, jnp.int32),
            pltpu.SMEM(far_list.shape, jnp.int32),
            pltpu.VMEM((2, rows, half), jnp.bfloat16),
            pltpu.VMEM(near_tiles.shape[2:], jnp.bfloat16),
            pltpu.VMEM(leaf_basis.shape[2:], jnp.bfloat16),
            pltpu.VMEM(transfer.shape[2:], jnp.bfloat16),
            pltpu.VMEM(coupling.shape[2:], jnp.bfloat16),
            pltpu.VMEM(top_coupling.shape[1:], jnp.bfloat16),
            pltpu.VMEM((SLOTS, 2, rows, half), jnp.bfloat16),
            pltpu.VMEM((leaves, rank, vecs), jnp.bfloat16),
            pltpu.VMEM((2, rank, half), jnp.float32),
            pltpu.VMEM((rank, half), jnp.float32),
            pltpu.VMEM((2, rank, quarter), jnp.float32),
            pltpu.VMEM((rank, quarter), jnp.float32),
            pltpu.VMEM((2, rank, quarter), jnp.float32),
            pltpu.VMEM((2, rank, quarter), jnp.float32),
            pltpu.VMEM((clusters, rank, quarter), jnp.bfloat16),
            pltpu.VMEM((4, rank, quarter), jnp.bfloat16),
            dma((9,)),
            dma((PARENT + clusters - 1,)),
            dma((ARRIVALS,)),
            dma((leaves // 2 + 1,)),
            dma((1,)),
            dma((1,)),
            dma((2,)),
            dma((clusters,)),
            dma((2,)),
        ],
        compiler_params=pltpu.CompilerParams(
            collective_id=0, has_side_effects=True, vmem_limit_bytes=48 * 1024 * 1024
        ),
    )(
        row_counts,
        *[
            pltpu.with_memory_space_constraint(array, pltpu.HBM)
            for array in (
                near_list,
                far_list,
                vectors,
                near_tiles,
                leaf_basis,
                transfer,
                coupling,
                top_coupling,
            )
        ],
    )
    result = pl.pallas_call(
        finish_kernel,
        out_shape=jax.ShapeDtypeStruct((rows, vecs), jnp.float32),
        in_specs=[smem, vmem],
        out_specs=pl.BlockSpec(memory_space=pl.ANY),
        scratch_shapes=[
            pltpu.VMEM((PIECES, rows // PIECES, vecs), jnp.float32),
            dma((PIECES,)),
        ],
        compiler_params=pltpu.CompilerParams(vmem_limit_bytes=8 * 1024 * 1024),
    )(row_counts, acc)
    return result[None, None]


def solution(mesh):
    in_specs = (
        P("top", "leaf", None, None),
        P("top", "leaf", None, None, None),
        P("top", "leaf", None, None),
        P("top", "leaf", None, None),
        P("top", "leaf", None, None, None),
        P("top", None, None, None),
        P("top", "leaf", None),
        P("top", "leaf", None),
        P("top", "leaf"),
    )
    out_specs = P("top", "leaf", None, None)
    return jax.shard_map(body, mesh=mesh, in_specs=in_specs, out_specs=out_specs, check_vma=False)
```

```python
import functools

import jax
import jax.numpy as jnp
from jax import lax
from jax.experimental import pallas as pl
from jax.experimental.pallas import tpu as pltpu
from jax.sharding import PartitionSpec as P

REACH = 4
SLOTS = 2 * REACH + 2
PIECES = 3
SPANS = ((0, 1), (1, 3), (3, 5), (5, 6))
BESIDE, BELOW, ABOVE, PARTNER, FAR_BESIDE, BRIDGED = 0, 2, 4, 6, 8, 10
DIAGONAL, FAR_DIAGONAL, SPAN = 12, 12 + PIECES, 12 + 2 * PIECES
FAR_SPAN = SPAN + len(SPANS)
ARRIVALS = FAR_SPAN + len(SPANS)
(
    TO_BESIDE,
    TO_ABOVE,
    TO_BELOW,
    TO_PARTNER,
    OVER,
    OVER_SPAN,
    ALONG,
    HAND_BESIDE,
    HAND_COLUMN,
    HAND_DIAGONAL,
    COEFF_ABOVE,
    COEFF_BELOW,
    COEFF_BESIDE,
    COEFF_PARTNER,
    HALF,
    QUARTER,
    LINE,
    FIELD,
    FIELD_PAIR,
    PARENT,
) = range(20)


def contract(left, right):
    return lax.dot_general(left, right, (((0,), (0,)), ((), ())), preferred_element_type=jnp.float32)


def dot(left, right):
    return jnp.dot(left, right, preferred_element_type=jnp.float32)


def exchange_kernel(
    levels,
    clusters,
    count_ref,
    near_source,
    far_source,
    vectors_ref,
    tiles_ref,
    basis_ref,
    nested_ref,
    coupling_ref,
    top_ref,
    acc,
    near_ref,
    far_ref,
    raw,
    tiles,
    basis,
    nested,
    coupling,
    top,
    window,
    coeffs,
    halves,
    half_in,
    partial,
    quarter_in,
    line_out,
    line_in,
    parents,
    fields,
    load_sem,
    send_sem,
    block_sem,
    coeff_sem,
    half_sem,
    quarter_sem,
    line_sem,
    parent_sem,
    field_sem,
):
    me = lax.axis_index("leaf")
    cluster = lax.axis_index("top")
    core = lax.rem(me, 2)
    column = lax.rem(lax.div(me, 2), 2)
    level = lax.div(me, 4)
    other = 1 - core
    partner = me + 1 - 2 * core
    beside = me + 2 - 4 * column
    above = level < levels - 1
    below = level > 0
    first_column = column == 0
    rows, half = raw.shape[1:]
    vecs = 2 * half
    quarter = half // 2
    sixth = rows // 6
    piece = rows // PIECES
    tile_count = tiles.shape[0]

    def load(source, target, sem):
        return pltpu.make_async_copy(source, target, sem)

    raw_loads = [
        load(vectors_ref.at[0, 0, :, pl.ds(part * half, half)], raw.at[part], load_sem.at[part])
        for part in range(2)
    ]
    basis_load = load(basis_ref.at[0, 0], basis, load_sem.at[2])
    nested_load = load(nested_ref.at[0, 0], nested, load_sem.at[7])
    coupling_load = load(coupling_ref.at[0, 0], coupling, load_sem.at[3])
    top_load = load(top_ref.at[0], top, load_sem.at[4])
    tile_loads = [load(tiles_ref.at[0, 0, k], tiles.at[k], load_sem.at[8]) for k in range(tile_count)]
    all_tiles = load(tiles_ref.at[0, 0], tiles, load_sem.at[8])
    near_load = load(near_source, near_ref, load_sem.at[5])
    far_load = load(far_source, far_ref, load_sem.at[6])

    barrier = pltpu.get_barrier_semaphore()

    def greet(peer):
        pl.semaphore_signal(barrier, inc=1, device_id=peer, device_id_type=pl.DeviceIdType.MESH)

    greet({"leaf": partner})
    greet({"leaf": beside})
    for step in range(1, clusters):
        greet({"top": lax.rem(cluster + step, clusters)})
    pl.when(above)(lambda: greet({"leaf": me + 4}))
    pl.when(below)(lambda: greet({"leaf": me - 4}))
    expected = clusters + 1 + above.astype(jnp.int32) + below.astype(jnp.int32)
    for copy in raw_loads + [basis_load, nested_load, near_load]:
        copy.start()

    def remote(source, target, sem, peer, done):
        return pltpu.make_async_remote_copy(
            src_ref=source,
            dst_ref=target,
            send_sem=send_sem.at[done],
            recv_sem=sem,
            device_id=peer,
            device_id_type=pl.DeviceIdType.MESH,
        )

    def send(source, target, sem, peer, done, condition=None):
        copy = remote(source, target, sem, peer, done)
        if condition is None:
            copy.start()
        else:
            pl.when(condition)(copy.start)

    def receive(block, sem, condition=None):
        copy = remote(block, block, sem, {"leaf": partner}, 0)
        if condition is None:
            copy.wait_recv()
        else:
            pl.when(condition)(copy.wait_recv)

    def drain(block, done, condition=None):
        copy = remote(block, block, block_sem.at[0], {"leaf": partner}, done)
        if condition is None:
            copy.wait_send()
        else:
            pl.when(condition)(copy.wait_send)

    to_partner, to_beside = {"leaf": partner}, {"leaf": beside}
    to_above, to_below = {"leaf": me + 4}, {"leaf": me - 4}

    own_slot = REACH + core
    partner_slot = REACH + other
    beside_slot = core + 6 - 4 * column
    diagonal_slot = core + 2 + 4 * column
    below_slot = core
    above_slot = core + 8
    diagonal = jnp.logical_or(
        jnp.logical_and(first_column, below), jnp.logical_and(column == 1, above)
    )
    relay_over = jnp.logical_or(
        jnp.logical_and(column == 1, below), jnp.logical_and(first_column, above)
    )
    relay_up = jnp.logical_and(first_column, above)
    relay_down = jnp.logical_and(column == 1, below)

    def send_block(slot, part, target, arrival, peer, done, condition=None):
        send(
            window.at[slot, part],
            window.at[target, part],
            block_sem.at[arrival + part],
            peer,
            done,
            condition,
        )

    def wait_block(slot, part, arrival, condition=None):
        receive(window.at[slot, part], block_sem.at[arrival + part], condition)

    def rows_of(index):
        return pl.ds(index * piece, piece)

    def span_of(index):
        start, stop = SPANS[index]
        return pl.ds(start * sixth, (stop - start) * sixth)

    def send_rows(slot, part, span, target, arrival, peer, done, condition=None):
        send(
            window.at[slot, part, span],
            window.at[target, part, span],
            block_sem.at[arrival],
            peer,
            done,
            condition,
        )

    def wait_rows(slot, part, span, arrival, condition=None):
        receive(window.at[slot, part, span], block_sem.at[arrival], condition)

    def send_coeff(leaf, peer, done, condition=None):
        send(coeffs.at[leaf], coeffs.at[leaf], coeff_sem.at[lax.div(leaf, 2)], peer, done, condition)

    def hand_coeff(leaf, condition):
        send(
            coeffs.at[leaf],
            coeffs.at[leaf],
            coeff_sem.at[2 * levels],
            to_partner,
            COEFF_PARTNER,
            condition,
        )

    def wait_coeff(leaf, condition=None):
        receive(coeffs.at[leaf], coeff_sem.at[lax.div(leaf, 2)], condition)

    def for_count(conditions, run):
        count = 0
        for condition in conditions:
            count = count + jnp.where(condition, 1, 0)
        for n in range(1, len(conditions) + 1):
            pl.when(count == n)(lambda n=n: run(coeffs.at[pl.ds(0, n)]))

    def exists(step):
        return jnp.logical_and(level + step >= 0, level + step < levels)

    def crosses(step, from_first):
        return step <= -1 or step >= 2 if from_first else step >= 1 or step <= -2

    def crossing(step):
        if crosses(step, True) and crosses(step, False):
            return exists(step)
        return jnp.logical_and(exists(step), first_column if crosses(step, True) else column == 1)

    def crossed(step):
        if crosses(step, True) and crosses(step, False):
            return exists(step)
        return jnp.logical_and(exists(step), column == 1 if crosses(step, True) else first_column)

    def handed(step, which):
        if abs(step) >= 2:
            return exists(step)
        return jnp.logical_and(exists(step), which == (1 if step == 1 else 0))

    def relay_coeffs(hop):
        for step in (-hop, hop):
            wait_coeff(me + 4 * step, exists(step))
        if hop + 1 < levels:
            send_coeff(me - 4 * hop, to_above, COEFF_ABOVE, jnp.logical_and(exists(-hop), above))
            send_coeff(me + 4 * hop, to_below, COEFF_BELOW, jnp.logical_and(exists(hop), below))

    def cross_coeffs(hop):
        for step in (-hop, hop):
            send_coeff(me + 4 * step, to_beside, COEFF_BESIDE, crossing(step))
            hand_coeff(me + 4 * step, handed(step, core))

    def hand_crossed(hop):
        for step in (-hop, hop):
            wait_coeff(beside + 4 * step, crossed(step))
            hand_coeff(beside + 4 * step, crossed(step))

    def near(slot, part, condition=None, first=False, spans=None):
        offset = slot - REACH - core
        place, hit = 0, 0
        for k in range(tile_count):
            here = near_ref[0, 0, k] == offset
            place = jnp.where(here, k, place)
            hit = jnp.where(here, 1, hit)
        scale = hit.astype(jnp.float32)

        def run():
            if spans is None:
                product = dot(tiles[place], window[slot, part]) * scale
            else:
                product = 0.0
                for start, stop in spans:
                    span = slice(start * sixth, stop * sixth)
                    product = product + dot(tiles[place, :, span], window[slot, part, span, :])
                product = product * scale
            if first:
                acc[part] = product
            else:
                acc[part] += product

        if condition is None:
            run()
        else:
            pl.when(condition)(run)

    own_beside = own_slot + 4 * column - 2

    def send_own(part, index):
        span = rows_of(index)
        send_rows(own_slot, part, span, core, BELOW + part, to_above, TO_ABOVE, above)
        send_rows(own_slot, part, span, core + 8, ABOVE + part, to_below, TO_BELOW, below)

    def send_first(index):
        send_rows(own_slot, 0, rows_of(index), own_beside, BESIDE, to_beside, TO_BESIDE)

    live = lax.broadcasted_iota(jnp.int32, (rows, half), 0) < count_ref[0, 0]

    def mask(part):
        raw_loads[part].wait()
        window[own_slot, part] = jnp.where(live, raw[part], jnp.zeros((), jnp.bfloat16))

    mask(0)
    pl.semaphore_wait(barrier, expected)
    for index in range(PIECES - 1):
        send_first(index)
    send_own(0, 0)
    mask(1)
    basis_load.wait()
    for part in range(2):
        product = contract(basis[...], window[own_slot, part])
        coeffs[me, :, part * half : (part + 1) * half] = product.astype(jnp.bfloat16)
    nested_load.wait()
    for part in range(2):
        halves[part] = contract(nested[...], coeffs[me, :, part * half : (part + 1) * half])
    send_coeff(me, to_above, COEFF_ABOVE, above)
    send_coeff(me, to_below, COEFF_BELOW, below)
    for index in range(1, PIECES):
        send_own(0, index)
    send(halves.at[other], half_in, half_sem.at[0], to_partner, HALF)
    for part in range(2):
        send_block(own_slot, part, own_slot, PARTNER, to_partner, TO_PARTNER)
    for copy in tile_loads + [far_load, coupling_load, top_load]:
        copy.start()

    receive(half_in, half_sem.at[0])
    total = halves[core] + half_in[...]
    for part in range(2):
        partial[part] = total[:, part * quarter : (part + 1) * quarter]
    send(partial.at[1 - column], quarter_in, quarter_sem.at[0], to_beside, QUARTER)
    send_first(PIECES - 1)
    near_load.wait()
    all_tiles.wait()
    near(own_slot, 0, first=True)
    near(own_slot, 1, first=True)
    for part in range(2):
        wait_block(partner_slot, part, PARTNER)
        near(partner_slot, part)

    relay_coeffs(1)
    cross_coeffs(1)
    send_block(own_slot, 1, own_beside, BESIDE, to_beside, TO_BESIDE)
    receive(quarter_in, quarter_sem.at[0])
    partial[column] += quarter_in[...]

    def line(turn):
        for way, at, step in ((0, turn - 1, 4), (1, levels - turn, -4)):
            here = level == at
            if turn > 1:
                receive(line_in.at[way], line_sem.at[way], here)
            if turn < levels:

                @pl.when(here)
                def _(way=way):
                    value = partial[column]
                    if turn > 1:
                        value = value + line_in[way]
                    line_out[way] = value

                send(line_out.at[way], line_in.at[way], line_sem.at[way], {"leaf": me + step}, LINE, here)

    line(1)
    send_own(1, 0)

    bridged_slot = jnp.where(core == 0, 1, 8)
    bridged = jnp.logical_or(
        jnp.logical_and(core == 0, below), jnp.logical_and(core == 1, above)
    )
    hand_below = jnp.logical_and(core == 1, below)
    hand_above = jnp.logical_and(core == 0, above)
    far_beside_slot = other + 6 - 4 * column
    far_diagonal_slot = other + 2 + 4 * column

    def hand_neighbours(part):
        send_block(below_slot, part, below_slot, BRIDGED, to_partner, HAND_COLUMN, hand_below)
        send_block(above_slot, part, above_slot, BRIDGED, to_partner, HAND_COLUMN, hand_above)

    def send_over(index):
        span = rows_of(index)
        arrival = DIAGONAL + index
        send_rows(below_slot, 0, span, core + 2, arrival, to_beside, OVER, relay_down)
        send_rows(above_slot, 0, span, core + 6, arrival, to_beside, OVER, relay_up)

    wait_block(beside_slot, 0, BESIDE)
    send_block(beside_slot, 0, beside_slot, FAR_BESIDE, to_partner, HAND_BESIDE)
    near(beside_slot, 0)
    wait_block(below_slot, 0, BELOW, below)
    wait_block(above_slot, 0, ABOVE, above)
    hand_neighbours(0)
    near(below_slot, 0, below)
    near(above_slot, 0, above)
    line(2)
    send_own(1, 1)

    hand_crossed(1)
    if levels > 2:
        relay_coeffs(2)
        cross_coeffs(2)
    for index in range(PIECES - 1):
        send_over(index)
    wait_block(far_beside_slot, 0, FAR_BESIDE)
    near(far_beside_slot, 0)
    wait_block(bridged_slot, 0, BRIDGED, bridged)
    near(bridged_slot, 0, bridged)
    for turn in range(3, levels):
        line(turn)
    send_own(1, 2)

    wait_block(beside_slot, 1, BESIDE)
    inner_up = jnp.logical_and(relay_up, level < levels - 2)
    inner_down = jnp.logical_and(relay_down, level > 1)
    for index in range(len(SPANS)):
        span = span_of(index)
        arrival = SPAN + index
        up, down = (relay_up, relay_down) if index else (inner_up, inner_down)
        send_rows(beside_slot, 1, span, core + 2, arrival, to_above, ALONG, up)
        send_rows(beside_slot, 1, span, core + 6, arrival, to_below, ALONG, down)
    send_block(beside_slot, 1, beside_slot, FAR_BESIDE, to_partner, HAND_BESIDE)
    near(beside_slot, 1)
    for hop in range(3, levels):
        relay_coeffs(hop)
        cross_coeffs(hop)
    if levels > 2:
        line(levels)
    whole = partial[column]
    for way, condition in ((0, below), (1, above)):
        whole = whole + jnp.where(condition, line_in[way], 0.0)
    parents[cluster] = whole.astype(jnp.bfloat16)
    for step in range(1, clusters):
        send(
            parents.at[cluster],
            parents.at[cluster],
            parent_sem.at[cluster],
            {"top": lax.rem(cluster + step, clusters)},
            PARENT + step - 1,
        )
    wait_block(far_beside_slot, 1, FAR_BESIDE)
    near(far_beside_slot, 1)
    coupling_load.wait()
    top_load.wait()
    for step in range(1, clusters):
        source = lax.rem(cluster + step, clusters)
        receive(parents.at[source], parent_sem.at[source])
    over = jnp.zeros(parents.shape[1:], jnp.float32)
    for m in range(top.shape[0]):
        over = over + dot(top[m], parents[lax.rem(cluster + 1 + m, clusters)])
    place = 2 * core + column
    fields[place] = over.astype(jnp.bfloat16)
    send(fields.at[place], fields.at[place], field_sem.at[0], to_beside, FIELD)
    send_over(PIECES - 1)
    if levels > 2:
        hand_crossed(2)
    wait_block(below_slot, 1, BELOW, below)
    wait_block(above_slot, 1, ABOVE, above)
    span = span_of(0)
    last_down = jnp.logical_and(relay_down, level == levels - 1)
    last_up = jnp.logical_and(relay_up, level == 0)
    send_rows(below_slot, 1, span, core + 2, SPAN, to_beside, OVER_SPAN, last_down)
    send_rows(above_slot, 1, span, core + 6, SPAN, to_beside, OVER_SPAN, last_up)
    hand_neighbours(1)
    near(below_slot, 1, below)
    near(above_slot, 1, above)

    def hand_first(index):
        span = rows_of(index)
        arrival = FAR_DIAGONAL + index
        wait_rows(diagonal_slot, 0, span, DIAGONAL + index, diagonal)
        send_rows(diagonal_slot, 0, span, diagonal_slot, arrival, to_partner, HAND_DIAGONAL, diagonal)

    def own_first(index):
        near(diagonal_slot, 0, diagonal, spans=((2 * index, 2 * index + 2),))

    def far_first(index):
        wait_rows(far_diagonal_slot, 0, rows_of(index), FAR_DIAGONAL + index, diagonal)
        near(far_diagonal_slot, 0, diagonal, spans=((2 * index, 2 * index + 2),))

    def hand_second(index):
        span = span_of(index)
        arrival = FAR_SPAN + index
        wait_rows(diagonal_slot, 1, span, SPAN + index, diagonal)
        send_rows(diagonal_slot, 1, span, diagonal_slot, arrival, to_partner, HAND_DIAGONAL, diagonal)

    def own_second(*indices):
        near(diagonal_slot, 1, diagonal, spans=[SPANS[index] for index in indices])

    def far_second(*indices):
        for index in indices:
            wait_rows(far_diagonal_slot, 1, span_of(index), FAR_SPAN + index, diagonal)
        near(far_diagonal_slot, 1, diagonal, spans=[SPANS[index] for index in indices])

    hand_first(0)
    own_first(0)
    wait_block(bridged_slot, 1, BRIDGED, bridged)
    near(bridged_slot, 1, bridged)
    hand_second(1)
    own_second(1)
    hand_first(1)
    own_first(1)
    far_first(0)
    far_second(1)
    next_place = 2 * core + 1 - column
    receive(fields.at[next_place], field_sem.at[0])
    pair = fields.at[pl.ds(2 * core, 2)]
    send(pair, pair, field_sem.at[1], to_partner, FIELD_PAIR)
    for hop in range(3, levels):
        hand_crossed(hop)
    far_first(1)
    hand_second(2)
    own_second(2)

    steps = [step for hop in range(1, levels) for step in (-hop, hop)]
    theirs_count = [handed(step, other) for step in steps] + [crossed(step) for step in steps]
    for_count(theirs_count, lambda block: receive(block, coeff_sem.at[2 * levels]))
    theirs = fields.at[pl.ds(2 * other, 2)]
    receive(theirs, field_sem.at[1])
    far_load.wait()
    field = dot(nested[...], jnp.concatenate([fields[k] for k in range(4)], axis=1))
    for m in range(coupling.shape[0]):
        field = field + dot(coupling[m], coeffs[far_ref[0, 0, m]])
    field = field.astype(jnp.bfloat16)
    for part in range(2):
        acc[part] += dot(basis[...], field[:, part * half : (part + 1) * half])

    hand_first(2)
    own_first(2)
    hand_second(3)
    far_second(2)
    hand_second(0)
    own_second(3, 0)
    far_first(2)
    far_second(3, 0)

    whole_block = window.at[own_slot]
    for done, condition in (
        (TO_BESIDE, None),
        (TO_ABOVE, above),
        (TO_BELOW, below),
        (TO_PARTNER, None),
        (HAND_BESIDE, None),
        (HAND_COLUMN, jnp.logical_or(hand_below, hand_above)),
        (HAND_DIAGONAL, diagonal),
    ):
        drain(whole_block, done, condition)
    drain(window.at[own_slot, 0], OVER, relay_over)
    drain(window.at[own_slot, 1, span_of(0)], OVER_SPAN, jnp.logical_or(last_down, last_up))
    inner = jnp.logical_or(inner_up, inner_down)
    outer = jnp.logical_and(relay_over, jnp.logical_not(inner))
    drain(window.at[own_slot, 1], ALONG, inner)
    drain(window.at[own_slot, 1, pl.ds(sixth, 5 * sixth)], ALONG, outer)
    drain(halves.at[0], HALF)
    drain(partial.at[0], QUARTER)
    drain(fields.at[0], FIELD)
    drain(fields.at[pl.ds(0, 2)], FIELD_PAIR)
    for step in range(1, clusters):
        drain(parents.at[0], PARENT + step - 1)
    drain(line_out.at[0], LINE, jnp.logical_xor(above, below))
    drain(line_out, LINE, jnp.logical_and(above, below))
    ours = [handed(step, core) for step in steps] + [crossed(step) for step in steps]
    for_count(ours, lambda block: drain(block, COEFF_PARTNER))
    for_count([crossing(step) for step in steps], lambda block: drain(block, COEFF_BESIDE))
    up_count = [above] + [jnp.logical_and(exists(-hop), above) for hop in range(1, levels)]
    down_count = [below] + [jnp.logical_and(exists(hop), below) for hop in range(1, levels)]
    for_count(up_count, lambda block: drain(block, COEFF_ABOVE))
    for_count(down_count, lambda block: drain(block, COEFF_BELOW))


def finish_kernel(count_ref, acc_ref, out_ref, staged, sem):
    steps, rows = staged.shape[:2]
    half = acc_ref.shape[2]
    copies = []
    for step in range(steps):
        span = slice(step * rows, (step + 1) * rows)
        live = lax.broadcasted_iota(jnp.int32, (rows, half), 0) < count_ref[0, 0] - step * rows
        for part in range(2):
            columns = slice(part * half, (part + 1) * half)
            staged[step, :, columns] = jnp.where(live, acc_ref[part, span], 0.0)
        copy = pltpu.make_async_copy(staged.at[step], out_ref.at[span], sem.at[step])
        copy.start()
        copies.append(copy)
    for copy in copies:
        copy.wait()


def body(
    vectors,
    near_tiles,
    leaf_basis,
    transfer,
    coupling,
    top_coupling,
    near_list,
    far_list,
    row_counts,
):
    leaves = lax.axis_size("leaf")
    clusters = lax.axis_size("top")
    levels = leaves // 4
    rows, vecs = vectors.shape[2:]
    rank = transfer.shape[2]
    half, quarter = vecs // 2, vecs // 4
    smem = pl.BlockSpec(memory_space=pltpu.SMEM)
    vmem = pl.BlockSpec(memory_space=pltpu.VMEM)
    hbm = pl.BlockSpec(memory_space=pltpu.HBM)
    dma = pltpu.SemaphoreType.DMA
    acc = pl.pallas_call(
        functools.partial(exchange_kernel, levels, clusters),
        out_shape=jax.ShapeDtypeStruct((2, rows, half), jnp.float32),
        in_specs=[smem] + [hbm] * 8,
        out_specs=vmem,
        scratch_shapes=[
            pltpu.SMEM(near_list.shape, jnp.int32),
            pltpu.SMEM(far_list.shape, jnp.int32),
            pltpu.VMEM((2, rows, half), jnp.bfloat16),
            pltpu.VMEM(near_tiles.shape[2:], jnp.bfloat16),
            pltpu.VMEM(leaf_basis.shape[2:], jnp.bfloat16),
            pltpu.VMEM(transfer.shape[2:], jnp.bfloat16),
            pltpu.VMEM(coupling.shape[2:], jnp.bfloat16),
            pltpu.VMEM(top_coupling.shape[1:], jnp.bfloat16),
            pltpu.VMEM((SLOTS, 2, rows, half), jnp.bfloat16),
            pltpu.VMEM((leaves, rank, vecs), jnp.bfloat16),
            pltpu.VMEM((2, rank, half), jnp.float32),
            pltpu.VMEM((rank, half), jnp.float32),
            pltpu.VMEM((2, rank, quarter), jnp.float32),
            pltpu.VMEM((rank, quarter), jnp.float32),
            pltpu.VMEM((2, rank, quarter), jnp.float32),
            pltpu.VMEM((2, rank, quarter), jnp.float32),
            pltpu.VMEM((clusters, rank, quarter), jnp.bfloat16),
            pltpu.VMEM((4, rank, quarter), jnp.bfloat16),
            dma((9,)),
            dma((PARENT + clusters - 1,)),
            dma((ARRIVALS,)),
            dma((leaves // 2 + 1,)),
            dma((1,)),
            dma((1,)),
            dma((2,)),
            dma((clusters,)),
            dma((2,)),
        ],
        compiler_params=pltpu.CompilerParams(
            collective_id=0, has_side_effects=True, vmem_limit_bytes=48 * 1024 * 1024
        ),
    )(
        row_counts,
        *[
            pltpu.with_memory_space_constraint(array, pltpu.HBM)
            for array in (
                near_list,
                far_list,
                vectors,
                near_tiles,
                leaf_basis,
                transfer,
                coupling,
                top_coupling,
            )
        ],
    )
    result = pl.pallas_call(
        finish_kernel,
        out_shape=jax.ShapeDtypeStruct((rows, vecs), jnp.float32),
        in_specs=[smem, vmem],
        out_specs=pl.BlockSpec(memory_space=pl.ANY),
        scratch_shapes=[
            pltpu.VMEM((PIECES, rows // PIECES, vecs), jnp.float32),
            dma((PIECES,)),
        ],
        compiler_params=pltpu.CompilerParams(vmem_limit_bytes=8 * 1024 * 1024),
    )(row_counts, acc)
    return result[None, None]


def solution(mesh):
    in_specs = (
        P("top", "leaf", None, None),
        P("top", "leaf", None, None, None),
        P("top", "leaf", None, None),
        P("top", "leaf", None, None),
        P("top", "leaf", None, None, None),
        P("top", None, None, None),
        P("top", "leaf", None),
        P("top", "leaf", None),
        P("top", "leaf"),
    )
    out_specs = P("top", "leaf", None, None)
    return jax.shard_map(body, mesh=mesh, in_specs=in_specs, out_specs=out_specs, check_vma=False)
```

```python
import functools

import jax
import jax.numpy as jnp
from jax import lax
from jax.experimental import pallas as pl
from jax.experimental.pallas import tpu as pltpu
from jax.sharding import PartitionSpec as P

REACH = 4
SLOTS = 2 * REACH + 2
PIECES = 3
UNITS = 12
SPANS = ((8, 9), (0, 4), (4, 8), (9, 12))
BESIDE, BELOW, ABOVE, PARTNER, FAR_BESIDE, BRIDGED = 0, 2, 4, 6, 8, 10
DIAGONAL, FAR_DIAGONAL, SPAN = 12, 12 + PIECES, 12 + 2 * PIECES
FAR_SPAN = SPAN + len(SPANS)
ARRIVALS = FAR_SPAN + len(SPANS)
(
    TO_BESIDE,
    TO_ABOVE,
    TO_BELOW,
    TO_PARTNER,
    OVER,
    OVER_SPAN,
    ALONG,
    HAND_BESIDE,
    HAND_COLUMN,
    HAND_DIAGONAL,
    COEFF_ABOVE,
    COEFF_BELOW,
    COEFF_BESIDE,
    COEFF_PARTNER,
    HALF,
    QUARTER,
    LINE,
    TOTAL,
    FIELD,
    FIELD_PAIR,
    PARENT,
) = range(21)


def contract(left, right):
    return lax.dot_general(left, right, (((0,), (0,)), ((), ())), preferred_element_type=jnp.float32)


def dot(left, right):
    return jnp.dot(left, right, preferred_element_type=jnp.float32)


def exchange_kernel(
    levels,
    clusters,
    count_ref,
    near_source,
    far_source,
    vectors_ref,
    tiles_ref,
    basis_ref,
    nested_ref,
    coupling_ref,
    top_ref,
    acc,
    near_ref,
    far_ref,
    raw,
    tiles,
    basis,
    nested,
    coupling,
    top,
    window,
    coeffs,
    halves,
    half_in,
    partial,
    quarter_in,
    line_out,
    line_in,
    total_out,
    total_in,
    parents,
    fields,
    field_ref,
    load_sem,
    send_sem,
    block_sem,
    coeff_sem,
    half_sem,
    quarter_sem,
    line_sem,
    parent_sem,
    field_sem,
):
    me = lax.axis_index("leaf")
    cluster = lax.axis_index("top")
    core = lax.rem(me, 2)
    column = lax.rem(lax.div(me, 2), 2)
    level = lax.div(me, 4)
    other = 1 - core
    partner = me + 1 - 2 * core
    beside = me + 2 - 4 * column
    above = level < levels - 1
    below = level > 0
    first_column = column == 0
    rows, half = raw.shape[1:]
    vecs = 2 * half
    quarter = half // 2
    unit = rows // UNITS
    piece = rows // PIECES
    tile_count = tiles.shape[0]

    def load(source, target, sem):
        return pltpu.make_async_copy(source, target, sem)

    raw_loads = [
        load(vectors_ref.at[0, 0, :, pl.ds(part * half, half)], raw.at[part], load_sem.at[part])
        for part in range(2)
    ]
    basis_load = load(basis_ref.at[0, 0], basis, load_sem.at[2])
    nested_load = load(nested_ref.at[0, 0], nested, load_sem.at[7])
    coupling_load = load(coupling_ref.at[0, 0], coupling, load_sem.at[3])
    top_load = load(top_ref.at[0], top, load_sem.at[4])
    tile_loads = [load(tiles_ref.at[0, 0, k], tiles.at[k], load_sem.at[8]) for k in range(tile_count)]
    all_tiles = load(tiles_ref.at[0, 0], tiles, load_sem.at[8])
    near_load = load(near_source, near_ref, load_sem.at[5])
    far_load = load(far_source, far_ref, load_sem.at[6])

    barrier = pltpu.get_barrier_semaphore()

    def greet(peer):
        pl.semaphore_signal(barrier, inc=1, device_id=peer, device_id_type=pl.DeviceIdType.MESH)

    greet({"leaf": partner})
    greet({"leaf": beside})
    for step in range(1, clusters):
        greet({"top": lax.rem(cluster + step, clusters)})
    pl.when(above)(lambda: greet({"leaf": me + 4}))
    pl.when(below)(lambda: greet({"leaf": me - 4}))
    expected = clusters + 1 + above.astype(jnp.int32) + below.astype(jnp.int32)
    for copy in raw_loads + [basis_load, nested_load, near_load]:
        copy.start()

    def remote(source, target, sem, peer, done):
        return pltpu.make_async_remote_copy(
            src_ref=source,
            dst_ref=target,
            send_sem=send_sem.at[done],
            recv_sem=sem,
            device_id=peer,
            device_id_type=pl.DeviceIdType.MESH,
        )

    def send(source, target, sem, peer, done, condition=None):
        copy = remote(source, target, sem, peer, done)
        if condition is None:
            copy.start()
        else:
            pl.when(condition)(copy.start)

    def receive(block, sem, condition=None):
        copy = remote(block, block, sem, {"leaf": partner}, 0)
        if condition is None:
            copy.wait_recv()
        else:
            pl.when(condition)(copy.wait_recv)

    def drain(block, done, condition=None):
        copy = remote(block, block, block_sem.at[0], {"leaf": partner}, done)
        if condition is None:
            copy.wait_send()
        else:
            pl.when(condition)(copy.wait_send)

    to_partner, to_beside = {"leaf": partner}, {"leaf": beside}
    to_above, to_below = {"leaf": me + 4}, {"leaf": me - 4}

    own_slot = REACH + core
    partner_slot = REACH + other
    beside_slot = core + 6 - 4 * column
    diagonal_slot = core + 2 + 4 * column
    below_slot = core
    above_slot = core + 8
    diagonal = jnp.logical_or(
        jnp.logical_and(first_column, below), jnp.logical_and(column == 1, above)
    )
    relay_over = jnp.logical_or(
        jnp.logical_and(column == 1, below), jnp.logical_and(first_column, above)
    )
    relay_up = jnp.logical_and(first_column, above)
    relay_down = jnp.logical_and(column == 1, below)

    def send_block(slot, part, target, arrival, peer, done, condition=None):
        send(
            window.at[slot, part],
            window.at[target, part],
            block_sem.at[arrival + part],
            peer,
            done,
            condition,
        )

    def wait_block(slot, part, arrival, condition=None):
        receive(window.at[slot, part], block_sem.at[arrival + part], condition)

    def rows_of(index):
        return pl.ds(index * piece, piece)

    def span_of(index):
        start, stop = SPANS[index]
        return pl.ds(start * unit, (stop - start) * unit)

    def send_rows(slot, part, span, target, arrival, peer, done, condition=None):
        send(
            window.at[slot, part, span],
            window.at[target, part, span],
            block_sem.at[arrival],
            peer,
            done,
            condition,
        )

    def wait_rows(slot, part, span, arrival, condition=None):
        receive(window.at[slot, part, span], block_sem.at[arrival], condition)

    def send_coeff(leaf, peer, done, condition=None):
        send(coeffs.at[leaf], coeffs.at[leaf], coeff_sem.at[lax.div(leaf, 2)], peer, done, condition)

    def hand_coeff(leaf, condition):
        send(
            coeffs.at[leaf],
            coeffs.at[leaf],
            coeff_sem.at[2 * levels],
            to_partner,
            COEFF_PARTNER,
            condition,
        )

    def wait_coeff(leaf, condition=None):
        receive(coeffs.at[leaf], coeff_sem.at[lax.div(leaf, 2)], condition)

    def for_count(conditions, run):
        count = 0
        for condition in conditions:
            count = count + jnp.where(condition, 1, 0)
        for n in range(1, len(conditions) + 1):
            pl.when(count == n)(lambda n=n: run(coeffs.at[pl.ds(0, n)]))

    def exists(step):
        return jnp.logical_and(level + step >= 0, level + step < levels)

    def crosses(step, from_first):
        return step <= -1 or step >= 2 if from_first else step >= 1 or step <= -2

    def crossing(step):
        if crosses(step, True) and crosses(step, False):
            return exists(step)
        return jnp.logical_and(exists(step), first_column if crosses(step, True) else column == 1)

    def crossed(step):
        if crosses(step, True) and crosses(step, False):
            return exists(step)
        return jnp.logical_and(exists(step), column == 1 if crosses(step, True) else first_column)

    def handed(step, which):
        if abs(step) >= 2:
            return exists(step)
        return jnp.logical_and(exists(step), which == (1 if step == 1 else 0))

    def relay_coeffs(hop):
        for step in (-hop, hop):
            wait_coeff(me + 4 * step, exists(step))
        if hop + 1 < levels:
            send_coeff(me - 4 * hop, to_above, COEFF_ABOVE, jnp.logical_and(exists(-hop), above))
            send_coeff(me + 4 * hop, to_below, COEFF_BELOW, jnp.logical_and(exists(hop), below))

    def cross_coeffs(hop):
        for step in (-hop, hop):
            send_coeff(me + 4 * step, to_beside, COEFF_BESIDE, crossing(step))
            hand_coeff(me + 4 * step, handed(step, core))

    def hand_crossed(hop):
        for step in (-hop, hop):
            wait_coeff(beside + 4 * step, crossed(step))
            hand_coeff(beside + 4 * step, crossed(step))

    def far_product(part):
        return dot(basis[...], field_ref[:, part * half : (part + 1) * half])

    def near(slot, part, condition=None, first=False, span=None, far=False):
        offset = slot - REACH - core
        place, hit = 0, 0
        for k in range(tile_count):
            here = near_ref[0, 0, k] == offset
            place = jnp.where(here, k, place)
            hit = jnp.where(here, 1, hit)
        scale = hit.astype(jnp.float32)

        def run():
            if span is None:
                product = dot(tiles[place], window[slot, part]) * scale
            else:
                lines = slice(span[0] * unit, span[1] * unit)
                product = dot(tiles[place, :, lines], window[slot, part, lines, :]) * scale
            if far:
                product = product + far_product(part)
            if first:
                acc[part] = product
            else:
                acc[part] += product

        if condition is None:
            run()
        else:
            pl.when(condition)(run)

    own_beside = own_slot + 4 * column - 2

    def send_own(part, index):
        span = rows_of(index)
        send_rows(own_slot, part, span, core, BELOW + part, to_above, TO_ABOVE, above)
        send_rows(own_slot, part, span, core + 8, ABOVE + part, to_below, TO_BELOW, below)

    def send_first(index):
        send_rows(own_slot, 0, rows_of(index), own_beside, BESIDE, to_beside, TO_BESIDE)

    live = lax.broadcasted_iota(jnp.int32, (rows, half), 0) < count_ref[0, 0]

    def mask(part):
        raw_loads[part].wait()
        window[own_slot, part] = jnp.where(live, raw[part], jnp.zeros((), jnp.bfloat16))

    mask(0)
    pl.semaphore_wait(barrier, expected)
    for index in range(PIECES - 1):
        send_first(index)
    send_own(0, 0)
    mask(1)
    basis_load.wait()
    for part in range(2):
        product = contract(basis[...], window[own_slot, part])
        coeffs[me, :, part * half : (part + 1) * half] = product.astype(jnp.bfloat16)
    nested_load.wait()
    for part in range(2):
        halves[part] = contract(nested[...], coeffs[me, :, part * half : (part + 1) * half])
    send_coeff(me, to_above, COEFF_ABOVE, above)
    send_coeff(me, to_below, COEFF_BELOW, below)
    for index in range(1, PIECES):
        send_own(0, index)
    send(halves.at[other], half_in, half_sem.at[0], to_partner, HALF)
    for part in range(2):
        send_block(own_slot, part, own_slot, PARTNER, to_partner, TO_PARTNER)
    for copy in tile_loads + [far_load, coupling_load, top_load]:
        copy.start()

    receive(half_in, half_sem.at[0])
    total = halves[core] + half_in[...]
    for part in range(2):
        partial[part] = total[:, part * quarter : (part + 1) * quarter]
    send(partial.at[1 - column], quarter_in, quarter_sem.at[0], to_beside, QUARTER)
    send_first(PIECES - 1)
    near_load.wait()
    all_tiles.wait()
    near(own_slot, 0, first=True)
    near(own_slot, 1, first=True)
    for part in range(2):
        wait_block(partner_slot, part, PARTNER)
        near(partner_slot, part)

    relay_coeffs(1)
    cross_coeffs(1)
    send_block(own_slot, 1, own_beside, BESIDE, to_beside, TO_BESIDE)
    receive(quarter_in, quarter_sem.at[0])
    partial[column] += quarter_in[...]

    def line(turn):
        ways = ((0, turn - 1, 4), (1, levels - turn, -4))
        whole = 2 < levels == turn + 1
        if turn > 1:
            for way, at, _ in ways:
                block = total_in if 2 < levels == turn else line_in.at[way]
                receive(block, line_sem.at[way], level == at)
        if turn < levels:
            for way, at, step in ways:

                @pl.when(level == at)
                def _(way=way):
                    value = partial[column]
                    if turn > 1:
                        value = value + line_in[way]
                    if whole:
                        value = value + line_in[1 - way]
                        total_out[way] = value.astype(jnp.bfloat16)
                    else:
                        line_out[way] = value

                peer = {"leaf": me + step}
                if whole:
                    send(total_out.at[way], total_in, line_sem.at[way], peer, TOTAL, level == at)
                else:
                    send(line_out.at[way], line_in.at[way], line_sem.at[way], peer, LINE, level == at)

    line(1)
    send_own(1, 0)

    bridged_slot = jnp.where(core == 0, 1, 8)
    bridged = jnp.logical_or(
        jnp.logical_and(core == 0, below), jnp.logical_and(core == 1, above)
    )
    hand_below = jnp.logical_and(core == 1, below)
    hand_above = jnp.logical_and(core == 0, above)
    far_beside_slot = other + 6 - 4 * column
    far_diagonal_slot = other + 2 + 4 * column

    def hand_neighbours(part):
        send_block(below_slot, part, below_slot, BRIDGED, to_partner, HAND_COLUMN, hand_below)
        send_block(above_slot, part, above_slot, BRIDGED, to_partner, HAND_COLUMN, hand_above)

    def send_over(index):
        span = rows_of(index)
        arrival = DIAGONAL + index
        send_rows(below_slot, 0, span, core + 2, arrival, to_beside, OVER, relay_down)
        send_rows(above_slot, 0, span, core + 6, arrival, to_beside, OVER, relay_up)

    wait_block(beside_slot, 0, BESIDE)
    send_block(beside_slot, 0, beside_slot, FAR_BESIDE, to_partner, HAND_BESIDE)
    near(beside_slot, 0)
    wait_block(below_slot, 0, BELOW, below)
    wait_block(above_slot, 0, ABOVE, above)
    hand_neighbours(0)
    near(below_slot, 0, below)
    near(above_slot, 0, above)
    line(2)
    send_own(1, 1)

    hand_crossed(1)
    if levels > 2:
        relay_coeffs(2)
        cross_coeffs(2)
    for index in range(PIECES - 1):
        send_over(index)
    wait_block(far_beside_slot, 0, FAR_BESIDE)
    near(far_beside_slot, 0)
    wait_block(bridged_slot, 0, BRIDGED, bridged)
    near(bridged_slot, 0, bridged)
    for turn in range(3, levels):
        line(turn)
    send_own(1, 2)

    wait_block(beside_slot, 1, BESIDE)
    inner_up = jnp.logical_and(relay_up, level < levels - 2)
    inner_down = jnp.logical_and(relay_down, level > 1)

    def send_span(slot, index, target, peer, done, condition):
        span = span_of(index)
        send_rows(slot, 1, span, target, SPAN + index, peer, done, condition)

    for index in range(len(SPANS)):
        up, down = (inner_up, inner_down) if index == 0 else (relay_up, relay_down)
        send_span(beside_slot, index, core + 2, to_above, ALONG, up)
        send_span(beside_slot, index, core + 6, to_below, ALONG, down)
    send_block(beside_slot, 1, beside_slot, FAR_BESIDE, to_partner, HAND_BESIDE)
    near(beside_slot, 1)
    for hop in range(3, levels):
        relay_coeffs(hop)
        cross_coeffs(hop)
    if levels > 2:
        line(levels)
    whole = partial[column]
    for way, condition in ((0, below), (1, above)):
        whole = whole + jnp.where(condition, line_in[way], 0.0)
    whole = whole.astype(jnp.bfloat16)
    if levels > 2:
        whole = jnp.where(jnp.logical_xor(above, below), total_in[...], whole)
    parents[cluster] = whole
    for step in range(1, clusters):
        send(
            parents.at[cluster],
            parents.at[cluster],
            parent_sem.at[cluster],
            {"top": lax.rem(cluster + step, clusters)},
            PARENT + step - 1,
        )
    wait_block(far_beside_slot, 1, FAR_BESIDE)
    near(far_beside_slot, 1)
    coupling_load.wait()
    top_load.wait()
    for step in range(1, clusters):
        source = lax.rem(cluster + step, clusters)
        receive(parents.at[source], parent_sem.at[source])
    over = jnp.zeros(parents.shape[1:], jnp.float32)
    for m in range(top.shape[0]):
        over = over + dot(top[m], parents[lax.rem(cluster + 1 + m, clusters)])
    place = 2 * core + column
    fields[place] = over.astype(jnp.bfloat16)
    send(fields.at[place], fields.at[place], field_sem.at[0], to_beside, FIELD)
    send_over(PIECES - 1)
    if levels > 2:
        hand_crossed(2)
    wait_block(below_slot, 1, BELOW, below)
    wait_block(above_slot, 1, ABOVE, above)
    last_down = jnp.logical_and(relay_down, level == levels - 1)
    last_up = jnp.logical_and(relay_up, level == 0)
    send_span(below_slot, 0, core + 2, to_beside, OVER_SPAN, last_down)
    send_span(above_slot, 0, core + 6, to_beside, OVER_SPAN, last_up)
    hand_neighbours(1)
    near(below_slot, 1, below)
    near(above_slot, 1, above)

    def hand_first(index):
        span = rows_of(index)
        arrival = FAR_DIAGONAL + index
        wait_rows(diagonal_slot, 0, span, DIAGONAL + index, diagonal)
        send_rows(diagonal_slot, 0, span, diagonal_slot, arrival, to_partner, HAND_DIAGONAL, diagonal)

    def own_first(index, far=False):
        near(diagonal_slot, 0, diagonal, span=third(index), far=far)

    def far_first(index):
        wait_rows(far_diagonal_slot, 0, rows_of(index), FAR_DIAGONAL + index, diagonal)
        near(far_diagonal_slot, 0, diagonal, span=third(index))

    def third(index):
        return (index * UNITS // PIECES, (index + 1) * UNITS // PIECES)

    def wait_span(slot, index, arrival):
        wait_rows(slot, 1, span_of(index), arrival + index, diagonal)

    def hand_second(index):
        span = span_of(index)
        arrival = FAR_SPAN + index
        wait_span(diagonal_slot, index, SPAN)
        send_rows(diagonal_slot, 1, span, diagonal_slot, arrival, to_partner, HAND_DIAGONAL, diagonal)

    middle, later, ends = (0, 4), (4, 8), (8, 12)

    def own_second(span, far=False):
        near(diagonal_slot, 1, diagonal, span=span, far=far)

    def far_second(span):
        near(far_diagonal_slot, 1, diagonal, span=span)

    hand_first(0)
    own_first(0)
    wait_block(bridged_slot, 1, BRIDGED, bridged)
    near(bridged_slot, 1, bridged)
    hand_second(1)
    own_second(middle)
    hand_first(1)
    own_first(1)
    far_first(0)
    wait_span(far_diagonal_slot, 1, FAR_SPAN)
    far_second(middle)
    next_place = 2 * core + 1 - column
    receive(fields.at[next_place], field_sem.at[0])
    pair = fields.at[pl.ds(2 * core, 2)]
    send(pair, pair, field_sem.at[1], to_partner, FIELD_PAIR)
    for hop in range(3, levels):
        hand_crossed(hop)
    far_first(1)
    hand_second(2)
    own_second(later)

    steps = [step for hop in range(1, levels) for step in (-hop, hop)]
    theirs_count = [handed(step, other) for step in steps] + [crossed(step) for step in steps]
    for_count(theirs_count, lambda block: receive(block, coeff_sem.at[2 * levels]))
    theirs = fields.at[pl.ds(2 * other, 2)]
    receive(theirs, field_sem.at[1])
    far_load.wait()
    field = dot(nested[...], jnp.concatenate([fields[k] for k in range(4)], axis=1))
    for m in range(coupling.shape[0]):
        field = field + dot(coupling[m], coeffs[far_ref[0, 0, m]])
    field_ref[...] = field.astype(jnp.bfloat16)

    @pl.when(jnp.logical_not(diagonal))
    def _():
        for part in range(2):
            acc[part] += far_product(part)


    hand_first(2)
    own_first(2, far=True)
    hand_second(3)
    wait_span(far_diagonal_slot, 2, FAR_SPAN)
    far_second(later)
    hand_second(0)
    own_second(ends, far=True)
    far_first(2)
    wait_span(far_diagonal_slot, 3, FAR_SPAN)
    wait_span(far_diagonal_slot, 0, FAR_SPAN)
    far_second(ends)

    whole_block = window.at[own_slot]
    for done, condition in (
        (TO_BESIDE, None),
        (TO_ABOVE, above),
        (TO_BELOW, below),
        (TO_PARTNER, None),
        (HAND_BESIDE, None),
        (HAND_COLUMN, jnp.logical_or(hand_below, hand_above)),
    ):
        drain(whole_block, done, condition)
    drain(window.at[own_slot, 0], OVER, relay_over)

    def drain_units(units, done, condition):
        drain(window.at[own_slot, 1, pl.ds(0, units * unit)], done, condition)

    inner = jnp.logical_or(inner_up, inner_down)
    outer = jnp.logical_and(relay_over, jnp.logical_not(inner))
    last = jnp.logical_or(last_down, last_up)
    drain_units(1, OVER_SPAN, last)
    drain_units(UNITS, ALONG, inner)
    drain_units(UNITS - 1, ALONG, outer)
    drain(whole_block, HAND_DIAGONAL, diagonal)
    drain(halves.at[0], HALF)
    drain(partial.at[0], QUARTER)
    drain(fields.at[0], FIELD)
    drain(fields.at[pl.ds(0, 2)], FIELD_PAIR)
    for step in range(1, clusters):
        drain(parents.at[0], PARENT + step - 1)
    totals = [level == 1, level == levels - 2] if levels > 2 else [below & False] * 2
    lines = [
        jnp.logical_and(neighbour, jnp.logical_not(total))
        for neighbour, total in zip((below, above), totals)
    ]
    drain_pair = ((line_out, LINE, lines), (total_out, TOTAL, totals))
    for block, done, (one, two) in drain_pair:
        drain(block.at[0], done, jnp.logical_xor(one, two))
        drain(block, done, jnp.logical_and(one, two))
    ours = [handed(step, core) for step in steps] + [crossed(step) for step in steps]
    for_count(ours, lambda block: drain(block, COEFF_PARTNER))
    for_count([crossing(step) for step in steps], lambda block: drain(block, COEFF_BESIDE))
    up_count = [above] + [jnp.logical_and(exists(-hop), above) for hop in range(1, levels)]
    down_count = [below] + [jnp.logical_and(exists(hop), below) for hop in range(1, levels)]
    for_count(up_count, lambda block: drain(block, COEFF_ABOVE))
    for_count(down_count, lambda block: drain(block, COEFF_BELOW))


def finish_kernel(count_ref, acc_ref, out_ref, staged, sem):
    steps, rows = staged.shape[:2]
    half = acc_ref.shape[2]
    copies = []
    for step in range(steps):
        span = slice(step * rows, (step + 1) * rows)
        live = lax.broadcasted_iota(jnp.int32, (rows, half), 0) < count_ref[0, 0] - step * rows
        for part in range(2):
            columns = slice(part * half, (part + 1) * half)
            staged[step, :, columns] = jnp.where(live, acc_ref[part, span], 0.0)
        copy = pltpu.make_async_copy(staged.at[step], out_ref.at[span], sem.at[step])
        copy.start()
        copies.append(copy)
    for copy in copies:
        copy.wait()


def body(
    vectors,
    near_tiles,
    leaf_basis,
    transfer,
    coupling,
    top_coupling,
    near_list,
    far_list,
    row_counts,
):
    leaves = lax.axis_size("leaf")
    clusters = lax.axis_size("top")
    levels = leaves // 4
    rows, vecs = vectors.shape[2:]
    rank = transfer.shape[2]
    half, quarter = vecs // 2, vecs // 4
    smem = pl.BlockSpec(memory_space=pltpu.SMEM)
    vmem = pl.BlockSpec(memory_space=pltpu.VMEM)
    hbm = pl.BlockSpec(memory_space=pltpu.HBM)
    dma = pltpu.SemaphoreType.DMA
    acc = pl.pallas_call(
        functools.partial(exchange_kernel, levels, clusters),
        out_shape=jax.ShapeDtypeStruct((2, rows, half), jnp.float32),
        in_specs=[smem] + [hbm] * 8,
        out_specs=vmem,
        scratch_shapes=[
            pltpu.SMEM(near_list.shape, jnp.int32),
            pltpu.SMEM(far_list.shape, jnp.int32),
            pltpu.VMEM((2, rows, half), jnp.bfloat16),
            pltpu.VMEM(near_tiles.shape[2:], jnp.bfloat16),
            pltpu.VMEM(leaf_basis.shape[2:], jnp.bfloat16),
            pltpu.VMEM(transfer.shape[2:], jnp.bfloat16),
            pltpu.VMEM(coupling.shape[2:], jnp.bfloat16),
            pltpu.VMEM(top_coupling.shape[1:], jnp.bfloat16),
            pltpu.VMEM((SLOTS, 2, rows, half), jnp.bfloat16),
            pltpu.VMEM((leaves, rank, vecs), jnp.bfloat16),
            pltpu.VMEM((2, rank, half), jnp.float32),
            pltpu.VMEM((rank, half), jnp.float32),
            pltpu.VMEM((2, rank, quarter), jnp.float32),
            pltpu.VMEM((rank, quarter), jnp.float32),
            pltpu.VMEM((2, rank, quarter), jnp.float32),
            pltpu.VMEM((2, rank, quarter), jnp.float32),
            pltpu.VMEM((2, rank, quarter), jnp.bfloat16),
            pltpu.VMEM((rank, quarter), jnp.bfloat16),
            pltpu.VMEM((clusters, rank, quarter), jnp.bfloat16),
            pltpu.VMEM((4, rank, quarter), jnp.bfloat16),
            pltpu.VMEM((rank, vecs), jnp.bfloat16),
            dma((9,)),
            dma((PARENT + clusters - 1,)),
            dma((ARRIVALS,)),
            dma((leaves // 2 + 1,)),
            dma((1,)),
            dma((1,)),
            dma((2,)),
            dma((clusters,)),
            dma((2,)),
        ],
        compiler_params=pltpu.CompilerParams(
            collective_id=0, has_side_effects=True, vmem_limit_bytes=48 * 1024 * 1024
        ),
    )(
        row_counts,
        *[
            pltpu.with_memory_space_constraint(array, pltpu.HBM)
            for array in (
                near_list,
                far_list,
                vectors,
                near_tiles,
                leaf_basis,
                transfer,
                coupling,
                top_coupling,
            )
        ],
    )
    result = pl.pallas_call(
        finish_kernel,
        out_shape=jax.ShapeDtypeStruct((rows, vecs), jnp.float32),
        in_specs=[smem, vmem],
        out_specs=pl.BlockSpec(memory_space=pl.ANY),
        scratch_shapes=[
            pltpu.VMEM((PIECES, rows // PIECES, vecs), jnp.float32),
            dma((PIECES,)),
        ],
        compiler_params=pltpu.CompilerParams(vmem_limit_bytes=8 * 1024 * 1024),
    )(row_counts, acc)
    return result[None, None]


def solution(mesh):
    in_specs = (
        P("top", "leaf", None, None),
        P("top", "leaf", None, None, None),
        P("top", "leaf", None, None),
        P("top", "leaf", None, None),
        P("top", "leaf", None, None, None),
        P("top", None, None, None),
        P("top", "leaf", None),
        P("top", "leaf", None),
        P("top", "leaf"),
    )
    out_specs = P("top", "leaf", None, None)
    return jax.shard_map(body, mesh=mesh, in_specs=in_specs, out_specs=out_specs, check_vma=False)
```

```python
import functools

import jax
import jax.numpy as jnp
from jax import lax
from jax.experimental import pallas as pl
from jax.experimental.pallas import tpu as pltpu
from jax.sharding import PartitionSpec as P

REACH = 4
SLOTS = 2 * REACH + 2
PIECES = 3
UNITS = 12
SPANS = ((8, 9), (0, 4), (4, 8), (9, 11), (11, 12))
BESIDE, BELOW, ABOVE, PARTNER, FAR_BESIDE, BRIDGED = 0, 2, 4, 6, 8, 10
DIAGONAL, FAR_DIAGONAL, SPAN = 12, 12 + PIECES, 12 + 2 * PIECES
FAR_SPAN = SPAN + len(SPANS)
ARRIVALS = FAR_SPAN + len(SPANS)
(
    TO_BESIDE,
    TO_ABOVE,
    TO_BELOW,
    TO_PARTNER,
    OVER,
    OVER_SPAN,
    ALONG,
    HAND_BESIDE,
    HAND_COLUMN,
    HAND_DIAGONAL,
    COEFF_ABOVE,
    COEFF_BELOW,
    COEFF_BESIDE,
    COEFF_PARTNER,
    HALF,
    QUARTER,
    LINE,
    TOTAL,
    FIELD,
    FIELD_PAIR,
    PARENT,
) = range(21)


def contract(left, right):
    return lax.dot_general(left, right, (((0,), (0,)), ((), ())), preferred_element_type=jnp.float32)


def dot(left, right):
    return jnp.dot(left, right, preferred_element_type=jnp.float32)


def exchange_kernel(
    levels,
    clusters,
    count_ref,
    near_source,
    far_source,
    vectors_ref,
    tiles_ref,
    basis_ref,
    nested_ref,
    coupling_ref,
    top_ref,
    acc,
    near_ref,
    far_ref,
    raw,
    tiles,
    basis,
    nested,
    coupling,
    top,
    window,
    coeffs,
    halves,
    half_in,
    partial,
    quarter_in,
    line_out,
    line_in,
    total_out,
    total_in,
    parents,
    fields,
    field_ref,
    load_sem,
    send_sem,
    block_sem,
    coeff_sem,
    half_sem,
    quarter_sem,
    line_sem,
    parent_sem,
    field_sem,
):
    me = lax.axis_index("leaf")
    cluster = lax.axis_index("top")
    core = lax.rem(me, 2)
    column = lax.rem(lax.div(me, 2), 2)
    level = lax.div(me, 4)
    other = 1 - core
    partner = me + 1 - 2 * core
    beside = me + 2 - 4 * column
    above = level < levels - 1
    below = level > 0
    first_column = column == 0
    rows, half = raw.shape[1:]
    vecs = 2 * half
    quarter = half // 2
    unit = rows // UNITS
    piece = rows // PIECES
    tile_count = tiles.shape[0]

    def load(source, target, sem):
        return pltpu.make_async_copy(source, target, sem)

    raw_loads = [
        load(vectors_ref.at[0, 0, :, pl.ds(part * half, half)], raw.at[part], load_sem.at[part])
        for part in range(2)
    ]
    basis_load = load(basis_ref.at[0, 0], basis, load_sem.at[2])
    nested_load = load(nested_ref.at[0, 0], nested, load_sem.at[7])
    coupling_load = load(coupling_ref.at[0, 0], coupling, load_sem.at[3])
    top_load = load(top_ref.at[0], top, load_sem.at[4])
    tile_loads = [load(tiles_ref.at[0, 0, k], tiles.at[k], load_sem.at[8]) for k in range(tile_count)]
    all_tiles = load(tiles_ref.at[0, 0], tiles, load_sem.at[8])
    near_load = load(near_source, near_ref, load_sem.at[5])
    far_load = load(far_source, far_ref, load_sem.at[6])

    barrier = pltpu.get_barrier_semaphore()

    def greet(peer):
        pl.semaphore_signal(barrier, inc=1, device_id=peer, device_id_type=pl.DeviceIdType.MESH)

    greet({"leaf": partner})
    greet({"leaf": beside})
    for step in range(1, clusters):
        greet({"top": lax.rem(cluster + step, clusters)})
    pl.when(above)(lambda: greet({"leaf": me + 4}))
    pl.when(below)(lambda: greet({"leaf": me - 4}))
    expected = clusters + 1 + above.astype(jnp.int32) + below.astype(jnp.int32)
    for copy in raw_loads + [basis_load, nested_load, near_load]:
        copy.start()

    def remote(source, target, sem, peer, done):
        return pltpu.make_async_remote_copy(
            src_ref=source,
            dst_ref=target,
            send_sem=send_sem.at[done],
            recv_sem=sem,
            device_id=peer,
            device_id_type=pl.DeviceIdType.MESH,
        )

    def send(source, target, sem, peer, done, condition=None):
        copy = remote(source, target, sem, peer, done)
        if condition is None:
            copy.start()
        else:
            pl.when(condition)(copy.start)

    def receive(block, sem, condition=None):
        copy = remote(block, block, sem, {"leaf": partner}, 0)
        if condition is None:
            copy.wait_recv()
        else:
            pl.when(condition)(copy.wait_recv)

    def drain(block, done, condition=None):
        copy = remote(block, block, block_sem.at[0], {"leaf": partner}, done)
        if condition is None:
            copy.wait_send()
        else:
            pl.when(condition)(copy.wait_send)

    to_partner, to_beside = {"leaf": partner}, {"leaf": beside}
    to_above, to_below = {"leaf": me + 4}, {"leaf": me - 4}

    own_slot = REACH + core
    partner_slot = REACH + other
    beside_slot = core + 6 - 4 * column
    diagonal_slot = core + 2 + 4 * column
    below_slot = core
    above_slot = core + 8
    diagonal = jnp.logical_or(
        jnp.logical_and(first_column, below), jnp.logical_and(column == 1, above)
    )
    relay_over = jnp.logical_or(
        jnp.logical_and(column == 1, below), jnp.logical_and(first_column, above)
    )
    relay_up = jnp.logical_and(first_column, above)
    relay_down = jnp.logical_and(column == 1, below)

    def send_block(slot, part, target, arrival, peer, done, condition=None):
        send(
            window.at[slot, part],
            window.at[target, part],
            block_sem.at[arrival + part],
            peer,
            done,
            condition,
        )

    def wait_block(slot, part, arrival, condition=None):
        receive(window.at[slot, part], block_sem.at[arrival + part], condition)

    def rows_of(index):
        return pl.ds(index * piece, piece)

    def span_of(index):
        start, stop = SPANS[index]
        return pl.ds(start * unit, (stop - start) * unit)

    def send_rows(slot, part, span, target, arrival, peer, done, condition=None):
        send(
            window.at[slot, part, span],
            window.at[target, part, span],
            block_sem.at[arrival],
            peer,
            done,
            condition,
        )

    def wait_rows(slot, part, span, arrival, condition=None):
        receive(window.at[slot, part, span], block_sem.at[arrival], condition)

    def send_coeff(leaf, peer, done, condition=None):
        send(coeffs.at[leaf], coeffs.at[leaf], coeff_sem.at[lax.div(leaf, 2)], peer, done, condition)

    def hand_coeff(leaf, condition):
        send(
            coeffs.at[leaf],
            coeffs.at[leaf],
            coeff_sem.at[2 * levels],
            to_partner,
            COEFF_PARTNER,
            condition,
        )

    def wait_coeff(leaf, condition=None):
        receive(coeffs.at[leaf], coeff_sem.at[lax.div(leaf, 2)], condition)

    def for_count(conditions, run):
        count = 0
        for condition in conditions:
            count = count + jnp.where(condition, 1, 0)
        for n in range(1, len(conditions) + 1):
            pl.when(count == n)(lambda n=n: run(coeffs.at[pl.ds(0, n)]))

    def exists(step):
        return jnp.logical_and(level + step >= 0, level + step < levels)

    def crosses(step, from_first):
        return step <= -1 or step >= 2 if from_first else step >= 1 or step <= -2

    def crossing(step):
        if crosses(step, True) and crosses(step, False):
            return exists(step)
        return jnp.logical_and(exists(step), first_column if crosses(step, True) else column == 1)

    def crossed(step):
        if crosses(step, True) and crosses(step, False):
            return exists(step)
        return jnp.logical_and(exists(step), column == 1 if crosses(step, True) else first_column)

    def handed(step, which):
        if abs(step) >= 2:
            return exists(step)
        return jnp.logical_and(exists(step), which == (1 if step == 1 else 0))

    def relay_coeffs(hop):
        for step in (-hop, hop):
            wait_coeff(me + 4 * step, exists(step))
        if hop + 1 < levels:
            send_coeff(me - 4 * hop, to_above, COEFF_ABOVE, jnp.logical_and(exists(-hop), above))
            send_coeff(me + 4 * hop, to_below, COEFF_BELOW, jnp.logical_and(exists(hop), below))

    def cross_coeffs(hop):
        for step in (-hop, hop):
            send_coeff(me + 4 * step, to_beside, COEFF_BESIDE, crossing(step))
            hand_coeff(me + 4 * step, handed(step, core))

    def hand_crossed(hop):
        for step in (-hop, hop):
            wait_coeff(beside + 4 * step, crossed(step))
            hand_coeff(beside + 4 * step, crossed(step))

    def far_product(part):
        return dot(basis[...], field_ref[:, part * half : (part + 1) * half])

    def near(slot, part, condition=None, first=False, span=None, far=False):
        offset = slot - REACH - core
        place, hit = 0, 0
        for k in range(tile_count):
            here = near_ref[0, 0, k] == offset
            place = jnp.where(here, k, place)
            hit = jnp.where(here, 1, hit)
        scale = hit.astype(jnp.float32)

        def run():
            if span is None:
                product = dot(tiles[place], window[slot, part]) * scale
            else:
                lines = slice(span[0] * unit, span[1] * unit)
                product = dot(tiles[place, :, lines], window[slot, part, lines, :]) * scale
            if far:
                product = product + far_product(part)
            if first:
                acc[part] = product
            else:
                acc[part] += product

        if condition is None:
            run()
        else:
            pl.when(condition)(run)

    own_beside = own_slot + 4 * column - 2

    def send_own(part, index):
        span = rows_of(index)
        send_rows(own_slot, part, span, core, BELOW + part, to_above, TO_ABOVE, above)
        send_rows(own_slot, part, span, core + 8, ABOVE + part, to_below, TO_BELOW, below)

    def send_first(index):
        send_rows(own_slot, 0, rows_of(index), own_beside, BESIDE, to_beside, TO_BESIDE)

    live = lax.broadcasted_iota(jnp.int32, (rows, half), 0) < count_ref[0, 0]

    def mask(part):
        raw_loads[part].wait()
        window[own_slot, part] = jnp.where(live, raw[part], jnp.zeros((), jnp.bfloat16))

    mask(0)
    pl.semaphore_wait(barrier, expected)
    for index in range(PIECES - 1):
        send_first(index)
    send_own(0, 0)
    mask(1)
    basis_load.wait()
    for part in range(2):
        product = contract(basis[...], window[own_slot, part])
        coeffs[me, :, part * half : (part + 1) * half] = product.astype(jnp.bfloat16)
    nested_load.wait()
    for part in range(2):
        halves[part] = contract(nested[...], coeffs[me, :, part * half : (part + 1) * half])
    send_coeff(me, to_above, COEFF_ABOVE, above)
    send_coeff(me, to_below, COEFF_BELOW, below)
    for index in range(1, PIECES):
        send_own(0, index)
    send(halves.at[other], half_in, half_sem.at[0], to_partner, HALF)
    for part in range(2):
        send_block(own_slot, part, own_slot, PARTNER, to_partner, TO_PARTNER)
    for copy in tile_loads + [far_load, coupling_load, top_load]:
        copy.start()

    receive(half_in, half_sem.at[0])
    total = halves[core] + half_in[...]
    for part in range(2):
        partial[part] = total[:, part * quarter : (part + 1) * quarter]
    send(partial.at[1 - column], quarter_in, quarter_sem.at[0], to_beside, QUARTER)
    send_first(PIECES - 1)
    near_load.wait()
    all_tiles.wait()
    near(own_slot, 0, first=True)
    near(own_slot, 1, first=True)
    for part in range(2):
        wait_block(partner_slot, part, PARTNER)
        near(partner_slot, part)

    relay_coeffs(1)
    cross_coeffs(1)
    send_block(own_slot, 1, own_beside, BESIDE, to_beside, TO_BESIDE)
    receive(quarter_in, quarter_sem.at[0])
    partial[column] += quarter_in[...]

    def line(turn):
        ways = ((0, turn - 1, 4), (1, levels - turn, -4))
        whole = 2 < levels == turn + 1
        if turn > 1:
            for way, at, _ in ways:
                block = total_in if 2 < levels == turn else line_in.at[way]
                receive(block, line_sem.at[way], level == at)
        if turn < levels:
            for way, at, step in ways:

                @pl.when(level == at)
                def _(way=way):
                    value = partial[column]
                    if turn > 1:
                        value = value + line_in[way]
                    if whole:
                        value = value + line_in[1 - way]
                        total_out[way] = value.astype(jnp.bfloat16)
                    else:
                        line_out[way] = value

                peer = {"leaf": me + step}
                if whole:
                    send(total_out.at[way], total_in, line_sem.at[way], peer, TOTAL, level == at)
                else:
                    send(line_out.at[way], line_in.at[way], line_sem.at[way], peer, LINE, level == at)

    line(1)
    send_own(1, 0)

    bridged_slot = jnp.where(core == 0, 1, 8)
    bridged = jnp.logical_or(
        jnp.logical_and(core == 0, below), jnp.logical_and(core == 1, above)
    )
    hand_below = jnp.logical_and(core == 1, below)
    hand_above = jnp.logical_and(core == 0, above)
    far_beside_slot = other + 6 - 4 * column
    far_diagonal_slot = other + 2 + 4 * column

    def hand_neighbours(part):
        send_block(below_slot, part, below_slot, BRIDGED, to_partner, HAND_COLUMN, hand_below)
        send_block(above_slot, part, above_slot, BRIDGED, to_partner, HAND_COLUMN, hand_above)

    def send_over(index):
        span = rows_of(index)
        arrival = DIAGONAL + index
        send_rows(below_slot, 0, span, core + 2, arrival, to_beside, OVER, relay_down)
        send_rows(above_slot, 0, span, core + 6, arrival, to_beside, OVER, relay_up)

    wait_block(beside_slot, 0, BESIDE)
    send_block(beside_slot, 0, beside_slot, FAR_BESIDE, to_partner, HAND_BESIDE)
    near(beside_slot, 0)
    wait_block(below_slot, 0, BELOW, below)
    wait_block(above_slot, 0, ABOVE, above)
    hand_neighbours(0)
    near(below_slot, 0, below)
    near(above_slot, 0, above)
    line(2)
    send_own(1, 1)

    hand_crossed(1)
    if levels > 2:
        relay_coeffs(2)
        cross_coeffs(2)
    for index in range(PIECES - 1):
        send_over(index)
    wait_block(far_beside_slot, 0, FAR_BESIDE)
    near(far_beside_slot, 0)
    wait_block(bridged_slot, 0, BRIDGED, bridged)
    near(bridged_slot, 0, bridged)
    for turn in range(3, levels):
        line(turn)
    send_own(1, 2)

    wait_block(beside_slot, 1, BESIDE)
    inner_up = jnp.logical_and(relay_up, level < levels - 2)
    inner_down = jnp.logical_and(relay_down, level > 1)

    def send_span(slot, index, target, peer, done, condition):
        span = span_of(index)
        send_rows(slot, 1, span, target, SPAN + index, peer, done, condition)

    for index in range(len(SPANS)):
        up, down = (inner_up, inner_down) if index == 0 else (relay_up, relay_down)
        send_span(beside_slot, index, core + 2, to_above, ALONG, up)
        send_span(beside_slot, index, core + 6, to_below, ALONG, down)
    send_block(beside_slot, 1, beside_slot, FAR_BESIDE, to_partner, HAND_BESIDE)
    near(beside_slot, 1)
    for hop in range(3, levels):
        relay_coeffs(hop)
        cross_coeffs(hop)
    if levels > 2:
        line(levels)
    whole = partial[column]
    for way, condition in ((0, below), (1, above)):
        whole = whole + jnp.where(condition, line_in[way], 0.0)
    whole = whole.astype(jnp.bfloat16)
    if levels > 2:
        whole = jnp.where(jnp.logical_xor(above, below), total_in[...], whole)
    parents[cluster] = whole
    for step in range(1, clusters):
        send(
            parents.at[cluster],
            parents.at[cluster],
            parent_sem.at[cluster],
            {"top": lax.rem(cluster + step, clusters)},
            PARENT + step - 1,
        )
    wait_block(far_beside_slot, 1, FAR_BESIDE)
    near(far_beside_slot, 1)
    coupling_load.wait()
    top_load.wait()
    for step in range(1, clusters):
        source = lax.rem(cluster + step, clusters)
        receive(parents.at[source], parent_sem.at[source])
    over = jnp.zeros(parents.shape[1:], jnp.float32)
    for m in range(top.shape[0]):
        over = over + dot(top[m], parents[lax.rem(cluster + 1 + m, clusters)])
    place = 2 * core + column
    fields[place] = over.astype(jnp.bfloat16)
    send(fields.at[place], fields.at[place], field_sem.at[0], to_beside, FIELD)
    send_over(PIECES - 1)
    if levels > 2:
        hand_crossed(2)
    wait_block(below_slot, 1, BELOW, below)
    wait_block(above_slot, 1, ABOVE, above)
    last_down = jnp.logical_and(relay_down, level == levels - 1)
    last_up = jnp.logical_and(relay_up, level == 0)
    send_span(below_slot, 0, core + 2, to_beside, OVER_SPAN, last_down)
    send_span(above_slot, 0, core + 6, to_beside, OVER_SPAN, last_up)
    hand_neighbours(1)
    near(below_slot, 1, below)
    near(above_slot, 1, above)

    def hand_first(index):
        span = rows_of(index)
        arrival = FAR_DIAGONAL + index
        wait_rows(diagonal_slot, 0, span, DIAGONAL + index, diagonal)
        send_rows(diagonal_slot, 0, span, diagonal_slot, arrival, to_partner, HAND_DIAGONAL, diagonal)

    def own_first(index, far=False):
        near(diagonal_slot, 0, diagonal, span=third(index), far=far)

    def far_first(index):
        wait_rows(far_diagonal_slot, 0, rows_of(index), FAR_DIAGONAL + index, diagonal)
        near(far_diagonal_slot, 0, diagonal, span=third(index))

    def third(index):
        return (index * UNITS // PIECES, (index + 1) * UNITS // PIECES)

    def wait_span(slot, index, arrival):
        wait_rows(slot, 1, span_of(index), arrival + index, diagonal)

    def hand_second(index):
        span = span_of(index)
        arrival = FAR_SPAN + index
        wait_span(diagonal_slot, index, SPAN)
        send_rows(diagonal_slot, 1, span, diagonal_slot, arrival, to_partner, HAND_DIAGONAL, diagonal)

    middle, later, ends = (0, 4), (4, 8), (8, 12)

    def own_second(span, far=False):
        near(diagonal_slot, 1, diagonal, span=span, far=far)

    def far_second(span):
        near(far_diagonal_slot, 1, diagonal, span=span)

    hand_first(0)
    own_first(0)
    wait_block(bridged_slot, 1, BRIDGED, bridged)
    near(bridged_slot, 1, bridged)
    hand_second(1)
    own_second(middle)
    hand_first(1)
    own_first(1)
    far_first(0)
    wait_span(far_diagonal_slot, 1, FAR_SPAN)
    far_second(middle)
    next_place = 2 * core + 1 - column
    receive(fields.at[next_place], field_sem.at[0])
    pair = fields.at[pl.ds(2 * core, 2)]
    send(pair, pair, field_sem.at[1], to_partner, FIELD_PAIR)
    for hop in range(3, levels):
        hand_crossed(hop)
    far_first(1)
    hand_second(2)
    own_second(later)

    steps = [step for hop in range(1, levels) for step in (-hop, hop)]
    theirs_count = [handed(step, other) for step in steps] + [crossed(step) for step in steps]
    for_count(theirs_count, lambda block: receive(block, coeff_sem.at[2 * levels]))
    theirs = fields.at[pl.ds(2 * other, 2)]
    receive(theirs, field_sem.at[1])
    far_load.wait()
    field = dot(nested[...], jnp.concatenate([fields[k] for k in range(4)], axis=1))
    for m in range(coupling.shape[0]):
        field = field + dot(coupling[m], coeffs[far_ref[0, 0, m]])
    field_ref[...] = field.astype(jnp.bfloat16)

    @pl.when(jnp.logical_not(diagonal))
    def _():
        for part in range(2):
            acc[part] += far_product(part)


    hand_first(2)
    own_first(2, far=True)
    hand_second(3)
    wait_span(far_diagonal_slot, 2, FAR_SPAN)
    far_second(later)
    hand_second(0)
    hand_second(4)
    own_second(ends, far=True)
    far_first(2)
    for index in (0, 3, 4):
        wait_span(far_diagonal_slot, index, FAR_SPAN)
    far_second(ends)

    whole_block = window.at[own_slot]
    for done, condition in (
        (TO_BESIDE, None),
        (TO_ABOVE, above),
        (TO_BELOW, below),
        (TO_PARTNER, None),
        (HAND_BESIDE, None),
        (HAND_COLUMN, jnp.logical_or(hand_below, hand_above)),
    ):
        drain(whole_block, done, condition)
    drain(window.at[own_slot, 0], OVER, relay_over)

    def drain_units(units, done, condition):
        drain(window.at[own_slot, 1, pl.ds(0, units * unit)], done, condition)

    inner = jnp.logical_or(inner_up, inner_down)
    outer = jnp.logical_and(relay_over, jnp.logical_not(inner))
    last = jnp.logical_or(last_down, last_up)
    drain_units(1, OVER_SPAN, last)
    drain_units(UNITS, ALONG, inner)
    drain_units(UNITS - 1, ALONG, outer)
    drain(whole_block, HAND_DIAGONAL, diagonal)
    drain(halves.at[0], HALF)
    drain(partial.at[0], QUARTER)
    drain(fields.at[0], FIELD)
    drain(fields.at[pl.ds(0, 2)], FIELD_PAIR)
    for step in range(1, clusters):
        drain(parents.at[0], PARENT + step - 1)
    totals = [level == 1, level == levels - 2] if levels > 2 else [below & False] * 2
    lines = [
        jnp.logical_and(neighbour, jnp.logical_not(total))
        for neighbour, total in zip((below, above), totals)
    ]
    drain_pair = ((line_out, LINE, lines), (total_out, TOTAL, totals))
    for block, done, (one, two) in drain_pair:
        drain(block.at[0], done, jnp.logical_xor(one, two))
        drain(block, done, jnp.logical_and(one, two))
    ours = [handed(step, core) for step in steps] + [crossed(step) for step in steps]
    for_count(ours, lambda block: drain(block, COEFF_PARTNER))
    for_count([crossing(step) for step in steps], lambda block: drain(block, COEFF_BESIDE))
    up_count = [above] + [jnp.logical_and(exists(-hop), above) for hop in range(1, levels)]
    down_count = [below] + [jnp.logical_and(exists(hop), below) for hop in range(1, levels)]
    for_count(up_count, lambda block: drain(block, COEFF_ABOVE))
    for_count(down_count, lambda block: drain(block, COEFF_BELOW))


def finish_kernel(count_ref, acc_ref, out_ref, staged, sem):
    steps, rows = staged.shape[:2]
    half = acc_ref.shape[2]
    copies = []
    for step in range(steps):
        span = slice(step * rows, (step + 1) * rows)
        live = lax.broadcasted_iota(jnp.int32, (rows, half), 0) < count_ref[0, 0] - step * rows
        for part in range(2):
            columns = slice(part * half, (part + 1) * half)
            staged[step, :, columns] = jnp.where(live, acc_ref[part, span], 0.0)
        copy = pltpu.make_async_copy(staged.at[step], out_ref.at[span], sem.at[step])
        copy.start()
        copies.append(copy)
    for copy in copies:
        copy.wait()


def body(
    vectors,
    near_tiles,
    leaf_basis,
    transfer,
    coupling,
    top_coupling,
    near_list,
    far_list,
    row_counts,
):
    leaves = lax.axis_size("leaf")
    clusters = lax.axis_size("top")
    levels = leaves // 4
    rows, vecs = vectors.shape[2:]
    rank = transfer.shape[2]
    half, quarter = vecs // 2, vecs // 4
    smem = pl.BlockSpec(memory_space=pltpu.SMEM)
    vmem = pl.BlockSpec(memory_space=pltpu.VMEM)
    hbm = pl.BlockSpec(memory_space=pltpu.HBM)
    dma = pltpu.SemaphoreType.DMA
    acc = pl.pallas_call(
        functools.partial(exchange_kernel, levels, clusters),
        out_shape=jax.ShapeDtypeStruct((2, rows, half), jnp.float32),
        in_specs=[smem] + [hbm] * 8,
        out_specs=vmem,
        scratch_shapes=[
            pltpu.SMEM(near_list.shape, jnp.int32),
            pltpu.SMEM(far_list.shape, jnp.int32),
            pltpu.VMEM((2, rows, half), jnp.bfloat16),
            pltpu.VMEM(near_tiles.shape[2:], jnp.bfloat16),
            pltpu.VMEM(leaf_basis.shape[2:], jnp.bfloat16),
            pltpu.VMEM(transfer.shape[2:], jnp.bfloat16),
            pltpu.VMEM(coupling.shape[2:], jnp.bfloat16),
            pltpu.VMEM(top_coupling.shape[1:], jnp.bfloat16),
            pltpu.VMEM((SLOTS, 2, rows, half), jnp.bfloat16),
            pltpu.VMEM((leaves, rank, vecs), jnp.bfloat16),
            pltpu.VMEM((2, rank, half), jnp.float32),
            pltpu.VMEM((rank, half), jnp.float32),
            pltpu.VMEM((2, rank, quarter), jnp.float32),
            pltpu.VMEM((rank, quarter), jnp.float32),
            pltpu.VMEM((2, rank, quarter), jnp.float32),
            pltpu.VMEM((2, rank, quarter), jnp.float32),
            pltpu.VMEM((2, rank, quarter), jnp.bfloat16),
            pltpu.VMEM((rank, quarter), jnp.bfloat16),
            pltpu.VMEM((clusters, rank, quarter), jnp.bfloat16),
            pltpu.VMEM((4, rank, quarter), jnp.bfloat16),
            pltpu.VMEM((rank, vecs), jnp.bfloat16),
            dma((9,)),
            dma((PARENT + clusters - 1,)),
            dma((ARRIVALS,)),
            dma((leaves // 2 + 1,)),
            dma((1,)),
            dma((1,)),
            dma((2,)),
            dma((clusters,)),
            dma((2,)),
        ],
        compiler_params=pltpu.CompilerParams(
            collective_id=0, has_side_effects=True, vmem_limit_bytes=48 * 1024 * 1024
        ),
    )(
        row_counts,
        *[
            pltpu.with_memory_space_constraint(array, pltpu.HBM)
            for array in (
                near_list,
                far_list,
                vectors,
                near_tiles,
                leaf_basis,
                transfer,
                coupling,
                top_coupling,
            )
        ],
    )
    result = pl.pallas_call(
        finish_kernel,
        out_shape=jax.ShapeDtypeStruct((rows, vecs), jnp.float32),
        in_specs=[smem, vmem],
        out_specs=pl.BlockSpec(memory_space=pl.ANY),
        scratch_shapes=[
            pltpu.VMEM((PIECES, rows // PIECES, vecs), jnp.float32),
            dma((PIECES,)),
        ],
        compiler_params=pltpu.CompilerParams(vmem_limit_bytes=8 * 1024 * 1024),
    )(row_counts, acc)
    return result[None, None]


def solution(mesh):
    in_specs = (
        P("top", "leaf", None, None),
        P("top", "leaf", None, None, None),
        P("top", "leaf", None, None),
        P("top", "leaf", None, None),
        P("top", "leaf", None, None, None),
        P("top", None, None, None),
        P("top", "leaf", None),
        P("top", "leaf", None),
        P("top", "leaf"),
    )
    out_specs = P("top", "leaf", None, None)
    return jax.shard_map(body, mesh=mesh, in_specs=in_specs, out_specs=out_specs, check_vma=False)
```

```python
import functools

import jax
import jax.numpy as jnp
from jax import lax
from jax.experimental import pallas as pl
from jax.experimental.pallas import tpu as pltpu
from jax.sharding import PartitionSpec as P

REACH = 4
SLOTS = 2 * REACH + 2
PIECES = 3
UNITS = 12
SPANS = ((8, 9), (0, 4), (4, 8), (9, 12))
BESIDE, BELOW, ABOVE, PARTNER, FAR_BESIDE, BRIDGED = 0, 2, 4, 6, 8, 10
DIAGONAL, FAR_DIAGONAL, SPAN = 12, 12 + PIECES, 12 + 2 * PIECES
FAR_SPAN = SPAN + len(SPANS)
ARRIVALS = FAR_SPAN + len(SPANS)
(
    TO_BESIDE,
    TO_ABOVE,
    TO_BELOW,
    TO_PARTNER,
    OVER,
    OVER_SPAN,
    ALONG,
    HAND_BESIDE,
    HAND_COLUMN,
    HAND_DIAGONAL,
    COEFF_ABOVE,
    COEFF_BELOW,
    COEFF_BESIDE,
    COEFF_PARTNER,
    HALF,
    QUARTER,
    LINE,
    TOTAL,
    FIELD,
    FIELD_PAIR,
    PARENT,
) = range(21)


def contract(left, right):
    return lax.dot_general(left, right, (((0,), (0,)), ((), ())), preferred_element_type=jnp.float32)


def dot(left, right):
    return jnp.dot(left, right, preferred_element_type=jnp.float32)


def exchange_kernel(
    levels,
    clusters,
    count_ref,
    near_source,
    far_source,
    vectors_ref,
    tiles_ref,
    basis_ref,
    nested_ref,
    coupling_ref,
    top_ref,
    acc,
    near_ref,
    far_ref,
    raw,
    tiles,
    basis,
    nested,
    coupling,
    top,
    window,
    coeffs,
    halves,
    half_in,
    partial,
    quarter_in,
    line_out,
    line_in,
    total_out,
    total_in,
    parents,
    fields,
    field_ref,
    load_sem,
    send_sem,
    block_sem,
    coeff_sem,
    half_sem,
    quarter_sem,
    line_sem,
    parent_sem,
    field_sem,
):
    me = lax.axis_index("leaf")
    cluster = lax.axis_index("top")
    core = lax.rem(me, 2)
    column = lax.rem(lax.div(me, 2), 2)
    level = lax.div(me, 4)
    other = 1 - core
    partner = me + 1 - 2 * core
    beside = me + 2 - 4 * column
    above = level < levels - 1
    below = level > 0
    first_column = column == 0
    rows, half = raw.shape[1:]
    vecs = 2 * half
    quarter = half // 2
    unit = rows // UNITS
    piece = rows // PIECES
    tile_count = tiles.shape[0]

    def load(source, target, sem):
        return pltpu.make_async_copy(source, target, sem)

    raw_loads = [
        load(vectors_ref.at[0, 0, :, pl.ds(part * half, half)], raw.at[part], load_sem.at[part])
        for part in range(2)
    ]
    basis_load = load(basis_ref.at[0, 0], basis, load_sem.at[2])
    nested_load = load(nested_ref.at[0, 0], nested, load_sem.at[7])
    coupling_load = load(coupling_ref.at[0, 0], coupling, load_sem.at[3])
    top_load = load(top_ref.at[0], top, load_sem.at[4])
    tile_loads = [load(tiles_ref.at[0, 0, k], tiles.at[k], load_sem.at[8]) for k in range(tile_count)]
    all_tiles = load(tiles_ref.at[0, 0], tiles, load_sem.at[8])
    near_load = load(near_source, near_ref, load_sem.at[5])
    far_load = load(far_source, far_ref, load_sem.at[6])

    barrier = pltpu.get_barrier_semaphore()

    def greet(peer):
        pl.semaphore_signal(barrier, inc=1, device_id=peer, device_id_type=pl.DeviceIdType.MESH)

    greet({"leaf": partner})
    greet({"leaf": beside})
    for step in range(1, clusters):
        greet({"top": lax.rem(cluster + step, clusters)})
    pl.when(above)(lambda: greet({"leaf": me + 4}))
    pl.when(below)(lambda: greet({"leaf": me - 4}))
    expected = clusters + 1 + above.astype(jnp.int32) + below.astype(jnp.int32)
    for copy in raw_loads + [basis_load, nested_load, near_load]:
        copy.start()

    def remote(source, target, sem, peer, done):
        return pltpu.make_async_remote_copy(
            src_ref=source,
            dst_ref=target,
            send_sem=send_sem.at[done],
            recv_sem=sem,
            device_id=peer,
            device_id_type=pl.DeviceIdType.MESH,
        )

    def send(source, target, sem, peer, done, condition=None):
        copy = remote(source, target, sem, peer, done)
        if condition is None:
            copy.start()
        else:
            pl.when(condition)(copy.start)

    def receive(block, sem, condition=None):
        copy = remote(block, block, sem, {"leaf": partner}, 0)
        if condition is None:
            copy.wait_recv()
        else:
            pl.when(condition)(copy.wait_recv)

    def drain(block, done, condition=None):
        copy = remote(block, block, block_sem.at[0], {"leaf": partner}, done)
        if condition is None:
            copy.wait_send()
        else:
            pl.when(condition)(copy.wait_send)

    to_partner, to_beside = {"leaf": partner}, {"leaf": beside}
    to_above, to_below = {"leaf": me + 4}, {"leaf": me - 4}

    own_slot = REACH + core
    partner_slot = REACH + other
    beside_slot = core + 6 - 4 * column
    diagonal_slot = core + 2 + 4 * column
    below_slot = core
    above_slot = core + 8
    diagonal = jnp.logical_or(
        jnp.logical_and(first_column, below), jnp.logical_and(column == 1, above)
    )
    relay_over = jnp.logical_or(
        jnp.logical_and(column == 1, below), jnp.logical_and(first_column, above)
    )
    relay_up = jnp.logical_and(first_column, above)
    relay_down = jnp.logical_and(column == 1, below)

    def send_block(slot, part, target, arrival, peer, done, condition=None):
        send(
            window.at[slot, part],
            window.at[target, part],
            block_sem.at[arrival + part],
            peer,
            done,
            condition,
        )

    def wait_block(slot, part, arrival, condition=None):
        receive(window.at[slot, part], block_sem.at[arrival + part], condition)

    def rows_of(index):
        return pl.ds(index * piece, piece)

    def span_of(index):
        start, stop = SPANS[index]
        return pl.ds(start * unit, (stop - start) * unit)

    def send_rows(slot, part, span, target, arrival, peer, done, condition=None):
        send(
            window.at[slot, part, span],
            window.at[target, part, span],
            block_sem.at[arrival],
            peer,
            done,
            condition,
        )

    def wait_rows(slot, part, span, arrival, condition=None):
        receive(window.at[slot, part, span], block_sem.at[arrival], condition)

    def send_coeff(leaf, peer, done, condition=None):
        send(coeffs.at[leaf], coeffs.at[leaf], coeff_sem.at[lax.div(leaf, 2)], peer, done, condition)

    def hand_coeff(leaf, condition):
        send(
            coeffs.at[leaf],
            coeffs.at[leaf],
            coeff_sem.at[2 * levels],
            to_partner,
            COEFF_PARTNER,
            condition,
        )

    def wait_coeff(leaf, condition=None):
        receive(coeffs.at[leaf], coeff_sem.at[lax.div(leaf, 2)], condition)

    def for_count(conditions, run):
        count = 0
        for condition in conditions:
            count = count + jnp.where(condition, 1, 0)
        for n in range(1, len(conditions) + 1):
            pl.when(count == n)(lambda n=n: run(coeffs.at[pl.ds(0, n)]))

    def exists(step):
        return jnp.logical_and(level + step >= 0, level + step < levels)

    def crosses(step, from_first):
        return step <= -1 or step >= 2 if from_first else step >= 1 or step <= -2

    def crossing(step):
        if crosses(step, True) and crosses(step, False):
            return exists(step)
        return jnp.logical_and(exists(step), first_column if crosses(step, True) else column == 1)

    def crossed(step):
        if crosses(step, True) and crosses(step, False):
            return exists(step)
        return jnp.logical_and(exists(step), column == 1 if crosses(step, True) else first_column)

    def handed(step, which):
        if abs(step) >= 2:
            return exists(step)
        return jnp.logical_and(exists(step), which == (1 if step == 1 else 0))

    def relay_coeffs(hop):
        for step in (-hop, hop):
            wait_coeff(me + 4 * step, exists(step))
        if hop + 1 < levels:
            send_coeff(me - 4 * hop, to_above, COEFF_ABOVE, jnp.logical_and(exists(-hop), above))
            send_coeff(me + 4 * hop, to_below, COEFF_BELOW, jnp.logical_and(exists(hop), below))

    def cross_coeffs(hop):
        for step in (-hop, hop):
            send_coeff(me + 4 * step, to_beside, COEFF_BESIDE, crossing(step))
            hand_coeff(me + 4 * step, handed(step, core))

    def hand_crossed(hop):
        for step in (-hop, hop):
            wait_coeff(beside + 4 * step, crossed(step))
            hand_coeff(beside + 4 * step, crossed(step))

    def far_product(part):
        return dot(basis[...], field_ref[:, part * half : (part + 1) * half])

    def near(slot, part, condition=None, first=False, span=None, far=False):
        offset = slot - REACH - core
        place, hit = 0, 0
        for k in range(tile_count):
            here = near_ref[0, 0, k] == offset
            place = jnp.where(here, k, place)
            hit = jnp.where(here, 1, hit)
        scale = hit.astype(jnp.float32)

        def run():
            if span is None:
                product = dot(tiles[place], window[slot, part]) * scale
            else:
                lines = slice(span[0] * unit, span[1] * unit)
                product = dot(tiles[place, :, lines], window[slot, part, lines, :]) * scale
            if far:
                product = product + far_product(part)
            if first:
                acc[part] = product
            else:
                acc[part] += product

        if condition is None:
            run()
        else:
            pl.when(condition)(run)

    own_beside = own_slot + 4 * column - 2

    def send_own(part, index):
        span = rows_of(index)
        send_rows(own_slot, part, span, core, BELOW + part, to_above, TO_ABOVE, above)
        send_rows(own_slot, part, span, core + 8, ABOVE + part, to_below, TO_BELOW, below)

    def send_first(index):
        send_rows(own_slot, 0, rows_of(index), own_beside, BESIDE, to_beside, TO_BESIDE)

    live = lax.broadcasted_iota(jnp.int32, (rows, half), 0) < count_ref[0, 0]

    def mask(part):
        raw_loads[part].wait()
        window[own_slot, part] = jnp.where(live, raw[part], jnp.zeros((), jnp.bfloat16))

    mask(0)
    pl.semaphore_wait(barrier, expected)
    for index in range(PIECES - 1):
        send_first(index)
    send_own(0, 0)
    mask(1)
    basis_load.wait()
    for part in range(2):
        product = contract(basis[...], window[own_slot, part])
        coeffs[me, :, part * half : (part + 1) * half] = product.astype(jnp.bfloat16)
    nested_load.wait()
    for part in range(2):
        halves[part] = contract(nested[...], coeffs[me, :, part * half : (part + 1) * half])
    send_coeff(me, to_above, COEFF_ABOVE, above)
    send_coeff(me, to_below, COEFF_BELOW, below)
    for index in range(1, PIECES):
        send_own(0, index)
    send(halves.at[other], half_in, half_sem.at[0], to_partner, HALF)
    for part in range(2):
        send_block(own_slot, part, own_slot, PARTNER, to_partner, TO_PARTNER)
    for copy in tile_loads + [far_load, coupling_load, top_load]:
        copy.start()

    receive(half_in, half_sem.at[0])
    total = halves[core] + half_in[...]
    for part in range(2):
        partial[part] = total[:, part * quarter : (part + 1) * quarter]
    send(partial.at[1 - column], quarter_in, quarter_sem.at[0], to_beside, QUARTER)
    send_first(PIECES - 1)
    near_load.wait()
    all_tiles.wait()
    near(own_slot, 0, first=True)
    near(own_slot, 1, first=True)
    for part in range(2):
        wait_block(partner_slot, part, PARTNER)
        near(partner_slot, part)

    relay_coeffs(1)
    cross_coeffs(1)
    send_block(own_slot, 1, own_beside, BESIDE, to_beside, TO_BESIDE)
    receive(quarter_in, quarter_sem.at[0])
    partial[column] += quarter_in[...]

    def line(turn):
        ways = ((0, turn - 1, 4), (1, levels - turn, -4))
        whole = 2 < levels == turn + 1
        if turn > 1:
            for way, at, _ in ways:
                block = total_in if 2 < levels == turn else line_in.at[way]
                receive(block, line_sem.at[way], level == at)
        if turn < levels:
            for way, at, step in ways:

                @pl.when(level == at)
                def _(way=way):
                    value = partial[column]
                    if turn > 1:
                        value = value + line_in[way]
                    if whole:
                        value = value + line_in[1 - way]
                        total_out[way] = value.astype(jnp.bfloat16)
                    else:
                        line_out[way] = value

                peer = {"leaf": me + step}
                if whole:
                    send(total_out.at[way], total_in, line_sem.at[way], peer, TOTAL, level == at)
                else:
                    send(line_out.at[way], line_in.at[way], line_sem.at[way], peer, LINE, level == at)

    line(1)
    send_own(1, 0)

    bridged_slot = jnp.where(core == 0, 1, 8)
    bridged = jnp.logical_or(
        jnp.logical_and(core == 0, below), jnp.logical_and(core == 1, above)
    )
    hand_below = jnp.logical_and(core == 1, below)
    hand_above = jnp.logical_and(core == 0, above)
    far_beside_slot = other + 6 - 4 * column
    far_diagonal_slot = other + 2 + 4 * column

    def hand_neighbours(part):
        send_block(below_slot, part, below_slot, BRIDGED, to_partner, HAND_COLUMN, hand_below)
        send_block(above_slot, part, above_slot, BRIDGED, to_partner, HAND_COLUMN, hand_above)

    def send_over(index):
        span = rows_of(index)
        arrival = DIAGONAL + index
        send_rows(below_slot, 0, span, core + 2, arrival, to_beside, OVER, relay_down)
        send_rows(above_slot, 0, span, core + 6, arrival, to_beside, OVER, relay_up)

    wait_block(beside_slot, 0, BESIDE)
    send_block(beside_slot, 0, beside_slot, FAR_BESIDE, to_partner, HAND_BESIDE)
    near(beside_slot, 0)
    wait_block(below_slot, 0, BELOW, below)
    wait_block(above_slot, 0, ABOVE, above)
    hand_neighbours(0)
    near(below_slot, 0, below)
    near(above_slot, 0, above)
    line(2)
    send_own(1, 1)

    hand_crossed(1)
    if levels > 2:
        relay_coeffs(2)
        cross_coeffs(2)
    for index in range(PIECES - 1):
        send_over(index)
    wait_block(far_beside_slot, 0, FAR_BESIDE)
    near(far_beside_slot, 0)
    wait_block(bridged_slot, 0, BRIDGED, bridged)
    near(bridged_slot, 0, bridged)
    for turn in range(3, levels):
        line(turn)
    send_own(1, 2)

    wait_block(beside_slot, 1, BESIDE)
    inner_up = jnp.logical_and(relay_up, level < levels - 2)
    inner_down = jnp.logical_and(relay_down, level > 1)

    def send_span(slot, index, target, peer, done, condition):
        span = span_of(index)
        send_rows(slot, 1, span, target, SPAN + index, peer, done, condition)

    for index in range(len(SPANS)):
        up, down = (inner_up, inner_down) if index == 0 else (relay_up, relay_down)
        send_span(beside_slot, index, core + 2, to_above, ALONG, up)
        send_span(beside_slot, index, core + 6, to_below, ALONG, down)
    send_block(beside_slot, 1, beside_slot, FAR_BESIDE, to_partner, HAND_BESIDE)
    near(beside_slot, 1)
    for hop in range(3, levels):
        relay_coeffs(hop)
        cross_coeffs(hop)
    if levels > 2:
        line(levels)
    whole = partial[column]
    for way, condition in ((0, below), (1, above)):
        whole = whole + jnp.where(condition, line_in[way], 0.0)
    whole = whole.astype(jnp.bfloat16)
    if levels > 2:
        whole = jnp.where(jnp.logical_xor(above, below), total_in[...], whole)
    parents[cluster] = whole
    for step in range(1, clusters):
        send(
            parents.at[cluster],
            parents.at[cluster],
            parent_sem.at[cluster],
            {"top": lax.rem(cluster + step, clusters)},
            PARENT + step - 1,
        )
    wait_block(far_beside_slot, 1, FAR_BESIDE)
    near(far_beside_slot, 1)
    coupling_load.wait()
    top_load.wait()
    for step in range(1, clusters):
        source = lax.rem(cluster + step, clusters)
        receive(parents.at[source], parent_sem.at[source])
    over = jnp.zeros(parents.shape[1:], jnp.float32)
    for m in range(top.shape[0]):
        over = over + dot(top[m], parents[lax.rem(cluster + 1 + m, clusters)])
    place = 2 * core + column
    fields[place] = over.astype(jnp.bfloat16)
    send(fields.at[place], fields.at[place], field_sem.at[0], to_beside, FIELD)
    send_over(PIECES - 1)
    if levels > 2:
        hand_crossed(2)
    wait_block(below_slot, 1, BELOW, below)
    wait_block(above_slot, 1, ABOVE, above)
    last_down = jnp.logical_and(relay_down, level == levels - 1)
    last_up = jnp.logical_and(relay_up, level == 0)
    send_span(below_slot, 0, core + 2, to_beside, OVER_SPAN, last_down)
    send_span(above_slot, 0, core + 6, to_beside, OVER_SPAN, last_up)
    hand_neighbours(1)
    near(below_slot, 1, below)
    near(above_slot, 1, above)

    def hand_first(index):
        span = rows_of(index)
        arrival = FAR_DIAGONAL + index
        wait_rows(diagonal_slot, 0, span, DIAGONAL + index, diagonal)
        send_rows(diagonal_slot, 0, span, diagonal_slot, arrival, to_partner, HAND_DIAGONAL, diagonal)

    def own_first(index, far=False):
        near(diagonal_slot, 0, diagonal, span=third(index), far=far)

    def far_first(index):
        wait_rows(far_diagonal_slot, 0, rows_of(index), FAR_DIAGONAL + index, diagonal)
        near(far_diagonal_slot, 0, diagonal, span=third(index))

    def third(index):
        return (index * UNITS // PIECES, (index + 1) * UNITS // PIECES)

    def wait_span(slot, index, arrival):
        wait_rows(slot, 1, span_of(index), arrival + index, diagonal)

    def hand_second(index):
        span = span_of(index)
        arrival = FAR_SPAN + index
        wait_span(diagonal_slot, index, SPAN)
        send_rows(diagonal_slot, 1, span, diagonal_slot, arrival, to_partner, HAND_DIAGONAL, diagonal)

    middle, later, ends = (0, 4), (4, 8), (8, 12)

    def own_second(span, far=False):
        near(diagonal_slot, 1, diagonal, span=span, far=far)

    def far_second(span):
        near(far_diagonal_slot, 1, diagonal, span=span)

    hand_first(0)
    own_first(0)
    wait_block(bridged_slot, 1, BRIDGED, bridged)
    near(bridged_slot, 1, bridged)
    hand_second(1)
    own_second(middle)
    hand_first(1)
    own_first(1)
    far_first(0)
    wait_span(far_diagonal_slot, 1, FAR_SPAN)
    far_second(middle)
    next_place = 2 * core + 1 - column
    receive(fields.at[next_place], field_sem.at[0])
    pair = fields.at[pl.ds(2 * core, 2)]
    send(pair, pair, field_sem.at[1], to_partner, FIELD_PAIR)
    for hop in range(3, levels):
        hand_crossed(hop)
    far_first(1)
    hand_second(2)
    own_second(later)

    steps = [step for hop in range(1, levels) for step in (-hop, hop)]
    theirs_count = [handed(step, other) for step in steps] + [crossed(step) for step in steps]
    for_count(theirs_count, lambda block: receive(block, coeff_sem.at[2 * levels]))
    theirs = fields.at[pl.ds(2 * other, 2)]
    receive(theirs, field_sem.at[1])
    far_load.wait()
    field = dot(nested[...], jnp.concatenate([fields[k] for k in range(4)], axis=1))
    for m in range(coupling.shape[0]):
        field = field + dot(coupling[m], coeffs[far_ref[0, 0, m]])
    field_ref[...] = field.astype(jnp.bfloat16)

    @pl.when(jnp.logical_not(diagonal))
    def _():
        for part in range(2):
            acc[part] += far_product(part)


    hand_first(2)
    own_first(2, far=True)
    hand_second(3)
    hand_second(0)
    wait_span(far_diagonal_slot, 2, FAR_SPAN)
    far_second(later)
    own_second(ends, far=True)
    far_first(2)
    wait_span(far_diagonal_slot, 3, FAR_SPAN)
    wait_span(far_diagonal_slot, 0, FAR_SPAN)
    far_second(ends)

    whole_block = window.at[own_slot]
    for done, condition in (
        (TO_BESIDE, None),
        (TO_ABOVE, above),
        (TO_BELOW, below),
        (TO_PARTNER, None),
        (HAND_BESIDE, None),
        (HAND_COLUMN, jnp.logical_or(hand_below, hand_above)),
    ):
        drain(whole_block, done, condition)
    drain(window.at[own_slot, 0], OVER, relay_over)

    def drain_units(units, done, condition):
        drain(window.at[own_slot, 1, pl.ds(0, units * unit)], done, condition)

    inner = jnp.logical_or(inner_up, inner_down)
    outer = jnp.logical_and(relay_over, jnp.logical_not(inner))
    last = jnp.logical_or(last_down, last_up)
    drain_units(1, OVER_SPAN, last)
    drain_units(UNITS, ALONG, inner)
    drain_units(UNITS - 1, ALONG, outer)
    drain(whole_block, HAND_DIAGONAL, diagonal)
    drain(halves.at[0], HALF)
    drain(partial.at[0], QUARTER)
    drain(fields.at[0], FIELD)
    drain(fields.at[pl.ds(0, 2)], FIELD_PAIR)
    for step in range(1, clusters):
        drain(parents.at[0], PARENT + step - 1)
    totals = [level == 1, level == levels - 2] if levels > 2 else [below & False] * 2
    lines = [
        jnp.logical_and(neighbour, jnp.logical_not(total))
        for neighbour, total in zip((below, above), totals)
    ]
    drain_pair = ((line_out, LINE, lines), (total_out, TOTAL, totals))
    for block, done, (one, two) in drain_pair:
        drain(block.at[0], done, jnp.logical_xor(one, two))
        drain(block, done, jnp.logical_and(one, two))
    ours = [handed(step, core) for step in steps] + [crossed(step) for step in steps]
    for_count(ours, lambda block: drain(block, COEFF_PARTNER))
    for_count([crossing(step) for step in steps], lambda block: drain(block, COEFF_BESIDE))
    up_count = [above] + [jnp.logical_and(exists(-hop), above) for hop in range(1, levels)]
    down_count = [below] + [jnp.logical_and(exists(hop), below) for hop in range(1, levels)]
    for_count(up_count, lambda block: drain(block, COEFF_ABOVE))
    for_count(down_count, lambda block: drain(block, COEFF_BELOW))


def finish_kernel(count_ref, acc_ref, out_ref, staged, sem):
    steps, rows = staged.shape[:2]
    half = acc_ref.shape[2]
    copies = []
    for step in range(steps):
        span = slice(step * rows, (step + 1) * rows)
        live = lax.broadcasted_iota(jnp.int32, (rows, half), 0) < count_ref[0, 0] - step * rows
        for part in range(2):
            columns = slice(part * half, (part + 1) * half)
            staged[step, :, columns] = jnp.where(live, acc_ref[part, span], 0.0)
        copy = pltpu.make_async_copy(staged.at[step], out_ref.at[span], sem.at[step])
        copy.start()
        copies.append(copy)
    for copy in copies:
        copy.wait()


def body(
    vectors,
    near_tiles,
    leaf_basis,
    transfer,
    coupling,
    top_coupling,
    near_list,
    far_list,
    row_counts,
):
    leaves = lax.axis_size("leaf")
    clusters = lax.axis_size("top")
    levels = leaves // 4
    rows, vecs = vectors.shape[2:]
    rank = transfer.shape[2]
    half, quarter = vecs // 2, vecs // 4
    smem = pl.BlockSpec(memory_space=pltpu.SMEM)
    vmem = pl.BlockSpec(memory_space=pltpu.VMEM)
    hbm = pl.BlockSpec(memory_space=pltpu.HBM)
    dma = pltpu.SemaphoreType.DMA
    acc = pl.pallas_call(
        functools.partial(exchange_kernel, levels, clusters),
        out_shape=jax.ShapeDtypeStruct((2, rows, half), jnp.float32),
        in_specs=[smem] + [hbm] * 8,
        out_specs=vmem,
        scratch_shapes=[
            pltpu.SMEM(near_list.shape, jnp.int32),
            pltpu.SMEM(far_list.shape, jnp.int32),
            pltpu.VMEM((2, rows, half), jnp.bfloat16),
            pltpu.VMEM(near_tiles.shape[2:], jnp.bfloat16),
            pltpu.VMEM(leaf_basis.shape[2:], jnp.bfloat16),
            pltpu.VMEM(transfer.shape[2:], jnp.bfloat16),
            pltpu.VMEM(coupling.shape[2:], jnp.bfloat16),
            pltpu.VMEM(top_coupling.shape[1:], jnp.bfloat16),
            pltpu.VMEM((SLOTS, 2, rows, half), jnp.bfloat16),
            pltpu.VMEM((leaves, rank, vecs), jnp.bfloat16),
            pltpu.VMEM((2, rank, half), jnp.float32),
            pltpu.VMEM((rank, half), jnp.float32),
            pltpu.VMEM((2, rank, quarter), jnp.float32),
            pltpu.VMEM((rank, quarter), jnp.float32),
            pltpu.VMEM((2, rank, quarter), jnp.float32),
            pltpu.VMEM((2, rank, quarter), jnp.float32),
            pltpu.VMEM((2, rank, quarter), jnp.bfloat16),
            pltpu.VMEM((rank, quarter), jnp.bfloat16),
            pltpu.VMEM((clusters, rank, quarter), jnp.bfloat16),
            pltpu.VMEM((4, rank, quarter), jnp.bfloat16),
            pltpu.VMEM((rank, vecs), jnp.bfloat16),
            dma((9,)),
            dma((PARENT + clusters - 1,)),
            dma((ARRIVALS,)),
            dma((leaves // 2 + 1,)),
            dma((1,)),
            dma((1,)),
            dma((2,)),
            dma((clusters,)),
            dma((2,)),
        ],
        compiler_params=pltpu.CompilerParams(
            collective_id=0, has_side_effects=True, vmem_limit_bytes=48 * 1024 * 1024
        ),
    )(
        row_counts,
        *[
            pltpu.with_memory_space_constraint(array, pltpu.HBM)
            for array in (
                near_list,
                far_list,
                vectors,
                near_tiles,
                leaf_basis,
                transfer,
                coupling,
                top_coupling,
            )
        ],
    )
    result = pl.pallas_call(
        finish_kernel,
        out_shape=jax.ShapeDtypeStruct((rows, vecs), jnp.float32),
        in_specs=[smem, vmem],
        out_specs=pl.BlockSpec(memory_space=pl.ANY),
        scratch_shapes=[
            pltpu.VMEM((PIECES, rows // PIECES, vecs), jnp.float32),
            dma((PIECES,)),
        ],
        compiler_params=pltpu.CompilerParams(vmem_limit_bytes=8 * 1024 * 1024),
    )(row_counts, acc)
    return result[None, None]


def solution(mesh):
    in_specs = (
        P("top", "leaf", None, None),
        P("top", "leaf", None, None, None),
        P("top", "leaf", None, None),
        P("top", "leaf", None, None),
        P("top", "leaf", None, None, None),
        P("top", None, None, None),
        P("top", "leaf", None),
        P("top", "leaf", None),
        P("top", "leaf"),
    )
    out_specs = P("top", "leaf", None, None)
    return jax.shard_map(body, mesh=mesh, in_specs=in_specs, out_specs=out_specs, check_vma=False)
```
